128 devices in a mesh: cls: 4 (over z), site: 32 (over x, y, core).
Axes of the slice: x: 4, y: 4, z: 4, core: 2. Of those that a mesh axis runs over, the one named last changes fastest.
Arguments:
- tip_codes: int32 [1024, 32768], P('cls', 'site'), may hold values from 0 to 3
- counts: int32 [32768], P('site'), may hold values from 1 to 5
- children: int32 [1023, 2], replicated, may hold values from 0 to 2045, as said below
- lengths: float32 [4, 2046], replicated, may hold values from 0.01 to 1
- frequencies: float32 [4, 4], replicated, may hold values from 0.25 to 1.75
- weights: float32 [4], replicated, may hold values from 0.2 to 1
Outputs:
- site_loglik: float32 [4, 8192], P('cls', 'site')
- new_weights: float32 [4], P('cls')
- mean_loglik: float32 [], replicated
The draws below stay inside these ranges and needn't reach their ends.
Inputs may be any that keep to these rules, and one draw needn't show every extreme that they name: Row k lists the two children of internal node 1024 + k as node ids. Give the tips height 0 and the root height 10. The nodes of height h + 1 have exactly the nodes of height h as children, each once, and the root is node 2046. For every height h from 0 to 5, split the parents (height h + 1) and the children (height h) into 16 equal aligned blocks: the children of parent block j are child block j, so the tips j * 64 onward form clade j.
All inputs are finite; a program needn't handle non-finite values.
Results may differ from the reference program's by a relative error of at most 0.0003.
Values sent between devices are 32-bit elements; how exact they have to be, the bound alone decides.
No kernel may reach another device: no remote copies, remote signals or barrier semaphores. Data moves between devices by JAX's collectives and lax.ppermute only.
A program may use at most 64 MiB of HBM per device.

```python
import math
import jax
import jax.numpy as jnp
from jax import lax

LEVELS = 10
TOP = 4
CLS = 4
SITE_DEV = 1024
TAXA = 1024
BRANCHES = 2046
SITES = 32768
N_SITE = 32


def draw_children(key, part):
    pieces = []
    for tree_level in range(LEVELS):
        level_below = TAXA >> tree_level
        if tree_level == 0:
            first_id = 0
        else:
            first_id = TAXA + TAXA - (TAXA >> tree_level - 1)
        if tree_level < LEVELS - TOP:
            blocks = 2 ** TOP
        else:
            blocks = 1
        block_size = level_below // blocks
        level_key = jax.random.fold_in(key, 17 + tree_level)
        block_keys = jax.random.split(level_key, blocks)
        shuffled = jax.vmap(lambda one_key: jax.random.permutation(one_key, block_size))(block_keys)
        shuffled = shuffled.astype(jnp.int32) + (jnp.arange(blocks, dtype=jnp.int32) * block_size)[:, None]
        pieces.append((shuffled.reshape(level_below // 2, 2) + first_id).astype(jnp.int32))
    return jnp.concatenate(pieces, axis=0)


def draw_counts(key, part):
    position = jnp.arange(SITES, dtype=jnp.int32)
    upper_end = 2 + 5 * position // SITES
    return jax.random.randint(jax.random.fold_in(key, 5), (SITES,), 1, upper_end, dtype=jnp.int32)


def with_ends(values, own_key, low, high):
    dims = values.shape
    spot = [jax.random.randint(jax.random.fold_in(own_key, axis), (), 0, dims[axis]) for axis in range(len(dims))]
    values = values.at[tuple(spot)].set(low)
    longest = dims.index(max(dims))
    spot[longest] = (spot[longest] + 1) % dims[longest]
    return values.at[tuple(spot)].set(high)


def setup_inputs(seed: int = 0) -> dict:
    keys = jax.random.split(jax.random.key(seed), 7)
    return {
        "tip_codes": with_ends(jax.random.randint(keys[0], (TAXA, SITES), 0, 4), jax.random.fold_in(keys[0], 1), 0, 3).astype(jnp.int32),
        "counts": draw_counts(jax.random.fold_in(keys[6], 71), 0),
        "children": draw_children(jax.random.fold_in(keys[6], 71), 0),
        "lengths": jnp.clip(jnp.exp(jax.random.uniform(keys[3], (CLS, BRANCHES), jnp.float32, math.log(0.01), math.log(1.0))), 0.01, 1.0),
        "frequencies": jnp.clip(1.0 + 0.15 * jax.random.normal(keys[4], (CLS, 4), jnp.float32), 0.25, 1.75),
        "weights": jnp.clip(jnp.exp(jax.random.uniform(keys[5], (CLS,), jnp.float32, math.log(0.2), math.log(1.0))), 0.2, 1.0),
    }


def transit(values, decays, stationary):
    average = jnp.sum(stationary[None, :, None] * values, axis=1, keepdims=True)
    return decays[:, None, None] * values + (1.0 - decays)[:, None, None] * average


def from_codes(codes, decays, stationary):
    states = jnp.arange(4, dtype=jnp.int32)
    onehot = (codes[:, None, :] == states[None, :, None]).astype(jnp.float32)
    return transit(onehot, decays, stationary)


def join_pair(left_part, right_part, scale_sum):
    parent = left_part * right_part
    largest = jnp.max(parent, axis=1, keepdims=True)
    return parent / largest, scale_sum + jnp.log(largest)


def class_loglik(tip_block, children, length_row, stationary):
    rate_scale = 1.0 / (1.0 - jnp.sum(stationary * stationary))
    values = None
    scales = None
    for tree_level in range(LEVELS):
        node_count = TAXA >> (tree_level + 1)
        offset = TAXA - (TAXA >> tree_level)
        child_ids = children[offset:offset + node_count]
        left_ids = child_ids[:, 0]
        right_ids = child_ids[:, 1]
        left_decay = jnp.exp(-rate_scale * length_row[left_ids])
        right_decay = jnp.exp(-rate_scale * length_row[right_ids])
        if tree_level == 0:
            left_part = from_codes(tip_block[left_ids], left_decay, stationary)
            right_part = from_codes(tip_block[right_ids], right_decay, stationary)
            scale_sum = jnp.zeros((node_count, 1, tip_block.shape[1]), jnp.float32)
        else:
            anchor = TAXA + TAXA - (TAXA >> (tree_level - 1))
            left_rows = (left_ids - anchor).astype(jnp.int32)
            right_rows = (right_ids - anchor).astype(jnp.int32)
            left_part = transit(values[left_rows], left_decay, stationary)
            right_part = transit(values[right_rows], right_decay, stationary)
            scale_sum = scales[left_rows] + scales[right_rows]
        values, scales = join_pair(left_part, right_part, scale_sum)
    return scales[0, 0] + jnp.log(jnp.sum(stationary[:, None] * values[0], axis=0))


def reference(tip_codes, counts, children, lengths, frequencies, weights):
    stationary = frequencies / jnp.sum(frequencies, axis=1, keepdims=True)
    log_weight = jnp.log(weights / jnp.sum(weights))
    block_count = SITES // SITE_DEV
    tip_blocks = tip_codes.reshape(TAXA, block_count, SITE_DEV).transpose(1, 0, 2)

    def one_block(tip_block):
        return jnp.stack([class_loglik(tip_block, children, lengths[class_no], stationary[class_no]) for class_no in range(CLS)])

    per_class = lax.map(one_block, tip_blocks)
    per_class = per_class.transpose(1, 0, 2).reshape(CLS, SITES)
    shifted = per_class + log_weight[:, None]
    largest = jnp.max(shifted, axis=0)
    site_total = largest + jnp.log(jnp.sum(jnp.exp(shifted - largest[None, :]), axis=0))
    posterior = jnp.exp(shifted - site_total[None, :])
    pattern_weight = counts.astype(jnp.float32)
    class_mass = jnp.sum(pattern_weight[None, :] * posterior, axis=1)
    all_count = jnp.sum(pattern_weight)
    new_weights = class_mass / all_count
    mean_loglik = jnp.sum(pattern_weight * site_total) / (all_count * TAXA)
    per_taxon = (site_total / TAXA).reshape(N_SITE, CLS, SITE_DEV // CLS).transpose(1, 0, 2).reshape(CLS, SITES // CLS)
    return per_taxon, new_weights, mean_loglik
```

```python
import jax
import jax.numpy as jnp
from jax import lax
from jax.experimental import pallas as pl
from jax.experimental.pallas import tpu as pltpu
from jax.sharding import PartitionSpec as P

CLS = 4
STATES = 4
PAD = 2048
SMEM = pltpu.MemorySpace.SMEM
VMEM = pltpu.MemorySpace.VMEM


def mean_state(pi, values):
    return (pi[0] * values[0] + pi[1] * values[1]) + (pi[2] * values[2] + pi[3] * values[3])


def moved(values, rate, average):
    step = rate * average
    return [value + step for value in values]


def product(left, right):
    return [a * b for a, b in zip(left, right)]


def lower_kernel(group_ref, child_ref, rate_ref, pi_ref, codes_ref, out_ref, mid_ref, log_ref):
    group = group_ref[0]
    pis = [[pi_ref[4 * c + i] for i in range(STATES)] for c in range(CLS)]

    def pair_of(row):
        return child_ref[2 * row], child_ref[2 * row + 1]

    def tip_codes(tip):
        local = tip - group * 256
        start = lax.shift_left(lax.shift_right_logical(local, 3), 6) + lax.bitwise_and(local, 7)
        return codes_ref[pl.ds(start, 8, stride=8), :]

    def tip_part(code, c, rate):
        pi = pis[c]
        odd = lax.bitwise_and(code, 1) == 1
        high = code >= 2
        freq = jnp.where(high, jnp.where(odd, pi[3], pi[2]), jnp.where(odd, pi[1], pi[0]))
        step = rate * freq
        own = step + 1.0
        return [jnp.where(code == i, own, step) for i in range(STATES)]

    def small_tree(n, _):
        row = 768 + group * 32 + n
        tops = pair_of(row)
        pairs = [pair for top in tops for pair in pair_of(top - 1024)]
        tips = [tip for pair in pairs for tip in pair_of(pair - 1024)]
        codes = [tip_codes(tip) for tip in tips]
        for c in range(CLS):
            pi = pis[c]

            def rate(node):
                return rate_ref[PAD * c + node]

            halves = []
            for h in range(2):
                quads = []
                for p in range(2):
                    at = 2 * h + p
                    joined = product(
                        tip_part(codes[2 * at], c, rate(tips[2 * at])),
                        tip_part(codes[2 * at + 1], c, rate(tips[2 * at + 1])),
                    )
                    quads.append(moved(joined, rate(pairs[at]), mean_state(pi, joined)))
                joined = product(quads[0], quads[1])
                halves.append(moved(joined, rate(tops[h]), mean_state(pi, joined)))
            joined = product(halves[0], halves[1])
            average = mean_state(pi, joined)
            inverse = 1.0 / average
            own_rate = rate(1024 + row)
            for i in range(STATES):
                mid_ref[n, c, i] = joined[i] * inverse + own_rate
            log_ref[n, c] = jnp.log(average)
        return 0

    lax.fori_loop(0, 32, small_tree, 0)

    def clade(j, _):
        root = 992 + group * 4 + j
        tops = pair_of(root)
        pairs = [pair for top in tops for pair in pair_of(top - 1024)]
        leaves = [leaf - 1792 - group * 32 for pair in pairs for leaf in pair_of(pair - 1024)]
        for c in range(CLS):
            pi = pis[c]

            def rate(node):
                return rate_ref[PAD * c + node]

            scale = log_ref[leaves[0], c]
            for leaf in leaves[1:]:
                scale = scale + log_ref[leaf, c]
            halves = []
            for h in range(2):
                quads = []
                for p in range(2):
                    at = 2 * h + p
                    joined = [
                        mid_ref[leaves[2 * at], c, i] * mid_ref[leaves[2 * at + 1], c, i]
                        for i in range(STATES)
                    ]
                    quads.append(moved(joined, rate(pairs[at]), mean_state(pi, joined)))
                joined = product(quads[0], quads[1])
                halves.append(moved(joined, rate(tops[h]), mean_state(pi, joined)))
            joined = product(halves[0], halves[1])
            inverse = 1.0 / joined[3]
            sent = [joined[0] * inverse, joined[1] * inverse, joined[2] * inverse]
            sent.append(scale + jnp.log(joined[3]))
            for v in range(4):
                for q in range(4):
                    out_ref[q, j, v, 2 * c : 2 * c + 2, :] = sent[v][2 * q : 2 * q + 2, :]
        return 0

    lax.fori_loop(0, 4, clade, 0)


def upper_kernel(
    group_ref, child_ref, clade_ref, rate_ref, pi_ref, const_ref, count_ref, site_ref, part_ref, node_ref
):
    pi = [pi_ref[i] for i in range(STATES)]
    scale = const_ref[...]
    for k in range(16):
        values = [clade_ref[k, 0], clade_ref[k, 1], clade_ref[k, 2]]
        scale = scale + clade_ref[k, 3]
        average = (pi[0] * values[0] + pi[1] * values[1]) + (pi[2] * values[2] + pi[3])
        step = rate_ref[k] * average
        for i in range(3):
            node_ref[k, i] = values[i] + step
        node_ref[k, 3] = step + 1.0
    at = 16
    for level, count in ((6, 8), (7, 4), (8, 2), (9, 1)):
        first = 1024 - (1024 >> level)
        for k in range(count):
            left = child_ref[2 * (first + k)] - 2016
            right = child_ref[2 * (first + k) + 1] - 2016
            joined = [node_ref[left, i] * node_ref[right, i] for i in range(STATES)]
            average = mean_state(pi, joined)
            if level == 6:
                scale = scale + jnp.log(average)
                inverse = 1.0 / average
                for i in range(STATES):
                    node_ref[at, i] = joined[i] * inverse + rate_ref[at]
            elif level < 9:
                step = rate_ref[at] * average
                for i in range(STATES):
                    node_ref[at, i] = joined[i] + step
            else:
                scale = scale + jnp.log(average)
            at += 1
    top = jnp.maximum(scale, pltpu.roll(scale, 2, 0))
    top = jnp.maximum(top, pltpu.roll(top, 4, 0))
    share = jnp.exp(scale - top)
    mass = share + pltpu.roll(share, 2, 0)
    mass = mass + pltpu.roll(mass, 4, 0)
    total = top + jnp.log(mass)
    site_ref[...] = total[0:2] * (1.0 / 1024.0)
    quarter = count_ref[pl.ds(2 * group_ref[0], 2), :].astype(jnp.float32)
    weight = jnp.concatenate([quarter, quarter, quarter, quarter], axis=0)
    classes = weight * (share / mass)
    row = lax.broadcasted_iota(jnp.int32, (8, 128), 0)
    column = lax.broadcasted_iota(jnp.int32, (1, 128), 1)
    sums = [jnp.sum(jnp.where(lax.shift_right_logical(row, 1) == c, classes, 0.0), keepdims=True) for c in range(CLS)]
    sums.append(jnp.sum(jnp.where(row < 2, weight * total, 0.0), keepdims=True))
    sums.append(jnp.sum(jnp.where(row < 2, weight, 0.0), keepdims=True))
    line = jnp.zeros((1, 128), jnp.float32)
    for k, value in enumerate(sums):
        line = jnp.where(column == k, value, line)
    part_ref[...] = line


def per_device(tip_codes, counts, children, lengths, frequencies, weights):
    group = lax.axis_index("cls").astype(jnp.int32)
    group_line = group.reshape(1)
    stationary = frequencies / jnp.sum(frequencies, axis=1, keepdims=True)
    beta = 1.0 / (1.0 - jnp.sum(stationary * stationary, axis=1))
    rates = jnp.exp(beta[:, None] * lengths) - 1.0
    log_weight = jnp.log(weights / jnp.sum(weights))
    const = log_weight - beta * jnp.sum(lengths, axis=1)
    child_line = children.reshape(-1)
    rate_line = jnp.pad(rates, ((0, 0), (0, PAD - rates.shape[1]))).reshape(-1)
    codes = tip_codes.reshape(32, 8, 8, 128).transpose(0, 2, 1, 3).reshape(2048, 128)

    smem = pl.BlockSpec(memory_space=SMEM)
    vmem = pl.BlockSpec(memory_space=VMEM)
    ours = pl.pallas_call(
        lower_kernel,
        out_shape=jax.ShapeDtypeStruct((4, 4, 4, 8, 128), jnp.float32),
        in_specs=[smem, smem, smem, smem, vmem],
        out_specs=vmem,
        scratch_shapes=[
            pltpu.VMEM((32, CLS, STATES, 8, 128), jnp.float32),
            pltpu.VMEM((32, CLS, 8, 128), jnp.float32),
        ],
        name="lower_tree",
    )(group_line, child_line, rate_line, stationary.reshape(-1), codes)
    clades = lax.all_to_all(ours, "cls", split_axis=0, concat_axis=0, tiled=True)

    def spread(by_class):
        return jnp.broadcast_to(by_class[..., :, None, None], (*by_class.shape, 2, 128)).reshape(
            *by_class.shape[:-1], 8, 128
        )

    top_rates = spread(jnp.pad(rates[:, 2016:], ((0, 0), (0, 2))).T)
    site, part = pl.pallas_call(
        upper_kernel,
        out_shape=(
            jax.ShapeDtypeStruct((2, 128), jnp.float32),
            jax.ShapeDtypeStruct((1, 128), jnp.float32),
        ),
        in_specs=[smem, smem, vmem, vmem, vmem, vmem, vmem],
        out_specs=(vmem, vmem),
        scratch_shapes=[pltpu.VMEM((32, STATES, 8, 128), jnp.float32)],
        name="upper_tree",
    )(
        group_line,
        child_line,
        clades.reshape(16, 4, 8, 128),
        top_rates,
        spread(stationary.T),
        spread(const),
        counts.reshape(8, 128),
    )
    every = lax.all_to_all(
        jnp.broadcast_to(part, (128, 128)), ("cls", "site"), split_axis=0, concat_axis=0, tiled=True
    )
    sums = jnp.sum(every, axis=0)
    own = lax.dynamic_slice_in_dim(sums, group, 1, 0)
    return site.reshape(1, 256), own / sums[5], sums[4] / (sums[5] * 1024.0)


def solution(mesh):
    return jax.shard_map(
        per_device,
        mesh=mesh,
        in_specs=(P("cls", "site"), P("site"), P(), P(), P(), P()),
        out_specs=(P("cls", "site"), P("cls"), P()),
        check_vma=False,
    )
```

```python
import jax
import jax.numpy as jnp
from jax import lax
from jax.experimental import pallas as pl
from jax.experimental.pallas import tpu as pltpu
from jax.sharding import PartitionSpec as P

CLS = 4
STATES = 4
FLOAT = jnp.float32
SMEM = pltpu.MemorySpace.SMEM
VMEM = pltpu.MemorySpace.VMEM
TILE = (8, 128)
TOP_RATES, TOP_PI, TOP_CONST, TOP_WEIGHT, TOP_ROWS = 0, 30, 34, 35, 36


def mean_state(pi, values):
    return (pi[0] * values[0] + pi[1] * values[1]) + (pi[2] * values[2] + pi[3] * values[3])


def moved(values, rate, average):
    step = rate * average
    return [value + step for value in values]


def product(left, right):
    return [a * b for a, b in zip(left, right)]


def choose(selector, options):
    value = jnp.where(selector == 1, options[1], options[0])
    value = jnp.where(selector == 2, options[2], value)
    return jnp.where(selector == 3, options[3], value)


def lower_kernel(
    child_ref, freq_ref, weight_ref, lengths_ref, codes_hbm, counts_hbm,
    out_ref, top_ref,
    codes_ref, counts_ref, rate_vec, rate_ref, pi_ref, pattern_ref, mid_ref, log_ref, sems,
):
    group = lax.axis_index("cls")
    loads = [
        pltpu.make_async_copy(
            codes_hbm.at[pl.ds(512 * j, 512)], codes_ref.at[pl.ds(512 * j, 512)], sems.at[j]
        )
        for j in range(4)
    ]
    for load in loads:
        load.start()
    count_load = pltpu.make_async_copy(counts_hbm, counts_ref, sems.at[5])
    count_load.start()

    lane = lax.broadcasted_iota(jnp.int32, TILE, 1)
    sub = lax.broadcasted_iota(jnp.int32, TILE, 0)
    by_pair = lax.shift_right_logical(sub, 1)
    uniform, betas = [], []
    for c in range(CLS):
        raw = [jnp.full(TILE, freq_ref[c, i], FLOAT) for i in range(STATES)]
        inverse = 1.0 / ((raw[0] + raw[1]) + (raw[2] + raw[3]))
        uniform.append([value * inverse for value in raw])
        betas.append(1.0 / (1.0 - mean_state(uniform[c], uniform[c])))
    beta_rows = choose(lax.bitwise_and(sub, 3), betas)[:4]
    total = jnp.zeros((4, 128), FLOAT)
    for k in range(16):
        width = min(128, 2046 - 128 * k)
        part = lengths_ref[:, 128 * k : 128 * k + width]
        if width < 128:
            part = jnp.concatenate([part, jnp.zeros((4, 128 - width), FLOAT)], axis=1)
        total = total + part
        rate_vec[:, 128 * k : 128 * k + 128] = jnp.exp(beta_rows * part) - 1.0
    rate_load = pltpu.make_async_copy(rate_vec, rate_ref, sems.at[4])
    rate_load.start()

    own_state = lax.bitwise_and(lax.shift_right_logical(lane, 4), 3)
    left_code = lax.bitwise_and(lax.shift_right_logical(lane, 2), 3)
    right_code = lax.bitwise_and(lane, 3)
    left_own = own_state == left_code
    right_own = own_state == right_code
    first = lane < 64
    both_own = jnp.where(left_own, jnp.where(right_own, 1.0, 0.0), 0.0)
    for c in range(CLS):
        left_pi = choose(left_code, uniform[c])
        right_pi = choose(right_code, uniform[c])
        pattern_ref[c, 0] = jnp.where(left_own, right_pi, 0.0)
        pattern_ref[c, 1] = jnp.where(right_own, left_pi, 0.0)
        pattern_ref[c, 2] = left_pi * right_pi
        pattern_ref[c, 3] = jnp.where(left_code == right_code, left_pi, 0.0)
        for i in range(STATES):
            pi_ref[c, i] = uniform[c][i]

    for i in range(STATES):
        top_ref[TOP_PI + i] = choose(by_pair, [uniform[c][i] for c in range(CLS)])
    beta_pairs = choose(by_pair, betas)
    sums = choose(by_pair, [jnp.broadcast_to(total[c : c + 1], TILE) for c in range(CLS)])
    sums = jnp.broadcast_to(jnp.sum(sums, axis=1, keepdims=True), TILE)
    weights = [jnp.full(TILE, weight_ref[c], FLOAT) for c in range(CLS)]
    weight_sum = (weights[0] + weights[1]) + (weights[2] + weights[3])
    top_ref[TOP_CONST] = jnp.log(choose(by_pair, weights) / weight_sum) - beta_pairs * sums
    last = lengths_ref[:, 1920:2046]
    last = jnp.concatenate([last, jnp.zeros((4, 2), FLOAT)], axis=1)
    last = choose(by_pair, [jnp.broadcast_to(last[c : c + 1], TILE) for c in range(CLS)])
    last = jnp.exp(beta_pairs * last) - 1.0
    for k in range(30):
        top_ref[TOP_RATES + k] = jnp.broadcast_to(last[:, 96 + k : 97 + k], TILE)
    count_load.wait()
    quarter = counts_ref[pl.ds(2 * group, 2), :].astype(FLOAT)
    top_ref[TOP_WEIGHT] = jnp.concatenate([quarter, quarter, quarter, quarter], axis=0)
    rate_load.wait()

    def pair_of(row):
        return child_ref[0, row], child_ref[1, row]

    def tip_codes(tip):
        local = tip - group * 256
        start = lax.shift_left(lax.shift_right_logical(local, 3), 6) + lax.bitwise_and(local, 7)
        return codes_ref[pl.ds(start, 8, stride=8), :]

    def small_tree(n, _):
        row = 768 + group * 32 + n
        tops = pair_of(row)
        pairs = [pair for top in tops for pair in pair_of(top - 1024)]
        tips = [pair_of(pair - 1024) for pair in pairs]
        places = []
        for at in range(4):
            code = lax.shift_left(tip_codes(tips[at][0]), 2) + tip_codes(tips[at][1])
            places.append([code + (64 * (at % 2) + 16 * i) for i in range(STATES)])
        for c in range(CLS):
            pi = [pi_ref[c, i] for i in range(STATES)]
            halves = []
            for h in range(2):
                factors = []
                for at in (2 * h, 2 * h + 1):
                    left = rate_ref[c, tips[at][0]]
                    right = rate_ref[c, tips[at][1]]
                    own = rate_ref[c, pairs[at]]
                    both = left * right
                    factors.append((right, left, both + own * (left + right + both), own))
                table = both_own
                for k in range(4):
                    factor = jnp.where(first, factors[0][k], factors[1][k])
                    table = table + factor * pattern_ref[c, k]
                quads = [
                    [
                        jnp.take_along_axis(table, places[at][i], axis=1, mode="promise_in_bounds")
                        for i in range(STATES)
                    ]
                    for at in (2 * h, 2 * h + 1)
                ]
                joined = product(quads[0], quads[1])
                halves.append(moved(joined, rate_ref[c, tops[h]], mean_state(pi, joined)))
            joined = product(halves[0], halves[1])
            average = mean_state(pi, joined)
            inverse = 1.0 / average
            own_rate = rate_ref[c, 1024 + row]
            for i in range(STATES):
                mid_ref[n, c, i] = joined[i] * inverse + own_rate
            log_ref[n, c] = jnp.log(average)
        return 0

    def clade(j):
        root = 992 + group * 4 + j
        tops = pair_of(root)
        pairs = [pair for top in tops for pair in pair_of(top - 1024)]
        leaves = [leaf - 1792 - group * 32 for pair in pairs for leaf in pair_of(pair - 1024)]
        for c in range(CLS):
            pi = [pi_ref[c, i] for i in range(STATES)]
            scale = log_ref[leaves[0], c]
            for leaf in leaves[1:]:
                scale = scale + log_ref[leaf, c]
            halves = []
            for h in range(2):
                quads = []
                for at in (2 * h, 2 * h + 1):
                    joined = [
                        mid_ref[leaves[2 * at], c, i] * mid_ref[leaves[2 * at + 1], c, i]
                        for i in range(STATES)
                    ]
                    quads.append(moved(joined, rate_ref[c, pairs[at]], mean_state(pi, joined)))
                joined = product(quads[0], quads[1])
                halves.append(moved(joined, rate_ref[c, tops[h]], mean_state(pi, joined)))
            joined = product(halves[0], halves[1])
            inverse = 1.0 / joined[3]
            sent = [joined[0] * inverse, joined[1] * inverse, joined[2] * inverse]
            sent.append(scale + jnp.log(joined[3]))
            for v in range(4):
                for q in range(4):
                    out_ref[q, j, v, 2 * c : 2 * c + 2, :] = sent[v][2 * q : 2 * q + 2, :]

    for j in range(4):
        loads[j].wait()
        lax.fori_loop(8 * j, 8 * j + 8, small_tree, 0)

    def one_clade(j, _):
        clade(j)
        return 0

    lax.fori_loop(0, 4, one_clade, 0)


def upper_kernel(child_ref, clade_ref, top_ref, site_ref, part_ref, node_ref):
    pi = [top_ref[TOP_PI + i] for i in range(STATES)]
    scale = top_ref[TOP_CONST]
    for k in range(16):
        values = [clade_ref[k, 0], clade_ref[k, 1], clade_ref[k, 2]]
        scale = scale + clade_ref[k, 3]
        average = (pi[0] * values[0] + pi[1] * values[1]) + (pi[2] * values[2] + pi[3])
        step = top_ref[TOP_RATES + k] * average
        for i in range(3):
            node_ref[k, i] = values[i] + step
        node_ref[k, 3] = step + 1.0
    at = 16
    for level, count in ((6, 8), (7, 4), (8, 2), (9, 1)):
        begin = 1024 - (1024 >> level)
        for k in range(count):
            left = child_ref[0, begin + k] - 2016
            right = child_ref[1, begin + k] - 2016
            joined = [node_ref[left, i] * node_ref[right, i] for i in range(STATES)]
            average = mean_state(pi, joined)
            if level == 6:
                scale = scale + jnp.log(average)
                inverse = 1.0 / average
                for i in range(STATES):
                    node_ref[at, i] = joined[i] * inverse + top_ref[TOP_RATES + at]
            elif level < 9:
                step = top_ref[TOP_RATES + at] * average
                for i in range(STATES):
                    node_ref[at, i] = joined[i] + step
            else:
                scale = scale + jnp.log(average)
            at += 1
    top = jnp.maximum(scale, pltpu.roll(scale, 2, 0))
    top = jnp.maximum(top, pltpu.roll(top, 4, 0))
    share = jnp.exp(scale - top)
    mass = share + pltpu.roll(share, 2, 0)
    mass = mass + pltpu.roll(mass, 4, 0)
    total = top + jnp.log(mass)
    site_ref[...] = total[0:2] * (1.0 / 1024.0)
    weight = top_ref[TOP_WEIGHT]
    classes = weight * (share / mass)
    row = lax.broadcasted_iota(jnp.int32, TILE, 0)
    column = lax.broadcasted_iota(jnp.int32, TILE, 1)
    by_row = [
        jnp.sum(values, axis=1, keepdims=True) for values in (classes, weight * total, weight)
    ]
    by_pair = lax.shift_right_logical(row, 1)
    line = jnp.where(by_pair == column, by_row[0], 0.0)
    line = jnp.where((column == 4) & (row < 2), by_row[1], line)
    line = jnp.where((column == 5) & (row < 2), by_row[2], line)
    line = jnp.sum(line, axis=0, keepdims=True)
    for k in range(16):
        part_ref[8 * k : 8 * k + 8, :] = jnp.broadcast_to(line, TILE)


def last_kernel(every_ref, own_ref, mean_ref):
    group = lax.axis_index("cls")
    sums = every_ref[0:8, :]
    for k in range(1, 16):
        sums = sums + every_ref[8 * k : 8 * k + 8, :]
    sums = jnp.sum(sums, axis=0, keepdims=True)
    column = lax.broadcasted_iota(jnp.int32, (1, 128), 1)

    def entry(at):
        return jnp.sum(jnp.where(column == at, sums, 0.0), axis=1, keepdims=True)

    count = entry(5)
    own_ref[...] = entry(group) / count
    mean_ref[...] = entry(4) / (count * 1024.0)


def per_device(tip_codes, counts, children, lengths, frequencies, weights):
    codes = tip_codes.reshape(32, 8, 8, 128).transpose(0, 2, 1, 3).reshape(2048, 128)
    child_rows = children.T
    smem = pl.BlockSpec(memory_space=SMEM)
    vmem = pl.BlockSpec(memory_space=VMEM)
    anywhere = pl.BlockSpec(memory_space=pl.ANY)
    ours, top = pl.pallas_call(
        lower_kernel,
        out_shape=(pltpu.VMEM((4, 4, 4, 8, 128), FLOAT), pltpu.VMEM((TOP_ROWS, 8, 128), FLOAT)),
        in_specs=[smem, smem, smem, vmem, anywhere, anywhere],
        out_specs=(vmem, vmem),
        scratch_shapes=[
            pltpu.VMEM((2048, 128), jnp.int32),
            pltpu.VMEM(TILE, jnp.int32),
            pltpu.VMEM((4, 2048), FLOAT),
            pltpu.SMEM((4, 2048), FLOAT),
            pltpu.VMEM((CLS, STATES, 8, 128), FLOAT),
            pltpu.VMEM((CLS, 4, 8, 128), FLOAT),
            pltpu.VMEM((32, CLS, STATES, 8, 128), FLOAT),
            pltpu.VMEM((32, CLS, 8, 128), FLOAT),
            pltpu.SemaphoreType.DMA((6,)),
        ],
        compiler_params=pltpu.CompilerParams(vmem_limit_bytes=16 * 1024 * 1024),
        name="lower_tree",
    )(child_rows, frequencies, weights, lengths, codes, counts.reshape(8, 128))
    clades = lax.all_to_all(ours, "cls", split_axis=0, concat_axis=0, tiled=True)
    site, part = pl.pallas_call(
        upper_kernel,
        out_shape=(jax.ShapeDtypeStruct((2, 128), FLOAT), pltpu.VMEM((128, 128), FLOAT)),
        in_specs=[smem, vmem, vmem],
        out_specs=(vmem, vmem),
        scratch_shapes=[pltpu.VMEM((32, STATES, 8, 128), FLOAT)],
        compiler_params=pltpu.CompilerParams(vmem_limit_bytes=16 * 1024 * 1024),
        name="upper_tree",
    )(child_rows, clades.reshape(16, 4, 8, 128), top)
    every = lax.all_to_all(part, ("cls", "site"), split_axis=0, concat_axis=0, tiled=True)
    own, mean = pl.pallas_call(
        last_kernel,
        out_shape=(jax.ShapeDtypeStruct((1, 1), FLOAT), jax.ShapeDtypeStruct((1, 1), FLOAT)),
        in_specs=[vmem],
        out_specs=(vmem, vmem),
        compiler_params=pltpu.CompilerParams(vmem_limit_bytes=16 * 1024 * 1024),
        name="last_sums",
    )(every)
    return site.reshape(1, 256), own.reshape(1), mean.reshape(())


def solution(mesh):
    return jax.shard_map(
        per_device,
        mesh=mesh,
        in_specs=(P("cls", "site"), P("site"), P(), P(), P(), P()),
        out_specs=(P("cls", "site"), P("cls"), P()),
        check_vma=False,
    )
```

```python
import jax
import jax.numpy as jnp
from jax import lax
from jax.experimental import pallas as pl
from jax.experimental.pallas import tpu as pltpu
from jax.sharding import PartitionSpec as P

CLS = 4
STATES = 4
FLOAT = jnp.float32
SMEM = pltpu.MemorySpace.SMEM
VMEM = pltpu.MemorySpace.VMEM
TILE = (8, 128)
BUILD = 8
TREES = 2
TOP_RATES, TOP_PI, TOP_CONST, TOP_WEIGHT, TOP_ROWS = 0, 30, 34, 35, 36


def mean_state(pi, values):
    return (pi[0] * values[0] + pi[1] * values[1]) + (pi[2] * values[2] + pi[3] * values[3])


def moved(values, rate, average):
    step = rate * average
    return [value + step for value in values]


def product(left, right):
    return [a * b for a, b in zip(left, right)]


def choose(selector, options):
    value = jnp.where(selector == 1, options[1], options[0])
    value = jnp.where(selector == 2, options[2], value)
    return jnp.where(selector == 3, options[3], value)


def lanes_of(rows, places):
    return jnp.take_along_axis(rows, places, axis=1, mode="promise_in_bounds")


def lower_kernel(
    child_hbm, freq_hbm, weight_hbm, lengths_hbm, codes_hbm, counts_hbm,
    out_ref, top_ref,
    child_vec, freq_ref, weight_ref, lengths_ref, codes_ref, counts_ref, rate_vec,
    spot_vec, spot_ref, step_vec, step_ref,
    pi_ref, pattern_ref, factor_ref, table_ref, mid_ref, log_ref, sems,
):
    group = lax.axis_index("cls")
    small = [
        pltpu.make_async_copy(source, target, sems.at[4 + k])
        for k, (source, target) in enumerate(
            (
                (freq_hbm, freq_ref),
                (weight_hbm, weight_ref),
                (lengths_hbm, lengths_ref),
                (child_hbm, child_vec),
                (counts_hbm, counts_ref),
            )
        )
    ]
    for load in small:
        load.start()
    loads = [
        pltpu.make_async_copy(
            codes_hbm.at[pl.ds(512 * j, 512)], codes_ref.at[pl.ds(512 * j, 512)], sems.at[j]
        )
        for j in range(4)
    ]
    for load in loads:
        load.start()
    for load in small:
        load.wait()

    lane = lax.broadcasted_iota(jnp.int32, TILE, 1)
    sub = lax.broadcasted_iota(jnp.int32, TILE, 0)
    by_pair = lax.shift_right_logical(sub, 1)
    by_class = lax.bitwise_and(sub, 3)
    uniform, betas = [], []
    for c in range(CLS):
        raw = [jnp.full(TILE, freq_ref[c, i], FLOAT) for i in range(STATES)]
        inverse = 1.0 / ((raw[0] + raw[1]) + (raw[2] + raw[3]))
        uniform.append([value * inverse for value in raw])
        betas.append(1.0 / (1.0 - mean_state(uniform[c], uniform[c])))
        for i in range(STATES):
            pi_ref[c, i] = uniform[c][i]
    beta_rows = choose(by_class, betas)[:4]
    total = jnp.zeros((4, 128), FLOAT)
    for k in range(16):
        width = min(128, 2046 - 128 * k)
        part = lengths_ref[:, 128 * k : 128 * k + width]
        if width < 128:
            part = jnp.concatenate([part, jnp.zeros((4, 128 - width), FLOAT)], axis=1)
        total = total + part
        rate_vec[:, 128 * k : 128 * k + 128] = jnp.exp(beta_rows * part) - 1.0

    half = lax.shift_right_logical(group, 1)

    def block(ref, start):
        return ref[:, pl.ds(pl.multiple_of(start, 128), 128)]

    local = block(child_vec, 128 * group) - 256 * group
    spot_vec[0:2] = lax.shift_left(lax.shift_right_logical(local, 3), 6) + lax.bitwise_and(local, 7)
    spot_vec[2:4] = block(child_vec, 512 + 128 * half) - (1024 + 128 * group)
    spot_vec[4:6] = child_vec[:, 768:896] - (1536 + 128 * half)
    spot_vec[6:8] = jnp.concatenate([child_vec[:, 896:1023], jnp.zeros((2, 1), jnp.int32)], axis=1)
    spot_copy = pltpu.make_async_copy(spot_vec, spot_ref, sems.at[9])
    spot_copy.start()
    step_vec[0:4] = block(rate_vec, 1536 + 128 * half)
    step_vec[4:8] = rate_vec[:, 1792:1920]
    step_vec[8:12] = rate_vec[:, 1920:2048]
    step_vec[12:16] = jnp.zeros((4, 128), FLOAT)
    step_copy = pltpu.make_async_copy(step_vec, step_ref, sems.at[10])
    step_copy.start()

    def twice(rows):
        return jnp.concatenate([rows, rows], axis=0)

    low = twice(block(rate_vec, 256 * group))
    high = twice(block(rate_vec, 256 * group + 128))
    own = twice(block(rate_vec, 1024 + 128 * group))

    def rates_at(places):
        places = jnp.broadcast_to(places, TILE)
        inside = lax.bitwise_and(places, 127)
        return jnp.where(places < 128, lanes_of(low, inside), lanes_of(high, inside))

    left = rates_at(local[0:1])
    right = rates_at(local[1:2])
    both = left * right
    factor_ref[0] = right
    factor_ref[1] = left
    factor_ref[2] = both + own * (left + right + both)
    factor_ref[3] = own

    own_state = lax.bitwise_and(lax.shift_right_logical(lane, 4), 3)
    left_code = lax.bitwise_and(lax.shift_right_logical(lane, 2), 3)
    right_code = lax.bitwise_and(lane, 3)
    left_own = own_state == left_code
    right_own = own_state == right_code
    first = lane < 64
    both_own = jnp.where(left_own, jnp.where(right_own, 1.0, 0.0), 0.0)
    by_rows = [choose(by_class, [uniform[c][i] for c in range(CLS)]) for i in range(STATES)]
    left_pi = choose(left_code, by_rows)
    right_pi = choose(right_code, by_rows)
    pattern_ref[0] = jnp.where(left_own, right_pi, 0.0)
    pattern_ref[1] = jnp.where(right_own, left_pi, 0.0)
    pattern_ref[2] = left_pi * right_pi
    pattern_ref[3] = jnp.where(left_code == right_code, left_pi, 0.0)

    for i in range(STATES):
        top_ref[TOP_PI + i] = choose(by_pair, [uniform[c][i] for c in range(CLS)])
    beta_pairs = choose(by_pair, betas)
    sums = choose(by_pair, [jnp.broadcast_to(total[c : c + 1], TILE) for c in range(CLS)])
    sums = jnp.broadcast_to(jnp.sum(sums, axis=1, keepdims=True), TILE)
    weights = [jnp.full(TILE, weight_ref[c], FLOAT) for c in range(CLS)]
    weight_sum = (weights[0] + weights[1]) + (weights[2] + weights[3])
    top_ref[TOP_CONST] = jnp.log(choose(by_pair, weights) / weight_sum) - beta_pairs * sums
    last = rate_vec[:, 1920:2048]
    last = choose(by_pair, [jnp.broadcast_to(last[c : c + 1], TILE) for c in range(CLS)])
    for k in range(30):
        top_ref[TOP_RATES + k] = jnp.broadcast_to(last[:, 96 + k : 97 + k], TILE)
    quarter = counts_ref[pl.ds(2 * group, 2), :].astype(FLOAT)
    top_ref[TOP_WEIGHT] = jnp.concatenate([quarter, quarter, quarter, quarter], axis=0)
    spot_copy.wait()
    step_copy.wait()

    def pairs_of(n):
        tops = [spot_ref[4 + side, 32 * group + n] for side in range(2)]
        return tops, [spot_ref[2 + side, top] for top in tops for side in range(2)]

    upper_half = sub < 4

    def build_table(n):
        _, pairs = pairs_of(n)
        places = jnp.where(
            upper_half,
            jnp.where(first, pairs[0], pairs[1]),
            jnp.where(first, pairs[2], pairs[3]),
        )
        table = both_own
        for k in range(4):
            table = table + lanes_of(factor_ref[k], places) * pattern_ref[k]
        table_ref[n] = table

    def build_tables(m, _):
        for u in range(BUILD):
            build_table(BUILD * m + u)
        return 0

    lax.fori_loop(0, 32 // BUILD, build_tables, 0)

    def small_tree(n):
        tops, pairs = pairs_of(n)
        joined = []
        for h in range(2):
            tables = [
                jnp.broadcast_to(table_ref[n, 4 * h + c : 4 * h + c + 1, :], TILE) for c in range(CLS)
            ]
            quads = []
            for p in range(2):
                pair = pairs[2 * h + p]
                codes = [codes_ref[pl.ds(spot_ref[side, pair], 8, stride=8), :] for side in range(2)]
                code = lax.shift_left(codes[0], 2) + codes[1]
                found = []
                for i in range(STATES):
                    place = code + (64 * p + 16 * i)
                    found.append([lanes_of(tables[c], place) for c in range(CLS)])
                quads.append(found)
            halves = []
            for c in range(CLS):
                pi = [pi_ref[c, i] for i in range(STATES)]
                values = [quads[0][i][c] * quads[1][i][c] for i in range(STATES)]
                halves.append(moved(values, step_ref[c, tops[h]], mean_state(pi, values)))
            joined.append(halves)
        for c in range(CLS):
            pi = [pi_ref[c, i] for i in range(STATES)]
            values = product(joined[0][c], joined[1][c])
            average = mean_state(pi, values)
            inverse = 1.0 / average
            own_rate = step_ref[4 + c, 32 * group + n]
            for i in range(STATES):
                mid_ref[n, c, i] = values[i] * inverse + own_rate
            log_ref[n, c] = jnp.log(average)

    def small_trees(m, _):
        for u in range(TREES):
            small_tree(TREES * m + u)
        return 0

    def tail_pair(at):
        return [spot_ref[6 + side, at] for side in range(2)]

    def clade(j, _):
        tops = [top - 1920 for top in tail_pair(96 + 4 * group + j)]
        pairs = [pair - 1920 for top in tops for pair in tail_pair(top)]
        leaves = [leaf - 1792 - group * 32 for pair in pairs for leaf in tail_pair(pair)]
        for c in range(CLS):
            pi = [pi_ref[c, i] for i in range(STATES)]
            scale = log_ref[leaves[0], c]
            for leaf in leaves[1:]:
                scale = scale + log_ref[leaf, c]
            halves = []
            for h in range(2):
                quads = []
                for at in (2 * h, 2 * h + 1):
                    joined = [
                        mid_ref[leaves[2 * at], c, i] * mid_ref[leaves[2 * at + 1], c, i]
                        for i in range(STATES)
                    ]
                    quads.append(moved(joined, step_ref[8 + c, pairs[at]], mean_state(pi, joined)))
                joined = product(quads[0], quads[1])
                halves.append(moved(joined, step_ref[8 + c, tops[h]], mean_state(pi, joined)))
            joined = product(halves[0], halves[1])
            inverse = 1.0 / joined[3]
            sent = [joined[0] * inverse, joined[1] * inverse, joined[2] * inverse]
            sent.append(scale + jnp.log(joined[3]))
            for v in range(4):
                for q in range(4):
                    out_ref[q, j, v, 2 * c : 2 * c + 2, :] = sent[v][2 * q : 2 * q + 2, :]
        return 0

    for load in loads:
        load.wait()
    lax.fori_loop(0, 32 // TREES, small_trees, 0)
    lax.fori_loop(0, 4, clade, 0)


def upper_kernel(child_ref, clade_ref, top_ref, site_ref, part_ref, node_ref):
    pi = [top_ref[TOP_PI + i] for i in range(STATES)]
    scale = top_ref[TOP_CONST]
    for k in range(16):
        values = [clade_ref[k, 0], clade_ref[k, 1], clade_ref[k, 2]]
        scale = scale + clade_ref[k, 3]
        average = (pi[0] * values[0] + pi[1] * values[1]) + (pi[2] * values[2] + pi[3])
        step = top_ref[TOP_RATES + k] * average
        for i in range(3):
            node_ref[k, i] = values[i] + step
        node_ref[k, 3] = step + 1.0
    at = 16
    for level, count in ((6, 8), (7, 4), (8, 2), (9, 1)):
        begin = 1024 - (1024 >> level)
        for k in range(count):
            left = child_ref[0, begin + k] - 2016
            right = child_ref[1, begin + k] - 2016
            joined = [node_ref[left, i] * node_ref[right, i] for i in range(STATES)]
            average = mean_state(pi, joined)
            if level == 6:
                scale = scale + jnp.log(average)
                inverse = 1.0 / average
                for i in range(STATES):
                    node_ref[at, i] = joined[i] * inverse + top_ref[TOP_RATES + at]
            elif level < 9:
                step = top_ref[TOP_RATES + at] * average
                for i in range(STATES):
                    node_ref[at, i] = joined[i] + step
            else:
                scale = scale + jnp.log(average)
            at += 1
    top = jnp.maximum(scale, pltpu.roll(scale, 2, 0))
    top = jnp.maximum(top, pltpu.roll(top, 4, 0))
    share = jnp.exp(scale - top)
    mass = share + pltpu.roll(share, 2, 0)
    mass = mass + pltpu.roll(mass, 4, 0)
    total = top + jnp.log(mass)
    site_ref[...] = total[0:2] * (1.0 / 1024.0)
    weight = top_ref[TOP_WEIGHT]
    classes = weight * (share / mass)
    row = lax.broadcasted_iota(jnp.int32, TILE, 0)
    column = lax.broadcasted_iota(jnp.int32, TILE, 1)
    by_row = [
        jnp.sum(values, axis=1, keepdims=True) for values in (classes, weight * total, weight)
    ]
    by_pair = lax.shift_right_logical(row, 1)
    line = jnp.where(by_pair == column, by_row[0], 0.0)
    line = jnp.where((column == 4) & (row < 2), by_row[1], line)
    line = jnp.where((column == 5) & (row < 2), by_row[2], line)
    line = jnp.sum(line, axis=0, keepdims=True)
    for k in range(16):
        part_ref[8 * k : 8 * k + 8, :] = jnp.broadcast_to(line, TILE)


def last_kernel(every_ref, own_ref, mean_ref):
    group = lax.axis_index("cls")
    sums = every_ref[0:8, :]
    for k in range(1, 16):
        sums = sums + every_ref[8 * k : 8 * k + 8, :]
    sums = jnp.sum(sums, axis=0, keepdims=True)
    column = lax.broadcasted_iota(jnp.int32, (1, 128), 1)

    def entry(at):
        return jnp.sum(jnp.where(column == at, sums, 0.0), axis=1, keepdims=True)

    count = entry(5)
    own_ref[...] = entry(group) / count
    mean_ref[...] = entry(4) / (count * 1024.0)


def per_device(tip_codes, counts, children, lengths, frequencies, weights):
    codes = tip_codes.reshape(32, 8, 8, 128).transpose(0, 2, 1, 3).reshape(2048, 128)
    child_rows = children.T
    smem = pl.BlockSpec(memory_space=SMEM)
    vmem = pl.BlockSpec(memory_space=VMEM)
    hbm = pl.BlockSpec(memory_space=pltpu.MemorySpace.HBM)
    ours, top = pl.pallas_call(
        lower_kernel,
        out_shape=(pltpu.VMEM((4, 4, 4, 8, 128), FLOAT), pltpu.VMEM((TOP_ROWS, 8, 128), FLOAT)),
        in_specs=[hbm] * 6,
        out_specs=(vmem, vmem),
        scratch_shapes=[
            pltpu.VMEM((2, 1023), jnp.int32),
            pltpu.SMEM((4, 4), FLOAT),
            pltpu.SMEM((4,), FLOAT),
            pltpu.VMEM((4, 2046), FLOAT),
            pltpu.VMEM((2048, 128), jnp.int32),
            pltpu.VMEM(TILE, jnp.int32),
            pltpu.VMEM((4, 2048), FLOAT),
            pltpu.VMEM(TILE, jnp.int32),
            pltpu.SMEM(TILE, jnp.int32),
            pltpu.VMEM((16, 128), FLOAT),
            pltpu.SMEM((16, 128), FLOAT),
            pltpu.VMEM((CLS, STATES, 8, 128), FLOAT),
            pltpu.VMEM((4, 8, 128), FLOAT),
            pltpu.VMEM((4, 8, 128), FLOAT),
            pltpu.VMEM((32, 8, 128), FLOAT),
            pltpu.VMEM((32, CLS, STATES, 8, 128), FLOAT),
            pltpu.VMEM((32, CLS, 8, 128), FLOAT),
            pltpu.SemaphoreType.DMA((11,)),
        ],
        compiler_params=pltpu.CompilerParams(vmem_limit_bytes=16 * 1024 * 1024),
        name="lower_tree",
    )(child_rows, frequencies, weights, lengths, codes, counts.reshape(8, 128))
    clades = lax.all_to_all(ours, "cls", split_axis=0, concat_axis=0, tiled=True)
    site, part = pl.pallas_call(
        upper_kernel,
        out_shape=(jax.ShapeDtypeStruct((2, 128), FLOAT), pltpu.VMEM((128, 128), FLOAT)),
        in_specs=[smem, vmem, vmem],
        out_specs=(vmem, vmem),
        scratch_shapes=[pltpu.VMEM((32, STATES, 8, 128), FLOAT)],
        compiler_params=pltpu.CompilerParams(vmem_limit_bytes=16 * 1024 * 1024),
        name="upper_tree",
    )(child_rows, clades.reshape(16, 4, 8, 128), top)
    every = lax.all_to_all(part, ("cls", "site"), split_axis=0, concat_axis=0, tiled=True)
    own, mean = pl.pallas_call(
        last_kernel,
        out_shape=(jax.ShapeDtypeStruct((1, 1), FLOAT), jax.ShapeDtypeStruct((1, 1), FLOAT)),
        in_specs=[vmem],
        out_specs=(vmem, vmem),
        compiler_params=pltpu.CompilerParams(vmem_limit_bytes=16 * 1024 * 1024),
        name="last_sums",
    )(every)
    return site.reshape(1, 256), own.reshape(1), mean.reshape(())


def solution(mesh):
    return jax.shard_map(
        per_device,
        mesh=mesh,
        in_specs=(P("cls", "site"), P("site"), P(), P(), P(), P()),
        out_specs=(P("cls", "site"), P("cls"), P()),
        check_vma=False,
    )
```

```python
import jax
import jax.numpy as jnp
from jax import lax
from jax.experimental import pallas as pl
from jax.experimental.pallas import tpu as pltpu
from jax.sharding import PartitionSpec as P

CLS = 4
STATES = 4
FLOAT = jnp.float32
SMEM = pltpu.MemorySpace.SMEM
VMEM = pltpu.MemorySpace.VMEM
TILE = (8, 128)
BUILD = 8
TREES = 2
TOP_RATES, TOP_PI, TOP_CONST, TOP_WEIGHT, TOP_ROWS = 0, 30, 34, 35, 36


def mean_state(pi, values):
    return (pi[0] * values[0] + pi[1] * values[1]) + (pi[2] * values[2] + pi[3] * values[3])


def moved(values, rate, average):
    step = rate * average
    return [value + step for value in values]


def product(left, right):
    return [a * b for a, b in zip(left, right)]


def choose(selector, options):
    value = jnp.where(selector == 1, options[1], options[0])
    value = jnp.where(selector == 2, options[2], value)
    return jnp.where(selector == 3, options[3], value)


def lanes_of(rows, places):
    return jnp.take_along_axis(rows, places, axis=1, mode="promise_in_bounds")


def lower_kernel(
    child_hbm, freq_hbm, weight_hbm, lengths_hbm, codes_hbm, counts_hbm,
    out_ref, top_ref,
    child_vec, freq_ref, weight_ref, lengths_ref, codes_ref, counts_ref, rate_vec,
    spot_vec, spot_ref, step_vec, step_ref,
    pi_ref, pattern_ref, factor_ref, table_ref, mid_ref, log_ref, sems,
):
    group = lax.axis_index("cls")
    small = [
        pltpu.make_async_copy(source, target, sems.at[4 + k])
        for k, (source, target) in enumerate(
            (
                (freq_hbm, freq_ref),
                (weight_hbm, weight_ref),
                (lengths_hbm, lengths_ref),
                (child_hbm, child_vec),
                (counts_hbm, counts_ref),
            )
        )
    ]
    for load in small:
        load.start()
    loads = [
        pltpu.make_async_copy(
            codes_hbm.at[pl.ds(512 * j, 512)], codes_ref.at[pl.ds(512 * j, 512)], sems.at[j]
        )
        for j in range(4)
    ]
    for load in loads:
        load.start()
    for load in small:
        load.wait()

    lane = lax.broadcasted_iota(jnp.int32, TILE, 1)
    sub = lax.broadcasted_iota(jnp.int32, TILE, 0)
    by_pair = lax.shift_right_logical(sub, 1)
    by_class = lax.bitwise_and(sub, 3)
    uniform, betas = [], []
    for c in range(CLS):
        raw = [jnp.full(TILE, freq_ref[c, i], FLOAT) for i in range(STATES)]
        inverse = 1.0 / ((raw[0] + raw[1]) + (raw[2] + raw[3]))
        uniform.append([value * inverse for value in raw])
        betas.append(1.0 / (1.0 - mean_state(uniform[c], uniform[c])))
        for i in range(STATES):
            pi_ref[c, i] = uniform[c][i]
    beta_rows = choose(by_class, betas)[:4]
    total = jnp.zeros((4, 128), FLOAT)
    for k in range(16):
        width = min(128, 2046 - 128 * k)
        part = lengths_ref[:, 128 * k : 128 * k + width]
        if width < 128:
            part = jnp.concatenate([part, jnp.zeros((4, 128 - width), FLOAT)], axis=1)
        total = total + part
        rate_vec[:, 128 * k : 128 * k + 128] = jnp.exp(beta_rows * part) - 1.0

    half = lax.shift_right_logical(group, 1)

    def block(ref, start):
        return ref[:, pl.ds(pl.multiple_of(start, 128), 128)]

    local = block(child_vec, 128 * group) - 256 * group
    spot_vec[0:2] = lax.shift_left(lax.shift_right_logical(local, 3), 6) + lax.bitwise_and(local, 7)
    spot_vec[2:4] = block(child_vec, 512 + 128 * half) - (1024 + 128 * group)
    spot_vec[4:6] = child_vec[:, 768:896] - (1536 + 128 * half)
    spot_vec[6:8] = jnp.concatenate([child_vec[:, 896:1023], jnp.zeros((2, 1), jnp.int32)], axis=1)
    spot_copy = pltpu.make_async_copy(spot_vec, spot_ref, sems.at[9])
    spot_copy.start()
    step_vec[0:4] = block(rate_vec, 1536 + 128 * half)
    step_vec[4:8] = rate_vec[:, 1792:1920]
    step_vec[8:12] = rate_vec[:, 1920:2048]
    step_vec[12:16] = jnp.zeros((4, 128), FLOAT)
    step_copy = pltpu.make_async_copy(step_vec, step_ref, sems.at[10])
    step_copy.start()

    def twice(rows):
        return jnp.concatenate([rows, rows], axis=0)

    low = twice(block(rate_vec, 256 * group))
    high = twice(block(rate_vec, 256 * group + 128))
    own = twice(block(rate_vec, 1024 + 128 * group))

    def rates_at(places):
        places = jnp.broadcast_to(places, TILE)
        inside = lax.bitwise_and(places, 127)
        return jnp.where(places < 128, lanes_of(low, inside), lanes_of(high, inside))

    left = rates_at(local[0:1])
    right = rates_at(local[1:2])
    both = left * right
    factor_ref[0] = right
    factor_ref[1] = left
    factor_ref[2] = both + own * (left + right + both)
    factor_ref[3] = own

    own_state = lax.bitwise_and(lax.shift_right_logical(lane, 4), 3)
    left_code = lax.bitwise_and(lax.shift_right_logical(lane, 2), 3)
    right_code = lax.bitwise_and(lane, 3)
    left_own = own_state == left_code
    right_own = own_state == right_code
    first = lane < 64
    both_own = jnp.where(left_own, jnp.where(right_own, 1.0, 0.0), 0.0)
    by_rows = [choose(by_class, [uniform[c][i] for c in range(CLS)]) for i in range(STATES)]
    left_pi = choose(left_code, by_rows)
    right_pi = choose(right_code, by_rows)
    pattern_ref[0] = jnp.where(left_own, right_pi, 0.0)
    pattern_ref[1] = jnp.where(right_own, left_pi, 0.0)
    pattern_ref[2] = left_pi * right_pi
    pattern_ref[3] = jnp.where(left_code == right_code, left_pi, 0.0)

    for i in range(STATES):
        top_ref[TOP_PI + i] = choose(by_pair, [uniform[c][i] for c in range(CLS)])
    beta_pairs = choose(by_pair, betas)
    sums = choose(by_pair, [jnp.broadcast_to(total[c : c + 1], TILE) for c in range(CLS)])
    sums = jnp.broadcast_to(jnp.sum(sums, axis=1, keepdims=True), TILE)
    weights = [jnp.full(TILE, weight_ref[c], FLOAT) for c in range(CLS)]
    weight_sum = (weights[0] + weights[1]) + (weights[2] + weights[3])
    top_ref[TOP_CONST] = jnp.log(choose(by_pair, weights) / weight_sum) - beta_pairs * sums
    last = rate_vec[:, 1920:2048]
    last = choose(by_pair, [jnp.broadcast_to(last[c : c + 1], TILE) for c in range(CLS)])
    for k in range(30):
        top_ref[TOP_RATES + k] = jnp.broadcast_to(last[:, 96 + k : 97 + k], TILE)
    quarter = counts_ref[pl.ds(2 * group, 2), :].astype(FLOAT)
    top_ref[TOP_WEIGHT] = jnp.concatenate([quarter, quarter, quarter, quarter], axis=0)
    spot_copy.wait()
    step_copy.wait()

    def pairs_of(n):
        tops = [spot_ref[4 + side, 32 * group + n] for side in range(2)]
        return tops, [spot_ref[2 + side, top] for top in tops for side in range(2)]

    upper_half = sub < 4

    def build_table(n):
        _, pairs = pairs_of(n)
        places = jnp.where(
            upper_half,
            jnp.where(first, pairs[0], pairs[1]),
            jnp.where(first, pairs[2], pairs[3]),
        )
        table = both_own
        for k in range(4):
            table = table + lanes_of(factor_ref[k], places) * pattern_ref[k]
        table_ref[n] = table

    def build_tables(m, _):
        for u in range(BUILD):
            build_table(BUILD * m + u)
        return 0

    lax.fori_loop(0, 32 // BUILD, build_tables, 0)

    def small_tree(n):
        tops, pairs = pairs_of(n)
        joined = []
        for h in range(2):
            tables = [
                jnp.broadcast_to(table_ref[n, 4 * h + c : 4 * h + c + 1, :], TILE) for c in range(CLS)
            ]
            quads = []
            for p in range(2):
                pair = pairs[2 * h + p]
                codes = [codes_ref[pl.ds(spot_ref[side, pair], 8, stride=8), :] for side in range(2)]
                code = lax.shift_left(codes[0], 2) + codes[1]
                found = []
                for i in range(STATES):
                    place = code + (64 * p + 16 * i)
                    found.append([lanes_of(tables[c], place) for c in range(CLS)])
                quads.append(found)
            halves = []
            for c in range(CLS):
                pi = [pi_ref[c, i] for i in range(STATES)]
                values = [quads[0][i][c] * quads[1][i][c] for i in range(STATES)]
                halves.append(moved(values, step_ref[c, tops[h]], mean_state(pi, values)))
            joined.append(halves)
        for c in range(CLS):
            pi = [pi_ref[c, i] for i in range(STATES)]
            values = product(joined[0][c], joined[1][c])
            average = mean_state(pi, values)
            inverse = 1.0 / average
            own_rate = step_ref[4 + c, 32 * group + n]
            for i in range(STATES):
                mid_ref[n, c, i] = values[i] * inverse + own_rate
            log_ref[n, c] = jnp.log(average)

    def small_trees(m, _):
        for u in range(TREES):
            small_tree(TREES * m + u)
        return 0

    def tail_pair(at):
        return [spot_ref[6 + side, at] for side in range(2)]

    def clade(j, _):
        tops = [top - 1920 for top in tail_pair(96 + 4 * group + j)]
        pairs = [pair - 1920 for top in tops for pair in tail_pair(top)]
        leaves = [leaf - 1792 - group * 32 for pair in pairs for leaf in tail_pair(pair)]
        for c in range(CLS):
            pi = [pi_ref[c, i] for i in range(STATES)]
            scale = log_ref[leaves[0], c]
            for leaf in leaves[1:]:
                scale = scale + log_ref[leaf, c]
            halves = []
            for h in range(2):
                quads = []
                for at in (2 * h, 2 * h + 1):
                    joined = [
                        mid_ref[leaves[2 * at], c, i] * mid_ref[leaves[2 * at + 1], c, i]
                        for i in range(STATES)
                    ]
                    quads.append(moved(joined, step_ref[8 + c, pairs[at]], mean_state(pi, joined)))
                joined = product(quads[0], quads[1])
                halves.append(moved(joined, step_ref[8 + c, tops[h]], mean_state(pi, joined)))
            joined = product(halves[0], halves[1])
            inverse = 1.0 / joined[3]
            sent = [joined[0] * inverse, joined[1] * inverse, joined[2] * inverse]
            sent.append(scale + jnp.log(joined[3]))
            for v in range(4):
                for q in range(4):
                    out_ref[q, j, v, 2 * c : 2 * c + 2, :] = sent[v][2 * q : 2 * q + 2, :]
        return 0

    for load in loads:
        load.wait()
    lax.fori_loop(0, 32 // TREES, small_trees, 0)
    lax.fori_loop(0, 4, clade, 0)


def upper_kernel(child_ref, clade_ref, top_ref, site_ref, part_ref, node_ref):
    pi = [top_ref[TOP_PI + i] for i in range(STATES)]
    scale = top_ref[TOP_CONST]
    for k in range(16):
        values = [clade_ref[k, 0], clade_ref[k, 1], clade_ref[k, 2]]
        scale = scale + clade_ref[k, 3]
        average = (pi[0] * values[0] + pi[1] * values[1]) + (pi[2] * values[2] + pi[3])
        step = top_ref[TOP_RATES + k] * average
        for i in range(3):
            node_ref[k, i] = values[i] + step
        node_ref[k, 3] = step + 1.0
    at = 16
    for level, count in ((6, 8), (7, 4), (8, 2), (9, 1)):
        begin = 1024 - (1024 >> level)
        for k in range(count):
            left = child_ref[0, begin + k] - 2016
            right = child_ref[1, begin + k] - 2016
            joined = [node_ref[left, i] * node_ref[right, i] for i in range(STATES)]
            average = mean_state(pi, joined)
            if level == 6:
                scale = scale + jnp.log(average)
                inverse = 1.0 / average
                for i in range(STATES):
                    node_ref[at, i] = joined[i] * inverse + top_ref[TOP_RATES + at]
            elif level < 9:
                step = top_ref[TOP_RATES + at] * average
                for i in range(STATES):
                    node_ref[at, i] = joined[i] + step
            else:
                scale = scale + jnp.log(average)
            at += 1
    top = jnp.maximum(scale, pltpu.roll(scale, 2, 0))
    top = jnp.maximum(top, pltpu.roll(top, 4, 0))
    share = jnp.exp(scale - top)
    mass = share + pltpu.roll(share, 2, 0)
    mass = mass + pltpu.roll(mass, 4, 0)
    total = top + jnp.log(mass)
    site_ref[...] = total[0:2] * (1.0 / 1024.0)
    weight = top_ref[TOP_WEIGHT]
    classes = weight * (share / mass)
    row = lax.broadcasted_iota(jnp.int32, TILE, 0)
    column = lax.broadcasted_iota(jnp.int32, TILE, 1)
    by_row = [
        jnp.sum(values, axis=1, keepdims=True) for values in (classes, weight * total, weight)
    ]
    by_pair = lax.shift_right_logical(row, 1)
    line = jnp.where(by_pair == column, by_row[0], 0.0)
    line = jnp.where((column == 4) & (row < 2), by_row[1], line)
    line = jnp.where((column == 5) & (row < 2), by_row[2], line)
    line = jnp.sum(line, axis=0, keepdims=True)
    for k in range(16):
        part_ref[8 * k : 8 * k + 8, :] = jnp.broadcast_to(line, TILE)


def last_kernel(every_ref, own_ref, mean_ref):
    group = lax.axis_index("cls")
    sums = every_ref[0:8, :]
    for k in range(1, 16):
        sums = sums + every_ref[8 * k : 8 * k + 8, :]
    sums = jnp.sum(sums, axis=0, keepdims=True)
    column = lax.broadcasted_iota(jnp.int32, (1, 128), 1)

    def entry(at):
        return jnp.sum(jnp.where(column == at, sums, 0.0), axis=1, keepdims=True)

    count = entry(5)
    own_ref[...] = entry(group) / count
    mean_ref[...] = entry(4) / (count * 1024.0)


def per_device(tip_codes, counts, children, lengths, frequencies, weights):
    codes = tip_codes.reshape(32, 8, 8, 128).transpose(0, 2, 1, 3).reshape(2048, 128)
    child_rows = children.T
    smem = pl.BlockSpec(memory_space=SMEM)
    vmem = pl.BlockSpec(memory_space=VMEM)
    hbm = pl.BlockSpec(memory_space=pltpu.MemorySpace.HBM)
    ours, top = pl.pallas_call(
        lower_kernel,
        out_shape=(pltpu.VMEM((4, 4, 4, 8, 128), FLOAT), pltpu.VMEM((TOP_ROWS, 8, 128), FLOAT)),
        in_specs=[hbm] * 6,
        out_specs=(vmem, vmem),
        scratch_shapes=[
            pltpu.VMEM((2, 1023), jnp.int32),
            pltpu.SMEM((4, 4), FLOAT),
            pltpu.SMEM((4,), FLOAT),
            pltpu.VMEM((4, 2046), FLOAT),
            pltpu.VMEM((2048, 128), jnp.int32),
            pltpu.VMEM(TILE, jnp.int32),
            pltpu.VMEM((4, 2048), FLOAT),
            pltpu.VMEM(TILE, jnp.int32),
            pltpu.SMEM(TILE, jnp.int32),
            pltpu.VMEM((16, 128), FLOAT),
            pltpu.SMEM((16, 128), FLOAT),
            pltpu.VMEM((CLS, STATES, 8, 128), FLOAT),
            pltpu.VMEM((4, 8, 128), FLOAT),
            pltpu.VMEM((4, 8, 128), FLOAT),
            pltpu.VMEM((32, 8, 128), FLOAT),
            pltpu.VMEM((32, CLS, STATES, 8, 128), FLOAT),
            pltpu.VMEM((32, CLS, 8, 128), FLOAT),
            pltpu.SemaphoreType.DMA((11,)),
        ],
        compiler_params=pltpu.CompilerParams(vmem_limit_bytes=16 * 1024 * 1024),
        name="lower_tree",
    )(
        *(
            pltpu.with_memory_space_constraint(array, pltpu.MemorySpace.HBM)
            for array in (child_rows, frequencies, weights, lengths, codes, counts.reshape(8, 128))
        )
    )
    clades = lax.all_to_all(ours, "cls", split_axis=0, concat_axis=0, tiled=True)
    site, part = pl.pallas_call(
        upper_kernel,
        out_shape=(jax.ShapeDtypeStruct((2, 128), FLOAT), pltpu.VMEM((128, 128), FLOAT)),
        in_specs=[smem, vmem, vmem],
        out_specs=(vmem, vmem),
        scratch_shapes=[pltpu.VMEM((32, STATES, 8, 128), FLOAT)],
        compiler_params=pltpu.CompilerParams(vmem_limit_bytes=16 * 1024 * 1024),
        name="upper_tree",
    )(child_rows, clades.reshape(16, 4, 8, 128), top)
    every = lax.all_to_all(part, ("cls", "site"), split_axis=0, concat_axis=0, tiled=True)
    own, mean = pl.pallas_call(
        last_kernel,
        out_shape=(jax.ShapeDtypeStruct((1, 1), FLOAT), jax.ShapeDtypeStruct((1, 1), FLOAT)),
        in_specs=[vmem],
        out_specs=(vmem, vmem),
        compiler_params=pltpu.CompilerParams(vmem_limit_bytes=16 * 1024 * 1024),
        name="last_sums",
    )(every)
    return site.reshape(1, 256), own.reshape(1), mean.reshape(())


def solution(mesh):
    return jax.shard_map(
        per_device,
        mesh=mesh,
        in_specs=(P("cls", "site"), P("site"), P(), P(), P(), P()),
        out_specs=(P("cls", "site"), P("cls"), P()),
        check_vma=False,
    )
```

```python
import jax
import jax.numpy as jnp
from jax import lax
from jax.experimental import pallas as pl
from jax.experimental.pallas import tpu as pltpu
from jax.sharding import PartitionSpec as P

CLS = 4
STATES = 4
FLOAT = jnp.float32
SMEM = pltpu.MemorySpace.SMEM
VMEM = pltpu.MemorySpace.VMEM
TILE = (8, 128)
BUILD = 8
TOP_RATES, TOP_PI, TOP_CONST, TOP_WEIGHT, TOP_ROWS = 0, 30, 34, 35, 36


def mean_state(pi, values):
    return (pi[0] * values[0] + pi[1] * values[1]) + (pi[2] * values[2] + pi[3] * values[3])


def moved(values, rate, average):
    step = rate * average
    return [value + step for value in values]


def product(left, right):
    return [a * b for a, b in zip(left, right)]


def choose(selector, options):
    value = jnp.where(selector == 1, options[1], options[0])
    value = jnp.where(selector == 2, options[2], value)
    return jnp.where(selector == 3, options[3], value)


def lanes_of(rows, places):
    return jnp.take_along_axis(rows, places, axis=1, mode="promise_in_bounds")


def lower_kernel(
    child_hbm, freq_hbm, weight_hbm, lengths_hbm, codes_hbm, counts_hbm,
    out_ref, top_ref,
    child_vec, freq_ref, weight_ref, lengths_ref, codes_ref, counts_ref, rate_vec,
    spot_vec, spot_ref, step_vec, step_ref,
    pi_ref, pattern_ref, factor_ref, table_ref, even_ref, odd_ref, mid_ref, log_ref, sems,
):
    group = lax.axis_index("cls")
    small = [
        pltpu.make_async_copy(source, target, sems.at[4 + k])
        for k, (source, target) in enumerate(
            (
                (freq_hbm, freq_ref),
                (weight_hbm, weight_ref),
                (lengths_hbm, lengths_ref),
                (child_hbm, child_vec),
                (counts_hbm, counts_ref),
            )
        )
    ]
    for load in small:
        load.start()
    loads = [
        pltpu.make_async_copy(
            codes_hbm.at[pl.ds(512 * j, 512)], codes_ref.at[pl.ds(512 * j, 512)], sems.at[j]
        )
        for j in range(4)
    ]
    for load in loads:
        load.start()
    for load in small:
        load.wait()

    lane = lax.broadcasted_iota(jnp.int32, TILE, 1)
    sub = lax.broadcasted_iota(jnp.int32, TILE, 0)
    by_pair = lax.shift_right_logical(sub, 1)
    by_class = lax.bitwise_and(sub, 3)
    uniform, betas = [], []
    for c in range(CLS):
        raw = [jnp.full(TILE, freq_ref[c, i], FLOAT) for i in range(STATES)]
        inverse = 1.0 / ((raw[0] + raw[1]) + (raw[2] + raw[3]))
        uniform.append([value * inverse for value in raw])
        betas.append(1.0 / (1.0 - mean_state(uniform[c], uniform[c])))
        for i in range(STATES):
            pi_ref[c, i] = uniform[c][i]
    beta_rows = choose(by_class, betas)[:4]
    total = jnp.zeros((4, 128), FLOAT)
    for k in range(16):
        width = min(128, 2046 - 128 * k)
        part = lengths_ref[:, 128 * k : 128 * k + width]
        if width < 128:
            part = jnp.concatenate([part, jnp.zeros((4, 128 - width), FLOAT)], axis=1)
        total = total + part
        rate_vec[:, 128 * k : 128 * k + 128] = jnp.exp(beta_rows * part) - 1.0

    half = lax.shift_right_logical(group, 1)

    def block(ref, start):
        return ref[:, pl.ds(pl.multiple_of(start, 128), 128)]

    local = block(child_vec, 128 * group) - 256 * group
    spot_vec[0:2] = lax.shift_left(lax.shift_right_logical(local, 3), 6) + lax.bitwise_and(local, 7)
    spot_vec[2:4] = block(child_vec, 512 + 128 * half) - (1024 + 128 * group)
    spot_vec[4:6] = child_vec[:, 768:896] - (1536 + 128 * half)
    spot_vec[6:8] = jnp.concatenate([child_vec[:, 896:1023], jnp.zeros((2, 1), jnp.int32)], axis=1)
    spot_copy = pltpu.make_async_copy(spot_vec, spot_ref, sems.at[9])
    spot_copy.start()
    step_vec[0:4] = block(rate_vec, 1536 + 128 * half)
    step_vec[4:8] = rate_vec[:, 1792:1920]
    step_vec[8:12] = rate_vec[:, 1920:2048]
    step_vec[12:16] = jnp.zeros((4, 128), FLOAT)
    step_copy = pltpu.make_async_copy(step_vec, step_ref, sems.at[10])
    step_copy.start()

    def twice(rows):
        return jnp.concatenate([rows, rows], axis=0)

    low = twice(block(rate_vec, 256 * group))
    high = twice(block(rate_vec, 256 * group + 128))
    own = twice(block(rate_vec, 1024 + 128 * group))

    def rates_at(places):
        places = jnp.broadcast_to(places, TILE)
        inside = lax.bitwise_and(places, 127)
        return jnp.where(places < 128, lanes_of(low, inside), lanes_of(high, inside))

    left = rates_at(local[0:1])
    right = rates_at(local[1:2])
    both = left * right
    factor_ref[0] = right
    factor_ref[1] = left
    factor_ref[2] = both + own * (left + right + both)
    factor_ref[3] = own

    own_state = lax.bitwise_and(lax.shift_right_logical(lane, 4), 3)
    left_code = lax.bitwise_and(lax.shift_right_logical(lane, 2), 3)
    right_code = lax.bitwise_and(lane, 3)
    left_own = own_state == left_code
    right_own = own_state == right_code
    first = lane < 64
    both_own = jnp.where(left_own, jnp.where(right_own, 1.0, 0.0), 0.0)
    by_rows = [choose(by_class, [uniform[c][i] for c in range(CLS)]) for i in range(STATES)]
    left_pi = choose(left_code, by_rows)
    right_pi = choose(right_code, by_rows)
    pattern_ref[0] = jnp.where(left_own, right_pi, 0.0)
    pattern_ref[1] = jnp.where(right_own, left_pi, 0.0)
    pattern_ref[2] = left_pi * right_pi
    pattern_ref[3] = jnp.where(left_code == right_code, left_pi, 0.0)

    for i in range(STATES):
        top_ref[TOP_PI + i] = choose(by_pair, [uniform[c][i] for c in range(CLS)])
    beta_pairs = choose(by_pair, betas)
    sums = choose(by_pair, [jnp.broadcast_to(total[c : c + 1], TILE) for c in range(CLS)])
    sums = jnp.broadcast_to(jnp.sum(sums, axis=1, keepdims=True), TILE)
    weights = [jnp.full(TILE, weight_ref[c], FLOAT) for c in range(CLS)]
    weight_sum = (weights[0] + weights[1]) + (weights[2] + weights[3])
    top_ref[TOP_CONST] = jnp.log(choose(by_pair, weights) / weight_sum) - beta_pairs * sums
    last = rate_vec[:, 1920:2048]
    last = choose(by_pair, [jnp.broadcast_to(last[c : c + 1], TILE) for c in range(CLS)])
    for k in range(30):
        top_ref[TOP_RATES + k] = jnp.broadcast_to(last[:, 96 + k : 97 + k], TILE)
    quarter = counts_ref[pl.ds(2 * group, 2), :].astype(FLOAT)
    top_ref[TOP_WEIGHT] = jnp.concatenate([quarter, quarter, quarter, quarter], axis=0)
    spot_copy.wait()
    step_copy.wait()

    def pairs_of(n):
        tops = [spot_ref[4 + side, 32 * group + n] for side in range(2)]
        return tops, [spot_ref[2 + side, top] for top in tops for side in range(2)]

    upper_half = sub < 4

    def build_table(n):
        _, pairs = pairs_of(n)
        places = jnp.where(
            upper_half,
            jnp.where(first, pairs[0], pairs[1]),
            jnp.where(first, pairs[2], pairs[3]),
        )
        table = both_own
        for k in range(4):
            table = table + lanes_of(factor_ref[k], places) * pattern_ref[k]
        table_ref[n] = table

    def build_tables(m, _):
        for u in range(BUILD):
            build_table(BUILD * m + u)
        return 0

    lax.fori_loop(0, 32 // BUILD, build_tables, 0)

    def gather_tree(n, buffer):
        _, pairs = pairs_of(n)
        for h in range(2):
            tables = [
                jnp.broadcast_to(table_ref[n, 4 * h + c : 4 * h + c + 1, :], TILE) for c in range(CLS)
            ]
            codes = []
            for p in range(2):
                pair = pairs[2 * h + p]
                sides = [codes_ref[pl.ds(spot_ref[side, pair], 8, stride=8), :] for side in range(2)]
                codes.append(lax.shift_left(sides[0], 2) + sides[1])
            for i in range(STATES):
                places = [codes[p] + (64 * p + 16 * i) for p in range(2)]
                lefts = [lanes_of(tables[c], places[0]) for c in range(CLS)]
                rights = [lanes_of(tables[c], places[1]) for c in range(CLS)]
                for c in range(CLS):
                    buffer[h, c, i] = lefts[c] * rights[c]

    def finish_tree(n, buffer):
        tops, _ = pairs_of(n)
        for c in range(CLS):
            pi = [pi_ref[c, i] for i in range(STATES)]
            halves = []
            for h in range(2):
                values = [buffer[h, c, i] for i in range(STATES)]
                halves.append(moved(values, step_ref[c, tops[h]], mean_state(pi, values)))
            values = product(halves[0], halves[1])
            average = mean_state(pi, values)
            inverse = 1.0 / average
            own_rate = step_ref[4 + c, 32 * group + n]
            for i in range(STATES):
                mid_ref[n, c, i] = values[i] * inverse + own_rate
            log_ref[n, c] = jnp.log(average)

    def small_trees(m, _):
        finish_tree(2 * m, even_ref)
        gather_tree(2 * m + 1, odd_ref)
        finish_tree(2 * m + 1, odd_ref)
        gather_tree(jnp.minimum(2 * m + 2, 31), even_ref)
        return 0

    def tail_pair(at):
        return [spot_ref[6 + side, at] for side in range(2)]

    def clade(j, _):
        tops = [top - 1920 for top in tail_pair(96 + 4 * group + j)]
        pairs = [pair - 1920 for top in tops for pair in tail_pair(top)]
        leaves = [leaf - 1792 - group * 32 for pair in pairs for leaf in tail_pair(pair)]
        for c in range(CLS):
            pi = [pi_ref[c, i] for i in range(STATES)]
            scale = log_ref[leaves[0], c]
            for leaf in leaves[1:]:
                scale = scale + log_ref[leaf, c]
            halves = []
            for h in range(2):
                quads = []
                for at in (2 * h, 2 * h + 1):
                    joined = [
                        mid_ref[leaves[2 * at], c, i] * mid_ref[leaves[2 * at + 1], c, i]
                        for i in range(STATES)
                    ]
                    quads.append(moved(joined, step_ref[8 + c, pairs[at]], mean_state(pi, joined)))
                joined = product(quads[0], quads[1])
                halves.append(moved(joined, step_ref[8 + c, tops[h]], mean_state(pi, joined)))
            joined = product(halves[0], halves[1])
            inverse = 1.0 / joined[3]
            sent = [joined[0] * inverse, joined[1] * inverse, joined[2] * inverse]
            sent.append(scale + jnp.log(joined[3]))
            for v in range(4):
                for q in range(4):
                    out_ref[lax.bitwise_and(q - group, 3), j, v, 2 * c : 2 * c + 2, :] = sent[v][2 * q : 2 * q + 2, :]
        return 0

    for load in loads:
        load.wait()
    gather_tree(0, even_ref)
    lax.fori_loop(0, 16, small_trees, 0)
    lax.fori_loop(0, 4, clade, 0)


def upper_kernel(child_ref, own_ref, one_ref, two_ref, three_ref, top_ref, site_ref, part_ref, node_ref):
    group = lax.axis_index("cls")
    pi = [top_ref[TOP_PI + i] for i in range(STATES)]
    scale = top_ref[TOP_CONST]
    for hop, piece_ref in enumerate((own_ref, one_ref, two_ref, three_ref)):
        source = 4 * lax.bitwise_and(group - hop, 3)
        for j in range(4):
            values = [piece_ref[j, 0], piece_ref[j, 1], piece_ref[j, 2]]
            scale = scale + piece_ref[j, 3]
            average = (pi[0] * values[0] + pi[1] * values[1]) + (pi[2] * values[2] + pi[3])
            step = top_ref[TOP_RATES + source + j] * average
            for i in range(3):
                node_ref[source + j, i] = values[i] + step
            node_ref[source + j, 3] = step + 1.0
    at = 16
    for level, count in ((6, 8), (7, 4), (8, 2), (9, 1)):
        begin = 1024 - (1024 >> level)
        for k in range(count):
            left = child_ref[0, begin + k] - 2016
            right = child_ref[1, begin + k] - 2016
            joined = [node_ref[left, i] * node_ref[right, i] for i in range(STATES)]
            average = mean_state(pi, joined)
            if level == 6:
                scale = scale + jnp.log(average)
                inverse = 1.0 / average
                for i in range(STATES):
                    node_ref[at, i] = joined[i] * inverse + top_ref[TOP_RATES + at]
            elif level < 9:
                step = top_ref[TOP_RATES + at] * average
                for i in range(STATES):
                    node_ref[at, i] = joined[i] + step
            else:
                scale = scale + jnp.log(average)
            at += 1
    top = jnp.maximum(scale, pltpu.roll(scale, 2, 0))
    top = jnp.maximum(top, pltpu.roll(top, 4, 0))
    share = jnp.exp(scale - top)
    mass = share + pltpu.roll(share, 2, 0)
    mass = mass + pltpu.roll(mass, 4, 0)
    total = top + jnp.log(mass)
    site_ref[...] = total[0:2] * (1.0 / 1024.0)
    weight = top_ref[TOP_WEIGHT]
    classes = weight * (share / mass)
    row = lax.broadcasted_iota(jnp.int32, TILE, 0)
    column = lax.broadcasted_iota(jnp.int32, TILE, 1)
    by_row = [
        jnp.sum(values, axis=1, keepdims=True) for values in (classes, weight * total, weight)
    ]
    by_pair = lax.shift_right_logical(row, 1)
    line = jnp.where(by_pair == column, by_row[0], 0.0)
    line = jnp.where((column == 4) & (row < 2), by_row[1], line)
    line = jnp.where((column == 5) & (row < 2), by_row[2], line)
    line = jnp.sum(line, axis=0, keepdims=True)
    for k in range(16):
        part_ref[8 * k : 8 * k + 8, :] = jnp.broadcast_to(line, TILE)


def last_kernel(every_ref, own_ref, mean_ref):
    group = lax.axis_index("cls")
    sums = every_ref[0:8, :]
    for k in range(1, 16):
        sums = sums + every_ref[8 * k : 8 * k + 8, :]
    sums = jnp.sum(sums, axis=0, keepdims=True)
    column = lax.broadcasted_iota(jnp.int32, (1, 128), 1)

    def entry(at):
        return jnp.sum(jnp.where(column == at, sums, 0.0), axis=1, keepdims=True)

    count = entry(5)
    own_ref[...] = entry(group) / count
    mean_ref[...] = entry(4) / (count * 1024.0)


def per_device(tip_codes, counts, children, lengths, frequencies, weights):
    codes = tip_codes.reshape(32, 8, 8, 128).transpose(0, 2, 1, 3).reshape(2048, 128)
    child_rows = children.T
    smem = pl.BlockSpec(memory_space=SMEM)
    vmem = pl.BlockSpec(memory_space=VMEM)
    hbm = pl.BlockSpec(memory_space=pltpu.MemorySpace.HBM)
    ours, top = pl.pallas_call(
        lower_kernel,
        out_shape=(pltpu.VMEM((4, 4, 4, 8, 128), FLOAT), pltpu.VMEM((TOP_ROWS, 8, 128), FLOAT)),
        in_specs=[hbm] * 6,
        out_specs=(vmem, vmem),
        scratch_shapes=[
            pltpu.VMEM((2, 1023), jnp.int32),
            pltpu.SMEM((4, 4), FLOAT),
            pltpu.SMEM((4,), FLOAT),
            pltpu.VMEM((4, 2046), FLOAT),
            pltpu.VMEM((2048, 128), jnp.int32),
            pltpu.VMEM(TILE, jnp.int32),
            pltpu.VMEM((4, 2048), FLOAT),
            pltpu.VMEM(TILE, jnp.int32),
            pltpu.SMEM(TILE, jnp.int32),
            pltpu.VMEM((16, 128), FLOAT),
            pltpu.SMEM((16, 128), FLOAT),
            pltpu.VMEM((CLS, STATES, 8, 128), FLOAT),
            pltpu.VMEM((4, 8, 128), FLOAT),
            pltpu.VMEM((4, 8, 128), FLOAT),
            pltpu.VMEM((32, 8, 128), FLOAT),
            pltpu.VMEM((2, CLS, STATES, 8, 128), FLOAT),
            pltpu.VMEM((2, CLS, STATES, 8, 128), FLOAT),
            pltpu.VMEM((32, CLS, STATES, 8, 128), FLOAT),
            pltpu.VMEM((32, CLS, 8, 128), FLOAT),
            pltpu.SemaphoreType.DMA((11,)),
        ],
        compiler_params=pltpu.CompilerParams(vmem_limit_bytes=16 * 1024 * 1024),
        name="lower_tree",
    )(
        *(
            pltpu.with_memory_space_constraint(array, pltpu.MemorySpace.HBM)
            for array in (child_rows, frequencies, weights, lengths, codes, counts.reshape(8, 128))
        )
    )
    pieces = [ours[0]]
    for hop in range(1, 4):
        pieces.append(lax.ppermute(ours[hop], "cls", [(k, (k + hop) % 4) for k in range(4)]))
    site, part = pl.pallas_call(
        upper_kernel,
        out_shape=(jax.ShapeDtypeStruct((2, 128), FLOAT), pltpu.VMEM((128, 128), FLOAT)),
        in_specs=[smem] + [vmem] * 5,
        out_specs=(vmem, vmem),
        scratch_shapes=[pltpu.VMEM((32, STATES, 8, 128), FLOAT)],
        compiler_params=pltpu.CompilerParams(vmem_limit_bytes=16 * 1024 * 1024),
        name="upper_tree",
    )(child_rows, *pieces, top)
    every = lax.all_to_all(part, ("cls", "site"), split_axis=0, concat_axis=0, tiled=True)
    own, mean = pl.pallas_call(
        last_kernel,
        out_shape=(jax.ShapeDtypeStruct((1, 1), FLOAT), jax.ShapeDtypeStruct((1, 1), FLOAT)),
        in_specs=[vmem],
        out_specs=(vmem, vmem),
        compiler_params=pltpu.CompilerParams(vmem_limit_bytes=16 * 1024 * 1024),
        name="last_sums",
    )(every)
    return site.reshape(1, 256), own.reshape(1), mean.reshape(())


def solution(mesh):
    return jax.shard_map(
        per_device,
        mesh=mesh,
        in_specs=(P("cls", "site"), P("site"), P(), P(), P(), P()),
        out_specs=(P("cls", "site"), P("cls"), P()),
        check_vma=False,
    )
```

```python
import jax
import jax.numpy as jnp
from jax import lax
from jax.experimental import pallas as pl
from jax.experimental.pallas import tpu as pltpu
from jax.sharding import PartitionSpec as P

CLS = 4
STATES = 4
FLOAT = jnp.float32
SMEM = pltpu.MemorySpace.SMEM
VMEM = pltpu.MemorySpace.VMEM
TILE = (8, 128)
BUILD = 8
TOP_RATES, TOP_PI, TOP_CONST, TOP_WEIGHT, TOP_ROWS = 0, 30, 34, 35, 36


def mean_state(pi, values):
    return (pi[0] * values[0] + pi[1] * values[1]) + (pi[2] * values[2] + pi[3] * values[3])


def moved(values, rate, average):
    step = rate * average
    return [value + step for value in values]


def product(left, right):
    return [a * b for a, b in zip(left, right)]


def choose(selector, options):
    value = jnp.where(selector == 1, options[1], options[0])
    value = jnp.where(selector == 2, options[2], value)
    return jnp.where(selector == 3, options[3], value)


def lanes_of(rows, places):
    return jnp.take_along_axis(rows, places, axis=1, mode="promise_in_bounds")


def lower_kernel(
    child_hbm, freq_hbm, weight_hbm, lengths_hbm, codes_hbm, counts_hbm,
    out_ref, top_ref,
    child_vec, freq_ref, weight_ref, lengths_ref, codes_ref, counts_ref, rate_vec,
    spot_vec, spot_ref, step_vec, step_ref,
    pi_ref, pattern_ref, factor_ref, table_ref, rate4_vec, rate4_ref, mid_ref, log_ref, sems,
):
    group = lax.axis_index("cls")
    small = [
        pltpu.make_async_copy(source, target, sems.at[4 + k])
        for k, (source, target) in enumerate(
            (
                (freq_hbm, freq_ref),
                (weight_hbm, weight_ref),
                (lengths_hbm, lengths_ref),
                (child_hbm, child_vec),
                (counts_hbm, counts_ref),
            )
        )
    ]
    for load in small:
        load.start()
    loads = [
        pltpu.make_async_copy(
            codes_hbm.at[pl.ds(512 * j, 512)], codes_ref.at[pl.ds(512 * j, 512)], sems.at[j]
        )
        for j in range(4)
    ]
    for load in loads:
        load.start()
    for load in small:
        load.wait()

    lane = lax.broadcasted_iota(jnp.int32, TILE, 1)
    sub = lax.broadcasted_iota(jnp.int32, TILE, 0)
    by_pair = lax.shift_right_logical(sub, 1)
    by_class = lax.bitwise_and(sub, 3)
    uniform, betas = [], []
    for c in range(CLS):
        raw = [jnp.full(TILE, freq_ref[c, i], FLOAT) for i in range(STATES)]
        inverse = 1.0 / ((raw[0] + raw[1]) + (raw[2] + raw[3]))
        uniform.append([value * inverse for value in raw])
        betas.append(1.0 / (1.0 - mean_state(uniform[c], uniform[c])))
        for i in range(STATES):
            pi_ref[c, i] = uniform[c][i]
    beta_rows = choose(by_class, betas)[:4]
    total = jnp.zeros((4, 128), FLOAT)
    for k in range(16):
        width = min(128, 2046 - 128 * k)
        part = lengths_ref[:, 128 * k : 128 * k + width]
        if width < 128:
            part = jnp.concatenate([part, jnp.zeros((4, 128 - width), FLOAT)], axis=1)
        total = total + part
        rate_vec[:, 128 * k : 128 * k + 128] = jnp.exp(beta_rows * part) - 1.0

    half = lax.shift_right_logical(group, 1)

    def block(ref, start):
        return ref[:, pl.ds(pl.multiple_of(start, 128), 128)]

    local = block(child_vec, 128 * group) - 256 * group
    spot_vec[0:2] = lax.shift_left(lax.shift_right_logical(local, 3), 6) + lax.bitwise_and(local, 7)
    spot_vec[2:4] = block(child_vec, 512 + 128 * half) - (1024 + 128 * group)
    spot_vec[4:6] = child_vec[:, 768:896] - (1536 + 128 * half)
    spot_vec[6:8] = jnp.concatenate([child_vec[:, 896:1023], jnp.zeros((2, 1), jnp.int32)], axis=1)
    spot_copy = pltpu.make_async_copy(spot_vec, spot_ref, sems.at[9])
    spot_copy.start()
    step_vec[0:4] = block(rate_vec, 1536 + 128 * half)
    step_vec[4:8] = rate_vec[:, 1792:1920]
    step_vec[8:12] = rate_vec[:, 1920:2048]
    step_vec[12:16] = jnp.zeros((4, 128), FLOAT)
    step_copy = pltpu.make_async_copy(step_vec, step_ref, sems.at[10])
    step_copy.start()

    def twice(rows):
        return jnp.concatenate([rows, rows], axis=0)

    low = twice(block(rate_vec, 256 * group))
    high = twice(block(rate_vec, 256 * group + 128))
    own = twice(block(rate_vec, 1024 + 128 * group))

    def rates_at(places):
        places = jnp.broadcast_to(places, TILE)
        inside = lax.bitwise_and(places, 127)
        return jnp.where(places < 128, lanes_of(low, inside), lanes_of(high, inside))

    left = rates_at(local[0:1])
    right = rates_at(local[1:2])
    both = left * right
    factor_ref[0] = right
    factor_ref[1] = left
    factor_ref[2] = both + own * (left + right + both)
    factor_ref[3] = own
    for k in range(4):
        rate4_vec[4 * k : 4 * k + 4] = factor_ref[k, 0:4]
    rate4_copy = pltpu.make_async_copy(rate4_vec, rate4_ref, sems.at[11])
    rate4_copy.start()

    own_state = lax.bitwise_and(lax.shift_right_logical(lane, 4), 3)
    left_code = lax.bitwise_and(lax.shift_right_logical(lane, 2), 3)
    right_code = lax.bitwise_and(lane, 3)
    left_own = own_state == left_code
    right_own = own_state == right_code
    first = lane < 64
    both_own = jnp.where(left_own, jnp.where(right_own, 1.0, 0.0), 0.0)
    by_rows = [choose(by_class, [uniform[c][i] for c in range(CLS)]) for i in range(STATES)]
    left_pi = choose(left_code, by_rows)
    right_pi = choose(right_code, by_rows)
    pattern_ref[0] = jnp.where(left_own, right_pi, 0.0)
    pattern_ref[1] = jnp.where(right_own, left_pi, 0.0)
    pattern_ref[2] = left_pi * right_pi
    pattern_ref[3] = jnp.where(left_code == right_code, left_pi, 0.0)

    for i in range(STATES):
        top_ref[TOP_PI + i] = choose(by_pair, [uniform[c][i] for c in range(CLS)])
    beta_pairs = choose(by_pair, betas)
    sums = choose(by_pair, [jnp.broadcast_to(total[c : c + 1], TILE) for c in range(CLS)])
    sums = jnp.broadcast_to(jnp.sum(sums, axis=1, keepdims=True), TILE)
    weights = [jnp.full(TILE, weight_ref[c], FLOAT) for c in range(CLS)]
    weight_sum = (weights[0] + weights[1]) + (weights[2] + weights[3])
    top_ref[TOP_CONST] = jnp.log(choose(by_pair, weights) / weight_sum) - beta_pairs * sums
    last = rate_vec[:, 1920:2048]
    last = choose(by_pair, [jnp.broadcast_to(last[c : c + 1], TILE) for c in range(CLS)])
    for k in range(30):
        top_ref[TOP_RATES + k] = jnp.broadcast_to(last[:, 96 + k : 97 + k], TILE)
    quarter = counts_ref[pl.ds(2 * group, 2), :].astype(FLOAT)
    top_ref[TOP_WEIGHT] = jnp.concatenate([quarter, quarter, quarter, quarter], axis=0)
    spot_copy.wait()
    step_copy.wait()
    rate4_copy.wait()

    def pairs_of(n):
        tops = [spot_ref[4 + side, 32 * group + n] for side in range(2)]
        return tops, [spot_ref[2 + side, top] for top in tops for side in range(2)]

    upper_half = sub < 4

    def build_table(m):
        pairs = [pairs_of(2 * m + u)[1] for u in range(2)]
        places = jnp.where(
            upper_half,
            jnp.where(first, pairs[0][0], pairs[0][2]),
            jnp.where(first, pairs[1][0], pairs[1][2]),
        )
        table = both_own
        for k in range(4):
            table = table + lanes_of(factor_ref[k], places) * pattern_ref[k]
        table_ref[m] = table

    def build_tables(m, _):
        for u in range(BUILD):
            build_table(BUILD * m + u)
        return 0

    lax.fori_loop(0, 16 // BUILD, build_tables, 0)

    def codes_of(pair):
        return [codes_ref[pl.ds(spot_ref[side, pair], 8, stride=8), :] for side in range(2)]

    def chosen_pair(pair):
        left, right = codes_of(pair)
        left_odd = lax.bitwise_and(left, 1) == 1
        right_odd = lax.bitwise_and(right, 1) == 1
        left_high = left >= 2
        right_high = right >= 2
        same = left == right
        left_is = [left == i for i in range(STATES)]
        right_is = [right == i for i in range(STATES)]
        found = []
        for c in range(CLS):
            pi = [pi_ref[c, i] for i in range(STATES)]
            left_pi = jnp.where(
                left_high, jnp.where(left_odd, pi[3], pi[2]), jnp.where(left_odd, pi[1], pi[0])
            )
            right_pi = jnp.where(
                right_high, jnp.where(right_odd, pi[3], pi[2]), jnp.where(right_odd, pi[1], pi[0])
            )
            left_step = rate4_ref[4 + c, pair] * left_pi
            right_step = rate4_ref[c, pair] * right_pi
            base = rate4_ref[8 + c, pair] * (left_pi * right_pi)
            base = base + jnp.where(same, rate4_ref[12 + c, pair] * left_pi, 0.0)
            at_right = base + left_step
            at_left = base + right_step
            at_left = jnp.where(same, at_left + (left_step + 1.0), at_left)
            found.append(
                [
                    jnp.where(left_is[i], at_left, jnp.where(right_is[i], at_right, base))
                    for i in range(STATES)
                ]
            )
        return found

    def small_tree(m, u):
        n = 2 * m + u
        tops, pairs = pairs_of(n)
        tables = [
            jnp.broadcast_to(table_ref[m, 4 * u + c : 4 * u + c + 1, :], TILE) for c in range(CLS)
        ]
        halves = []
        for h in range(2):
            sides = codes_of(pairs[2 * h])
            code = lax.shift_left(sides[0], 2) + sides[1] + 64 * h
            looked = []
            for i in range(STATES):
                place = code + 16 * i if i else code
                looked.append([lanes_of(tables[c], place) for c in range(CLS)])
            chosen = chosen_pair(pairs[2 * h + 1])
            parts = []
            for c in range(CLS):
                pi = [pi_ref[c, i] for i in range(STATES)]
                values = [looked[i][c] * chosen[c][i] for i in range(STATES)]
                parts.append(moved(values, step_ref[c, tops[h]], mean_state(pi, values)))
            halves.append(parts)
        for c in range(CLS):
            pi = [pi_ref[c, i] for i in range(STATES)]
            values = product(halves[0][c], halves[1][c])
            average = mean_state(pi, values)
            inverse = 1.0 / average
            own_rate = step_ref[4 + c, 32 * group + n]
            for i in range(STATES):
                mid_ref[n, c, i] = values[i] * inverse + own_rate
            log_ref[n, c] = jnp.log(average)

    def small_trees(m, _):
        for u in range(2):
            small_tree(m, u)
        return 0

    def tail_pair(at):
        return [spot_ref[6 + side, at] for side in range(2)]

    def clade(j, _):
        tops = [top - 1920 for top in tail_pair(96 + 4 * group + j)]
        pairs = [pair - 1920 for top in tops for pair in tail_pair(top)]
        leaves = [leaf - 1792 - group * 32 for pair in pairs for leaf in tail_pair(pair)]
        for c in range(CLS):
            pi = [pi_ref[c, i] for i in range(STATES)]
            scale = log_ref[leaves[0], c]
            for leaf in leaves[1:]:
                scale = scale + log_ref[leaf, c]
            halves = []
            for h in range(2):
                quads = []
                for at in (2 * h, 2 * h + 1):
                    joined = [
                        mid_ref[leaves[2 * at], c, i] * mid_ref[leaves[2 * at + 1], c, i]
                        for i in range(STATES)
                    ]
                    quads.append(moved(joined, step_ref[8 + c, pairs[at]], mean_state(pi, joined)))
                joined = product(quads[0], quads[1])
                halves.append(moved(joined, step_ref[8 + c, tops[h]], mean_state(pi, joined)))
            joined = product(halves[0], halves[1])
            inverse = 1.0 / joined[3]
            sent = [joined[0] * inverse, joined[1] * inverse, joined[2] * inverse]
            sent.append(scale + jnp.log(joined[3]))
            for v in range(4):
                for q in range(4):
                    out_ref[lax.bitwise_and(q - group, 3), j, v, 2 * c : 2 * c + 2, :] = sent[v][2 * q : 2 * q + 2, :]
        return 0

    for load in loads:
        load.wait()
    lax.fori_loop(0, 16, small_trees, 0)
    lax.fori_loop(0, 4, clade, 0)


def upper_kernel(child_ref, own_ref, one_ref, two_ref, three_ref, top_ref, site_ref, part_ref, node_ref):
    group = lax.axis_index("cls")
    pi = [top_ref[TOP_PI + i] for i in range(STATES)]
    scale = top_ref[TOP_CONST]
    for hop, piece_ref in enumerate((own_ref, one_ref, two_ref, three_ref)):
        source = 4 * lax.bitwise_and(group - hop, 3)
        for j in range(4):
            values = [piece_ref[j, 0], piece_ref[j, 1], piece_ref[j, 2]]
            scale = scale + piece_ref[j, 3]
            average = (pi[0] * values[0] + pi[1] * values[1]) + (pi[2] * values[2] + pi[3])
            step = top_ref[TOP_RATES + source + j] * average
            for i in range(3):
                node_ref[source + j, i] = values[i] + step
            node_ref[source + j, 3] = step + 1.0
    at = 16
    for level, count in ((6, 8), (7, 4), (8, 2), (9, 1)):
        begin = 1024 - (1024 >> level)
        for k in range(count):
            left = child_ref[0, begin + k] - 2016
            right = child_ref[1, begin + k] - 2016
            joined = [node_ref[left, i] * node_ref[right, i] for i in range(STATES)]
            average = mean_state(pi, joined)
            if level == 6:
                scale = scale + jnp.log(average)
                inverse = 1.0 / average
                for i in range(STATES):
                    node_ref[at, i] = joined[i] * inverse + top_ref[TOP_RATES + at]
            elif level < 9:
                step = top_ref[TOP_RATES + at] * average
                for i in range(STATES):
                    node_ref[at, i] = joined[i] + step
            else:
                scale = scale + jnp.log(average)
            at += 1
    top = jnp.maximum(scale, pltpu.roll(scale, 2, 0))
    top = jnp.maximum(top, pltpu.roll(top, 4, 0))
    share = jnp.exp(scale - top)
    mass = share + pltpu.roll(share, 2, 0)
    mass = mass + pltpu.roll(mass, 4, 0)
    total = top + jnp.log(mass)
    site_ref[...] = total[0:2] * (1.0 / 1024.0)
    weight = top_ref[TOP_WEIGHT]
    classes = weight * (share / mass)
    row = lax.broadcasted_iota(jnp.int32, TILE, 0)
    column = lax.broadcasted_iota(jnp.int32, TILE, 1)
    by_row = [
        jnp.sum(values, axis=1, keepdims=True) for values in (classes, weight * total, weight)
    ]
    by_pair = lax.shift_right_logical(row, 1)
    line = jnp.where(by_pair == column, by_row[0], 0.0)
    line = jnp.where((column == 4) & (row < 2), by_row[1], line)
    line = jnp.where((column == 5) & (row < 2), by_row[2], line)
    line = jnp.sum(line, axis=0, keepdims=True)
    for k in range(16):
        part_ref[8 * k : 8 * k + 8, :] = jnp.broadcast_to(line, TILE)


def last_kernel(every_ref, own_ref, mean_ref):
    group = lax.axis_index("cls")
    sums = every_ref[0:8, :]
    for k in range(1, 16):
        sums = sums + every_ref[8 * k : 8 * k + 8, :]
    sums = jnp.sum(sums, axis=0, keepdims=True)
    column = lax.broadcasted_iota(jnp.int32, (1, 128), 1)

    def entry(at):
        return jnp.sum(jnp.where(column == at, sums, 0.0), axis=1, keepdims=True)

    count = entry(5)
    own_ref[...] = entry(group) / count
    mean_ref[...] = entry(4) / (count * 1024.0)


def per_device(tip_codes, counts, children, lengths, frequencies, weights):
    codes = tip_codes.reshape(32, 8, 8, 128).transpose(0, 2, 1, 3).reshape(2048, 128)
    child_rows = children.T
    smem = pl.BlockSpec(memory_space=SMEM)
    vmem = pl.BlockSpec(memory_space=VMEM)
    hbm = pl.BlockSpec(memory_space=pltpu.MemorySpace.HBM)
    ours, top = pl.pallas_call(
        lower_kernel,
        out_shape=(pltpu.VMEM((4, 4, 4, 8, 128), FLOAT), pltpu.VMEM((TOP_ROWS, 8, 128), FLOAT)),
        in_specs=[hbm] * 6,
        out_specs=(vmem, vmem),
        scratch_shapes=[
            pltpu.VMEM((2, 1023), jnp.int32),
            pltpu.SMEM((4, 4), FLOAT),
            pltpu.SMEM((4,), FLOAT),
            pltpu.VMEM((4, 2046), FLOAT),
            pltpu.VMEM((2048, 128), jnp.int32),
            pltpu.VMEM(TILE, jnp.int32),
            pltpu.VMEM((4, 2048), FLOAT),
            pltpu.VMEM(TILE, jnp.int32),
            pltpu.SMEM(TILE, jnp.int32),
            pltpu.VMEM((16, 128), FLOAT),
            pltpu.SMEM((16, 128), FLOAT),
            pltpu.VMEM((CLS, STATES, 8, 128), FLOAT),
            pltpu.VMEM((4, 8, 128), FLOAT),
            pltpu.VMEM((4, 8, 128), FLOAT),
            pltpu.VMEM((16, 8, 128), FLOAT),
            pltpu.VMEM((16, 128), FLOAT),
            pltpu.SMEM((16, 128), FLOAT),
            pltpu.VMEM((32, CLS, STATES, 8, 128), FLOAT),
            pltpu.VMEM((32, CLS, 8, 128), FLOAT),
            pltpu.SemaphoreType.DMA((12,)),
        ],
        compiler_params=pltpu.CompilerParams(vmem_limit_bytes=16 * 1024 * 1024),
        name="lower_tree",
    )(
        *(
            pltpu.with_memory_space_constraint(array, pltpu.MemorySpace.HBM)
            for array in (child_rows, frequencies, weights, lengths, codes, counts.reshape(8, 128))
        )
    )
    pieces = [ours[0]]
    for hop in range(1, 4):
        pieces.append(lax.ppermute(ours[hop], "cls", [(k, (k + hop) % 4) for k in range(4)]))
    site, part = pl.pallas_call(
        upper_kernel,
        out_shape=(jax.ShapeDtypeStruct((2, 128), FLOAT), pltpu.VMEM((128, 128), FLOAT)),
        in_specs=[smem] + [vmem] * 5,
        out_specs=(vmem, vmem),
        scratch_shapes=[pltpu.VMEM((32, STATES, 8, 128), FLOAT)],
        compiler_params=pltpu.CompilerParams(vmem_limit_bytes=16 * 1024 * 1024),
        name="upper_tree",
    )(child_rows, *pieces, top)
    every = lax.all_to_all(part, ("cls", "site"), split_axis=0, concat_axis=0, tiled=True)
    own, mean = pl.pallas_call(
        last_kernel,
        out_shape=(jax.ShapeDtypeStruct((1, 1), FLOAT), jax.ShapeDtypeStruct((1, 1), FLOAT)),
        in_specs=[vmem],
        out_specs=(vmem, vmem),
        compiler_params=pltpu.CompilerParams(vmem_limit_bytes=16 * 1024 * 1024),
        name="last_sums",
    )(every)
    return site.reshape(1, 256), own.reshape(1), mean.reshape(())


def solution(mesh):
    return jax.shard_map(
        per_device,
        mesh=mesh,
        in_specs=(P("cls", "site"), P("site"), P(), P(), P(), P()),
        out_specs=(P("cls", "site"), P("cls"), P()),
        check_vma=False,
    )
```

```python
import jax
import jax.numpy as jnp
from jax import lax
from jax.experimental import pallas as pl
from jax.experimental.pallas import tpu as pltpu
from jax.sharding import PartitionSpec as P

CLS = 4
STATES = 4
FLOAT = jnp.float32
SMEM = pltpu.MemorySpace.SMEM
VMEM = pltpu.MemorySpace.VMEM
TILE = (8, 128)
BUILD = 8
TOP_RATES, TOP_PI, TOP_CONST, TOP_WEIGHT, TOP_ROWS = 0, 30, 34, 35, 36


def mean_state(pi, values):
    return (pi[0] * values[0] + pi[1] * values[1]) + (pi[2] * values[2] + pi[3] * values[3])


def moved(values, rate, average):
    step = rate * average
    return [value + step for value in values]


def product(left, right):
    return [a * b for a, b in zip(left, right)]


def choose(selector, options):
    value = jnp.where(selector == 1, options[1], options[0])
    value = jnp.where(selector == 2, options[2], value)
    return jnp.where(selector == 3, options[3], value)


def pick(masks, options):
    value = jnp.where(masks[1], options[1], options[0])
    value = jnp.where(masks[2], options[2], value)
    return jnp.where(masks[3], options[3], value)


def lanes_of(rows, places):
    return jnp.take_along_axis(rows, places, axis=1, mode="promise_in_bounds")


def lower_kernel(
    child_hbm, freq_hbm, weight_hbm, lengths_hbm, codes_hbm, counts_hbm,
    out_ref, top_ref,
    child_vec, freq_ref, weight_ref, lengths_ref, codes_ref, counts_ref, rate_vec,
    spot_vec, spot_ref, step_vec, step_ref,
    pi_ref, pattern_ref, factor_ref, table_ref, rate4_vec, rate4_ref, mid_ref, log_ref, sems,
):
    group = lax.axis_index("cls")
    small = [
        pltpu.make_async_copy(source, target, sems.at[4 + k])
        for k, (source, target) in enumerate(
            (
                (child_hbm, child_vec),
                (lengths_hbm, lengths_ref),
                (freq_hbm, freq_ref),
                (weight_hbm, weight_ref),
                (counts_hbm, counts_ref),
            )
        )
    ]
    for load in small:
        load.start()
    loads = [
        pltpu.make_async_copy(
            codes_hbm.at[pl.ds(512 * j, 512)], codes_ref.at[pl.ds(512 * j, 512)], sems.at[j]
        )
        for j in range(4)
    ]
    for load in loads:
        load.start()
    small[0].wait()
    half = lax.shift_right_logical(group, 1)

    def block(ref, start):
        return ref[:, pl.ds(pl.multiple_of(start, 128), 128)]

    local = block(child_vec, 128 * group) - 256 * group
    spot_vec[0:2] = lax.shift_left(lax.shift_right_logical(local, 3), 6) + lax.bitwise_and(local, 7)
    spot_vec[2:4] = block(child_vec, 512 + 128 * half) - (1024 + 128 * group)
    spot_vec[4:6] = child_vec[:, 768:896] - (1536 + 128 * half)
    spot_vec[6:8] = jnp.concatenate([child_vec[:, 896:1023], jnp.zeros((2, 1), jnp.int32)], axis=1)
    spot_copy = pltpu.make_async_copy(spot_vec, spot_ref, sems.at[9])
    spot_copy.start()
    for load in small[1:]:
        load.wait()

    lane = lax.broadcasted_iota(jnp.int32, TILE, 1)
    sub = lax.broadcasted_iota(jnp.int32, TILE, 0)
    by_pair = lax.shift_right_logical(sub, 1)
    by_class = lax.bitwise_and(sub, 3)
    uniform, betas = [], []
    for c in range(CLS):
        raw = [jnp.full(TILE, freq_ref[c, i], FLOAT) for i in range(STATES)]
        inverse = 1.0 / ((raw[0] + raw[1]) + (raw[2] + raw[3]))
        uniform.append([value * inverse for value in raw])
        betas.append(1.0 / (1.0 - mean_state(uniform[c], uniform[c])))
        for i in range(STATES):
            pi_ref[c, i] = uniform[c][i]
    beta_rows = choose(by_class, betas)[:4]
    total = jnp.zeros((4, 128), FLOAT)
    for k in range(16):
        width = min(128, 2046 - 128 * k)
        part = lengths_ref[:, 128 * k : 128 * k + width]
        if width < 128:
            part = jnp.concatenate([part, jnp.zeros((4, 128 - width), FLOAT)], axis=1)
        total = total + part
        rate_vec[:, 128 * k : 128 * k + 128] = jnp.exp(beta_rows * part) - 1.0

    step_vec[0:4] = block(rate_vec, 1536 + 128 * half)
    step_vec[4:8] = rate_vec[:, 1792:1920]
    step_vec[8:12] = rate_vec[:, 1920:2048]
    step_vec[12:16] = jnp.zeros((4, 128), FLOAT)
    step_copy = pltpu.make_async_copy(step_vec, step_ref, sems.at[10])
    step_copy.start()

    def twice(rows):
        return jnp.concatenate([rows, rows], axis=0)

    low = twice(block(rate_vec, 256 * group))
    high = twice(block(rate_vec, 256 * group + 128))
    own = twice(block(rate_vec, 1024 + 128 * group))

    def rates_at(places):
        places = jnp.broadcast_to(places, TILE)
        inside = lax.bitwise_and(places, 127)
        return jnp.where(places < 128, lanes_of(low, inside), lanes_of(high, inside))

    left = rates_at(local[0:1])
    right = rates_at(local[1:2])
    both = left * right
    factor_ref[0] = right
    factor_ref[1] = left
    factor_ref[2] = both + own * (left + right + both)
    factor_ref[3] = own
    for k in range(4):
        rate4_vec[4 * k : 4 * k + 4] = factor_ref[k, 0:4]
    rate4_copy = pltpu.make_async_copy(rate4_vec, rate4_ref, sems.at[11])
    rate4_copy.start()

    own_state = lax.bitwise_and(lax.shift_right_logical(lane, 4), 3)
    left_code = lax.bitwise_and(lax.shift_right_logical(lane, 2), 3)
    right_code = lax.bitwise_and(lane, 3)
    left_own = own_state == left_code
    right_own = own_state == right_code
    first = lane < 64
    both_own = jnp.where(left_own, jnp.where(right_own, 1.0, 0.0), 0.0)
    by_rows = [choose(by_class, [uniform[c][i] for c in range(CLS)]) for i in range(STATES)]
    left_pi = choose(left_code, by_rows)
    right_pi = choose(right_code, by_rows)
    pattern_ref[0] = jnp.where(left_own, right_pi, 0.0)
    pattern_ref[1] = jnp.where(right_own, left_pi, 0.0)
    pattern_ref[2] = left_pi * right_pi
    pattern_ref[3] = jnp.where(left_code == right_code, left_pi, 0.0)

    for i in range(STATES):
        top_ref[TOP_PI + i] = choose(by_pair, [uniform[c][i] for c in range(CLS)])
    beta_pairs = choose(by_pair, betas)
    sums = choose(by_pair, [jnp.broadcast_to(total[c : c + 1], TILE) for c in range(CLS)])
    sums = jnp.broadcast_to(jnp.sum(sums, axis=1, keepdims=True), TILE)
    weights = [jnp.full(TILE, weight_ref[c], FLOAT) for c in range(CLS)]
    weight_sum = (weights[0] + weights[1]) + (weights[2] + weights[3])
    top_ref[TOP_CONST] = jnp.log(choose(by_pair, weights) / weight_sum) - beta_pairs * sums
    last = rate_vec[:, 1920:2048]
    last = choose(by_pair, [jnp.broadcast_to(last[c : c + 1], TILE) for c in range(CLS)])
    for k in range(30):
        top_ref[TOP_RATES + k] = jnp.broadcast_to(last[:, 96 + k : 97 + k], TILE)
    quarter = counts_ref[pl.ds(2 * group, 2), :].astype(FLOAT)
    top_ref[TOP_WEIGHT] = jnp.concatenate([quarter, quarter, quarter, quarter], axis=0)
    spot_copy.wait()

    def pairs_of(n):
        tops = [spot_ref[4 + side, 32 * group + n] for side in range(2)]
        return tops, [spot_ref[2 + side, top] for top in tops for side in range(2)]

    upper_half = sub < 4

    def build_table(m):
        pairs = [pairs_of(2 * m + u)[1] for u in range(2)]
        places = jnp.where(
            upper_half,
            jnp.where(first, pairs[0][0], pairs[0][2]),
            jnp.where(first, pairs[1][0], pairs[1][2]),
        )
        table = both_own
        for k in range(4):
            table = table + lanes_of(factor_ref[k], places) * pattern_ref[k]
        table_ref[m] = table

    def build_tables(m, _):
        for u in range(BUILD):
            build_table(BUILD * m + u)
        return 0

    lax.fori_loop(0, 16 // BUILD, build_tables, 0)

    def codes_of(pair):
        return [codes_ref[pl.ds(spot_ref[side, pair], 8, stride=8), :] for side in range(2)]

    def chosen_pair(pair):
        left, right = codes_of(pair)
        same = left == right
        left_is = [left == i for i in range(STATES)]
        right_is = [right == i for i in range(STATES)]
        found = []
        for c in range(CLS):
            pi = [pi_ref[c, i] for i in range(STATES)]
            left_pi = pick(left_is, pi)
            right_pi = pick(right_is, pi)
            left_step = rate4_ref[4 + c, pair] * left_pi
            right_step = rate4_ref[c, pair] * right_pi
            base = rate4_ref[8 + c, pair] * (left_pi * right_pi)
            base = base + jnp.where(same, rate4_ref[12 + c, pair] * left_pi, 0.0)
            at_right = base + left_step
            at_left = base + right_step
            at_left = jnp.where(same, at_left + (left_step + 1.0), at_left)
            found.append(
                [
                    jnp.where(left_is[i], at_left, jnp.where(right_is[i], at_right, base))
                    for i in range(STATES)
                ]
            )
        return found

    def small_tree(m, u):
        n = 2 * m + u
        tops, pairs = pairs_of(n)
        tables = [
            jnp.broadcast_to(table_ref[m, 4 * u + c : 4 * u + c + 1, :], TILE) for c in range(CLS)
        ]
        halves = []
        for h in range(2):
            sides = codes_of(pairs[2 * h])
            code = lax.shift_left(sides[0], 2) + sides[1] + 64 * h
            looked = []
            for i in range(STATES):
                place = code + 16 * i if i else code
                looked.append([lanes_of(tables[c], place) for c in range(CLS)])
            chosen = chosen_pair(pairs[2 * h + 1])
            parts = []
            for c in range(CLS):
                pi = [pi_ref[c, i] for i in range(STATES)]
                values = [looked[i][c] * chosen[c][i] for i in range(STATES)]
                parts.append(moved(values, step_ref[c, tops[h]], mean_state(pi, values)))
            halves.append(parts)
        for c in range(CLS):
            pi = [pi_ref[c, i] for i in range(STATES)]
            values = product(halves[0][c], halves[1][c])
            average = mean_state(pi, values)
            inverse = 1.0 / average
            own_rate = step_ref[4 + c, 32 * group + n]
            for i in range(STATES):
                mid_ref[n, c, i] = values[i] * inverse + own_rate
            log_ref[n, c] = jnp.log(average)

    def small_trees(m, _):
        for u in range(8):
            small_tree(4 * m + u // 2, u % 2)
        return 0

    def tail_pair(at):
        return [spot_ref[6 + side, at] for side in range(2)]

    def clade(j, _):
        tops = [top - 1920 for top in tail_pair(96 + 4 * group + j)]
        pairs = [pair - 1920 for top in tops for pair in tail_pair(top)]
        leaves = [leaf - 1792 - group * 32 for pair in pairs for leaf in tail_pair(pair)]
        for c in range(CLS):
            pi = [pi_ref[c, i] for i in range(STATES)]
            scale = log_ref[leaves[0], c]
            for leaf in leaves[1:]:
                scale = scale + log_ref[leaf, c]
            halves = []
            for h in range(2):
                quads = []
                for at in (2 * h, 2 * h + 1):
                    joined = [
                        mid_ref[leaves[2 * at], c, i] * mid_ref[leaves[2 * at + 1], c, i]
                        for i in range(STATES)
                    ]
                    quads.append(moved(joined, step_ref[8 + c, pairs[at]], mean_state(pi, joined)))
                joined = product(quads[0], quads[1])
                halves.append(moved(joined, step_ref[8 + c, tops[h]], mean_state(pi, joined)))
            joined = product(halves[0], halves[1])
            inverse = 1.0 / joined[3]
            sent = [joined[0] * inverse, joined[1] * inverse, joined[2] * inverse]
            sent.append(scale + jnp.log(joined[3]))
            for v in range(4):
                for q in range(4):
                    out_ref[lax.bitwise_and(q - group, 3), j, v, 2 * c : 2 * c + 2, :] = sent[v][2 * q : 2 * q + 2, :]
        return 0

    step_copy.wait()
    rate4_copy.wait()
    for load in loads:
        load.wait()
    lax.fori_loop(0, 4, small_trees, 0)
    lax.fori_loop(0, 4, clade, 0)


def upper_kernel(
    child_ref, own_ref, one_ref, two_ref, three_ref, top_ref, site_hbm, part_ref, node_ref, site_ref, sem
):
    group = lax.axis_index("cls")
    pi = [top_ref[TOP_PI + i] for i in range(STATES)]
    scale = top_ref[TOP_CONST]
    for hop, piece_ref in enumerate((own_ref, one_ref, two_ref, three_ref)):
        source = 4 * lax.bitwise_and(group - hop, 3)
        for j in range(4):
            values = [piece_ref[j, 0], piece_ref[j, 1], piece_ref[j, 2]]
            scale = scale + piece_ref[j, 3]
            average = (pi[0] * values[0] + pi[1] * values[1]) + (pi[2] * values[2] + pi[3])
            step = top_ref[TOP_RATES + source + j] * average
            for i in range(3):
                node_ref[source + j, i] = values[i] + step
            node_ref[source + j, 3] = step + 1.0
    at = 16
    for level, count in ((6, 8), (7, 4), (8, 2), (9, 1)):
        begin = 1024 - (1024 >> level)
        for k in range(count):
            left = child_ref[0, begin + k] - 2016
            right = child_ref[1, begin + k] - 2016
            joined = [node_ref[left, i] * node_ref[right, i] for i in range(STATES)]
            average = mean_state(pi, joined)
            if level == 6:
                scale = scale + jnp.log(average)
                inverse = 1.0 / average
                for i in range(STATES):
                    node_ref[at, i] = joined[i] * inverse + top_ref[TOP_RATES + at]
            elif level < 9:
                step = top_ref[TOP_RATES + at] * average
                for i in range(STATES):
                    node_ref[at, i] = joined[i] + step
            else:
                scale = scale + jnp.log(average)
            at += 1
    top = jnp.maximum(scale, pltpu.roll(scale, 2, 0))
    top = jnp.maximum(top, pltpu.roll(top, 4, 0))
    share = jnp.exp(scale - top)
    mass = share + pltpu.roll(share, 2, 0)
    mass = mass + pltpu.roll(mass, 4, 0)
    total = top + jnp.log(mass)
    site_ref[...] = total[0:2] * (1.0 / 1024.0)
    site_copy = pltpu.make_async_copy(site_ref, site_hbm, sem)
    site_copy.start()
    weight = top_ref[TOP_WEIGHT]
    classes = weight * (share / mass)
    row = lax.broadcasted_iota(jnp.int32, TILE, 0)
    column = lax.broadcasted_iota(jnp.int32, TILE, 1)
    by_row = [
        jnp.sum(values, axis=1, keepdims=True) for values in (classes, weight * total, weight)
    ]
    by_pair = lax.shift_right_logical(row, 1)
    line = jnp.where(by_pair == column, by_row[0], 0.0)
    line = jnp.where((column == 4) & (row < 2), by_row[1], line)
    line = jnp.where((column == 5) & (row < 2), by_row[2], line)
    line = jnp.sum(line, axis=0, keepdims=True)
    for k in range(16):
        part_ref[8 * k : 8 * k + 8, :] = jnp.broadcast_to(line, TILE)
    site_copy.wait()


def last_kernel(every_ref, own_hbm, mean_hbm, own_ref, mean_ref, sems):
    group = lax.axis_index("cls")
    sums = every_ref[0:8, :]
    for k in range(1, 16):
        sums = sums + every_ref[8 * k : 8 * k + 8, :]
    sums = jnp.sum(sums, axis=0, keepdims=True)
    column = lax.broadcasted_iota(jnp.int32, (1, 128), 1)

    def entry(at):
        return jnp.sum(jnp.where(column == at, sums, 0.0), axis=1, keepdims=True)

    count = entry(5)
    own_ref[...] = entry(group) / count
    mean_ref[...] = entry(4) / (count * 1024.0)
    own_copy = pltpu.make_async_copy(own_ref, own_hbm, sems.at[0])
    mean_copy = pltpu.make_async_copy(mean_ref, mean_hbm, sems.at[1])
    own_copy.start()
    mean_copy.start()
    own_copy.wait()
    mean_copy.wait()


def per_device(tip_codes, counts, children, lengths, frequencies, weights):
    codes = tip_codes.reshape(32, 8, 8, 128).transpose(0, 2, 1, 3).reshape(2048, 128)
    child_rows = children.T
    smem = pl.BlockSpec(memory_space=SMEM)
    vmem = pl.BlockSpec(memory_space=VMEM)
    hbm = pl.BlockSpec(memory_space=pltpu.MemorySpace.HBM)
    ours, top = pl.pallas_call(
        lower_kernel,
        out_shape=(pltpu.VMEM((4, 4, 4, 8, 128), FLOAT), pltpu.VMEM((TOP_ROWS, 8, 128), FLOAT)),
        in_specs=[hbm] * 6,
        out_specs=(vmem, vmem),
        scratch_shapes=[
            pltpu.VMEM((2, 1023), jnp.int32),
            pltpu.SMEM((4, 4), FLOAT),
            pltpu.SMEM((4,), FLOAT),
            pltpu.VMEM((4, 2046), FLOAT),
            pltpu.VMEM((2048, 128), jnp.int32),
            pltpu.VMEM(TILE, jnp.int32),
            pltpu.VMEM((4, 2048), FLOAT),
            pltpu.VMEM(TILE, jnp.int32),
            pltpu.SMEM(TILE, jnp.int32),
            pltpu.VMEM((16, 128), FLOAT),
            pltpu.SMEM((16, 128), FLOAT),
            pltpu.VMEM((CLS, STATES, 8, 128), FLOAT),
            pltpu.VMEM((4, 8, 128), FLOAT),
            pltpu.VMEM((4, 8, 128), FLOAT),
            pltpu.VMEM((16, 8, 128), FLOAT),
            pltpu.VMEM((16, 128), FLOAT),
            pltpu.SMEM((16, 128), FLOAT),
            pltpu.VMEM((32, CLS, STATES, 8, 128), FLOAT),
            pltpu.VMEM((32, CLS, 8, 128), FLOAT),
            pltpu.SemaphoreType.DMA((12,)),
        ],
        compiler_params=pltpu.CompilerParams(vmem_limit_bytes=16 * 1024 * 1024),
        name="lower_tree",
    )(
        *(
            pltpu.with_memory_space_constraint(array, pltpu.MemorySpace.HBM)
            for array in (child_rows, frequencies, weights, lengths, codes, counts.reshape(8, 128))
        )
    )
    pieces = [ours[0]]
    for hop in range(1, 4):
        pieces.append(lax.ppermute(ours[hop], "cls", [(k, (k + hop) % 4) for k in range(4)]))
    site, part = pl.pallas_call(
        upper_kernel,
        out_shape=(jax.ShapeDtypeStruct((2, 128), FLOAT), pltpu.VMEM((128, 128), FLOAT)),
        in_specs=[smem] + [vmem] * 5,
        out_specs=(hbm, vmem),
        scratch_shapes=[
            pltpu.VMEM((32, STATES, 8, 128), FLOAT),
            pltpu.VMEM((2, 128), FLOAT),
            pltpu.SemaphoreType.DMA,
        ],
        compiler_params=pltpu.CompilerParams(vmem_limit_bytes=16 * 1024 * 1024),
        name="upper_tree",
    )(child_rows, *pieces, top)
    every = lax.all_to_all(part, ("cls", "site"), split_axis=0, concat_axis=0, tiled=True)
    own, mean = pl.pallas_call(
        last_kernel,
        out_shape=(jax.ShapeDtypeStruct((1, 1), FLOAT), jax.ShapeDtypeStruct((1, 1), FLOAT)),
        in_specs=[vmem],
        out_specs=(hbm, hbm),
        scratch_shapes=[
            pltpu.VMEM((1, 1), FLOAT),
            pltpu.VMEM((1, 1), FLOAT),
            pltpu.SemaphoreType.DMA((2,)),
        ],
        compiler_params=pltpu.CompilerParams(vmem_limit_bytes=16 * 1024 * 1024),
        name="last_sums",
    )(every)
    return site.reshape(1, 256), own.reshape(1), mean.reshape(())


def solution(mesh):
    return jax.shard_map(
        per_device,
        mesh=mesh,
        in_specs=(P("cls", "site"), P("site"), P(), P(), P(), P()),
        out_specs=(P("cls", "site"), P("cls"), P()),
        check_vma=False,
    )
```

```python
import jax
import jax.numpy as jnp
from jax import lax
from jax.experimental import pallas as pl
from jax.experimental.pallas import tpu as pltpu
from jax.sharding import PartitionSpec as P

CLS = 4
STATES = 4
FLOAT = jnp.float32
SMEM = pltpu.MemorySpace.SMEM
VMEM = pltpu.MemorySpace.VMEM
TILE = (8, 128)
BUILD = 8
TOP_RATES, TOP_PI, TOP_CONST, TOP_WEIGHT, TOP_ROWS = 0, 30, 34, 35, 36


def mean_state(pi, values):
    return (pi[0] * values[0] + pi[1] * values[1]) + (pi[2] * values[2] + pi[3] * values[3])


def moved(values, rate, average):
    step = rate * average
    return [value + step for value in values]


def product(left, right):
    return [a * b for a, b in zip(left, right)]


def choose(selector, options):
    value = jnp.where(selector == 1, options[1], options[0])
    value = jnp.where(selector == 2, options[2], value)
    return jnp.where(selector == 3, options[3], value)


def pick(masks, options):
    value = jnp.where(masks[1], options[1], options[0])
    value = jnp.where(masks[2], options[2], value)
    return jnp.where(masks[3], options[3], value)


def lanes_of(rows, places):
    return jnp.take_along_axis(rows, places, axis=1, mode="promise_in_bounds")


def lower_kernel(
    child_hbm, freq_hbm, weight_hbm, lengths_hbm, codes_hbm, counts_hbm,
    out_ref, top_ref, place_ref,
    child_vec, freq_ref, weight_ref, lengths_ref, codes_ref, counts_ref, rate_vec,
    spot_vec, spot_ref, step_vec, step_ref,
    pi_ref, pattern_ref, factor_ref, table_ref, rate4_vec, rate4_ref, mid_ref, log_ref, sems,
):
    group = lax.axis_index("cls")
    small = [
        pltpu.make_async_copy(source, target, sems.at[4 + k])
        for k, (source, target) in enumerate(
            (
                (child_hbm, child_vec),
                (lengths_hbm, lengths_ref),
                (freq_hbm, freq_ref),
                (weight_hbm, weight_ref),
                (counts_hbm, counts_ref),
            )
        )
    ]
    for load in small:
        load.start()
    loads = [
        pltpu.make_async_copy(
            codes_hbm.at[pl.ds(512 * j, 512)], codes_ref.at[pl.ds(512 * j, 512)], sems.at[j]
        )
        for j in range(4)
    ]
    for load in loads:
        load.start()
    small[0].wait()
    half = lax.shift_right_logical(group, 1)

    def block(ref, start):
        return ref[:, pl.ds(pl.multiple_of(start, 128), 128)]

    local = block(child_vec, 128 * group) - 256 * group
    spot_vec[0:2] = lax.shift_left(lax.shift_right_logical(local, 3), 6) + lax.bitwise_and(local, 7)
    spot_vec[2:4] = block(child_vec, 512 + 128 * half) - (1024 + 128 * group)
    spot_vec[4:6] = child_vec[:, 768:896] - (1536 + 128 * half)
    spot_vec[6:8] = jnp.concatenate([child_vec[:, 896:1023], jnp.zeros((2, 1), jnp.int32)], axis=1)
    spot_copy = pltpu.make_async_copy(spot_vec, spot_ref, sems.at[9])
    spot_copy.start()
    for load in small[1:]:
        load.wait()

    lane = lax.broadcasted_iota(jnp.int32, TILE, 1)
    sub = lax.broadcasted_iota(jnp.int32, TILE, 0)
    by_pair = lax.shift_right_logical(sub, 1)
    by_class = lax.bitwise_and(sub, 3)
    uniform, betas = [], []
    for c in range(CLS):
        raw = [jnp.full(TILE, freq_ref[c, i], FLOAT) for i in range(STATES)]
        inverse = 1.0 / ((raw[0] + raw[1]) + (raw[2] + raw[3]))
        uniform.append([value * inverse for value in raw])
        betas.append(1.0 / (1.0 - mean_state(uniform[c], uniform[c])))
        for i in range(STATES):
            pi_ref[c, i] = uniform[c][i]
    beta_rows = choose(by_class, betas)[:4]
    total = jnp.zeros((4, 128), FLOAT)
    for k in range(16):
        width = min(128, 2046 - 128 * k)
        part = lengths_ref[:, 128 * k : 128 * k + width]
        if width < 128:
            part = jnp.concatenate([part, jnp.zeros((4, 128 - width), FLOAT)], axis=1)
        total = total + part
        rate_vec[:, 128 * k : 128 * k + 128] = jnp.exp(beta_rows * part) - 1.0

    step_vec[0:4] = block(rate_vec, 1536 + 128 * half)
    step_vec[4:8] = rate_vec[:, 1792:1920]
    step_vec[8:12] = rate_vec[:, 1920:2048]
    step_vec[12:16] = jnp.zeros((4, 128), FLOAT)
    step_copy = pltpu.make_async_copy(step_vec, step_ref, sems.at[10])
    step_copy.start()

    def twice(rows):
        return jnp.concatenate([rows, rows], axis=0)

    low = twice(block(rate_vec, 256 * group))
    high = twice(block(rate_vec, 256 * group + 128))
    own = twice(block(rate_vec, 1024 + 128 * group))

    def rates_at(places):
        places = jnp.broadcast_to(places, TILE)
        inside = lax.bitwise_and(places, 127)
        return jnp.where(places < 128, lanes_of(low, inside), lanes_of(high, inside))

    left = rates_at(local[0:1])
    right = rates_at(local[1:2])
    both = left * right
    factor_ref[0] = right
    factor_ref[1] = left
    factor_ref[2] = both + own * (left + right + both)
    factor_ref[3] = own
    for k in range(4):
        rate4_vec[4 * k : 4 * k + 4] = factor_ref[k, 0:4]
    rate4_copy = pltpu.make_async_copy(rate4_vec, rate4_ref, sems.at[11])
    rate4_copy.start()

    own_state = lax.bitwise_and(lax.shift_right_logical(lane, 4), 3)
    left_code = lax.bitwise_and(lax.shift_right_logical(lane, 2), 3)
    right_code = lax.bitwise_and(lane, 3)
    left_own = own_state == left_code
    right_own = own_state == right_code
    first = lane < 64
    both_own = jnp.where(left_own, jnp.where(right_own, 1.0, 0.0), 0.0)
    by_rows = [choose(by_class, [uniform[c][i] for c in range(CLS)]) for i in range(STATES)]
    left_pi = choose(left_code, by_rows)
    right_pi = choose(right_code, by_rows)
    pattern_ref[0] = jnp.where(left_own, right_pi, 0.0)
    pattern_ref[1] = jnp.where(right_own, left_pi, 0.0)
    pattern_ref[2] = left_pi * right_pi
    pattern_ref[3] = jnp.where(left_code == right_code, left_pi, 0.0)

    for i in range(STATES):
        top_ref[TOP_PI + i] = choose(by_pair, [uniform[c][i] for c in range(CLS)])
    beta_pairs = choose(by_pair, betas)
    sums = choose(by_pair, [jnp.broadcast_to(total[c : c + 1], TILE) for c in range(CLS)])
    sums = jnp.broadcast_to(jnp.sum(sums, axis=1, keepdims=True), TILE)
    weights = [jnp.full(TILE, weight_ref[c], FLOAT) for c in range(CLS)]
    weight_sum = (weights[0] + weights[1]) + (weights[2] + weights[3])
    top_ref[TOP_CONST] = jnp.log(choose(by_pair, weights) / weight_sum) - beta_pairs * sums
    last = rate_vec[:, 1920:2048]
    last = choose(by_pair, [jnp.broadcast_to(last[c : c + 1], TILE) for c in range(CLS)])
    for k in range(30):
        top_ref[TOP_RATES + k] = jnp.broadcast_to(last[:, 96 + k : 97 + k], TILE)
    quarter = counts_ref[pl.ds(2 * group, 2), :].astype(FLOAT)
    top_ref[TOP_WEIGHT] = jnp.concatenate([quarter, quarter, quarter, quarter], axis=0)
    spot_copy.wait()

    for k in range(15):
        for side in range(2):
            place_ref[2 * k + side] = spot_ref[6 + side, 112 + k] - 2016

    def pairs_of(n):
        tops = [spot_ref[4 + side, 32 * group + n] for side in range(2)]
        return tops, [spot_ref[2 + side, top] for top in tops for side in range(2)]

    upper_half = sub < 4

    def build_table(m):
        pairs = [pairs_of(2 * m + u)[1] for u in range(2)]
        places = jnp.where(
            upper_half,
            jnp.where(first, pairs[0][0], pairs[0][2]),
            jnp.where(first, pairs[1][0], pairs[1][2]),
        )
        table = both_own
        for k in range(4):
            table = table + lanes_of(factor_ref[k], places) * pattern_ref[k]
        table_ref[m] = table

    def build_tables(m, _):
        for u in range(BUILD):
            build_table(BUILD * m + u)
        return 0

    lax.fori_loop(0, 16 // BUILD, build_tables, 0)

    def codes_of(pair):
        return [codes_ref[pl.ds(spot_ref[side, pair], 8, stride=8), :] for side in range(2)]

    def chosen_pair(pair):
        left, right = codes_of(pair)
        same = left == right
        left_is = [left == i for i in range(STATES)]
        right_is = [right == i for i in range(STATES)]
        found = []
        for c in range(CLS):
            pi = [pi_ref[c, i] for i in range(STATES)]
            left_pi = pick(left_is, pi)
            right_pi = pick(right_is, pi)
            left_step = rate4_ref[4 + c, pair] * left_pi
            right_step = rate4_ref[c, pair] * right_pi
            base = rate4_ref[8 + c, pair] * (left_pi * right_pi)
            base = base + jnp.where(same, rate4_ref[12 + c, pair] * left_pi, 0.0)
            at_right = base + left_step
            at_left = base + right_step
            at_left = jnp.where(same, at_left + (left_step + 1.0), at_left)
            found.append(
                [
                    jnp.where(left_is[i], at_left, jnp.where(right_is[i], at_right, base))
                    for i in range(STATES)
                ]
            )
        return found

    def small_tree(m, u):
        n = 2 * m + u
        tops, pairs = pairs_of(n)
        tables = [
            jnp.broadcast_to(table_ref[m, 4 * u + c : 4 * u + c + 1, :], TILE) for c in range(CLS)
        ]
        halves = []
        for h in range(2):
            sides = codes_of(pairs[2 * h])
            code = lax.shift_left(sides[0], 2) + sides[1] + 64 * h
            looked = []
            for i in range(STATES):
                place = code + 16 * i if i else code
                looked.append([lanes_of(tables[c], place) for c in range(CLS)])
            chosen = chosen_pair(pairs[2 * h + 1])
            parts = []
            for c in range(CLS):
                pi = [pi_ref[c, i] for i in range(STATES)]
                values = [looked[i][c] * chosen[c][i] for i in range(STATES)]
                parts.append(moved(values, step_ref[c, tops[h]], mean_state(pi, values)))
            halves.append(parts)
        for c in range(CLS):
            pi = [pi_ref[c, i] for i in range(STATES)]
            values = product(halves[0][c], halves[1][c])
            average = mean_state(pi, values)
            inverse = 1.0 / average
            own_rate = step_ref[4 + c, 32 * group + n]
            for i in range(STATES):
                mid_ref[n, c, i] = values[i] * inverse + own_rate
            log_ref[n, c] = jnp.log(average)

    def small_trees(m, _):
        for u in range(8):
            small_tree(4 * m + u // 2, u % 2)
        return 0

    def tail_pair(at):
        return [spot_ref[6 + side, at] for side in range(2)]

    def clade(j, _):
        tops = [top - 1920 for top in tail_pair(96 + 4 * group + j)]
        pairs = [pair - 1920 for top in tops for pair in tail_pair(top)]
        leaves = [leaf - 1792 - group * 32 for pair in pairs for leaf in tail_pair(pair)]
        for c in range(CLS):
            pi = [pi_ref[c, i] for i in range(STATES)]
            scale = log_ref[leaves[0], c]
            for leaf in leaves[1:]:
                scale = scale + log_ref[leaf, c]
            halves = []
            for h in range(2):
                quads = []
                for at in (2 * h, 2 * h + 1):
                    joined = [
                        mid_ref[leaves[2 * at], c, i] * mid_ref[leaves[2 * at + 1], c, i]
                        for i in range(STATES)
                    ]
                    quads.append(moved(joined, step_ref[8 + c, pairs[at]], mean_state(pi, joined)))
                joined = product(quads[0], quads[1])
                halves.append(moved(joined, step_ref[8 + c, tops[h]], mean_state(pi, joined)))
            joined = product(halves[0], halves[1])
            inverse = 1.0 / joined[3]
            sent = [joined[0] * inverse, joined[1] * inverse, joined[2] * inverse]
            sent.append(scale + jnp.log(joined[3]))
            for v in range(4):
                for q in range(4):
                    out_ref[lax.bitwise_and(q - group, 3), j, v, 2 * c : 2 * c + 2, :] = sent[v][2 * q : 2 * q + 2, :]
        return 0

    step_copy.wait()
    rate4_copy.wait()
    for load in loads:
        load.wait()
    lax.fori_loop(0, 4, small_trees, 0)
    lax.fori_loop(0, 4, clade, 0)


def upper_kernel(
    place_ref, own_ref, one_ref, two_ref, three_ref, top_ref, site_ref, part_ref, node_ref
):
    group = lax.axis_index("cls")
    pi = [top_ref[TOP_PI + i] for i in range(STATES)]
    scale = top_ref[TOP_CONST]
    for hop, piece_ref in enumerate((own_ref, one_ref, two_ref, three_ref)):
        source = 4 * lax.bitwise_and(group - hop, 3)
        for j in range(4):
            values = [piece_ref[j, 0], piece_ref[j, 1], piece_ref[j, 2]]
            scale = scale + piece_ref[j, 3]
            average = (pi[0] * values[0] + pi[1] * values[1]) + (pi[2] * values[2] + pi[3])
            step = top_ref[TOP_RATES + source + j] * average
            for i in range(3):
                node_ref[source + j, i] = values[i] + step
            node_ref[source + j, 3] = step + 1.0
    at = 16
    for level, count in ((6, 8), (7, 4), (8, 2), (9, 1)):
        for k in range(count):
            left = place_ref[2 * (at - 16)]
            right = place_ref[2 * (at - 16) + 1]
            joined = [node_ref[left, i] * node_ref[right, i] for i in range(STATES)]
            average = mean_state(pi, joined)
            if level == 6:
                scale = scale + jnp.log(average)
                inverse = 1.0 / average
                for i in range(STATES):
                    node_ref[at, i] = joined[i] * inverse + top_ref[TOP_RATES + at]
            elif level < 9:
                step = top_ref[TOP_RATES + at] * average
                for i in range(STATES):
                    node_ref[at, i] = joined[i] + step
            else:
                scale = scale + jnp.log(average)
            at += 1
    top = jnp.maximum(scale, pltpu.roll(scale, 2, 0))
    top = jnp.maximum(top, pltpu.roll(top, 4, 0))
    share = jnp.exp(scale - top)
    mass = share + pltpu.roll(share, 2, 0)
    mass = mass + pltpu.roll(mass, 4, 0)
    total = top + jnp.log(mass)
    site_ref[...] = total[0:2] * (1.0 / 1024.0)
    weight = top_ref[TOP_WEIGHT]
    classes = weight * (share / mass)
    row = lax.broadcasted_iota(jnp.int32, TILE, 0)
    column = lax.broadcasted_iota(jnp.int32, TILE, 1)
    by_row = [
        jnp.sum(values, axis=1, keepdims=True) for values in (classes, weight * total, weight)
    ]
    by_pair = lax.shift_right_logical(row, 1)
    line = jnp.where(by_pair == column, by_row[0], 0.0)
    line = jnp.where((column == 4) & (row < 2), by_row[1], line)
    line = jnp.where((column == 5) & (row < 2), by_row[2], line)
    line = jnp.sum(line, axis=0, keepdims=True)
    for k in range(16):
        part_ref[8 * k : 8 * k + 8, :] = jnp.broadcast_to(line, TILE)


def last_kernel(every_ref, site_ref, own_hbm, mean_hbm, site_hbm, own_ref, mean_ref, sems):
    site_copy = pltpu.make_async_copy(site_ref, site_hbm, sems.at[2])
    site_copy.start()
    group = lax.axis_index("cls")
    sums = every_ref[0:8, :]
    for k in range(1, 16):
        sums = sums + every_ref[8 * k : 8 * k + 8, :]
    sums = jnp.sum(sums, axis=0, keepdims=True)
    column = lax.broadcasted_iota(jnp.int32, (1, 128), 1)

    def entry(at):
        return jnp.sum(jnp.where(column == at, sums, 0.0), axis=1, keepdims=True)

    count = entry(5)
    own_ref[...] = entry(group) / count
    mean_ref[...] = entry(4) / (count * 1024.0)
    own_copy = pltpu.make_async_copy(own_ref, own_hbm, sems.at[0])
    mean_copy = pltpu.make_async_copy(mean_ref, mean_hbm, sems.at[1])
    own_copy.start()
    mean_copy.start()
    own_copy.wait()
    mean_copy.wait()
    site_copy.wait()


def per_device(tip_codes, counts, children, lengths, frequencies, weights):
    codes = tip_codes.reshape(32, 8, 8, 128).transpose(0, 2, 1, 3).reshape(2048, 128)
    child_rows = children.T
    smem = pl.BlockSpec(memory_space=SMEM)
    vmem = pl.BlockSpec(memory_space=VMEM)
    hbm = pl.BlockSpec(memory_space=pltpu.MemorySpace.HBM)
    ours, top, places = pl.pallas_call(
        lower_kernel,
        out_shape=(pltpu.VMEM((4, 4, 4, 8, 128), FLOAT), pltpu.VMEM((TOP_ROWS, 8, 128), FLOAT), pltpu.SMEM((32,), jnp.int32)),
        in_specs=[hbm] * 6,
        out_specs=(vmem, vmem, smem),
        scratch_shapes=[
            pltpu.VMEM((2, 1023), jnp.int32),
            pltpu.SMEM((4, 4), FLOAT),
            pltpu.SMEM((4,), FLOAT),
            pltpu.VMEM((4, 2046), FLOAT),
            pltpu.VMEM((2048, 128), jnp.int32),
            pltpu.VMEM(TILE, jnp.int32),
            pltpu.VMEM((4, 2048), FLOAT),
            pltpu.VMEM(TILE, jnp.int32),
            pltpu.SMEM(TILE, jnp.int32),
            pltpu.VMEM((16, 128), FLOAT),
            pltpu.SMEM((16, 128), FLOAT),
            pltpu.VMEM((CLS, STATES, 8, 128), FLOAT),
            pltpu.VMEM((4, 8, 128), FLOAT),
            pltpu.VMEM((4, 8, 128), FLOAT),
            pltpu.VMEM((16, 8, 128), FLOAT),
            pltpu.VMEM((16, 128), FLOAT),
            pltpu.SMEM((16, 128), FLOAT),
            pltpu.VMEM((32, CLS, STATES, 8, 128), FLOAT),
            pltpu.VMEM((32, CLS, 8, 128), FLOAT),
            pltpu.SemaphoreType.DMA((12,)),
        ],
        compiler_params=pltpu.CompilerParams(vmem_limit_bytes=16 * 1024 * 1024),
        name="lower_tree",
    )(
        *(
            pltpu.with_memory_space_constraint(array, pltpu.MemorySpace.HBM)
            for array in (child_rows, frequencies, weights, lengths, codes, counts.reshape(8, 128))
        )
    )
    pieces = [ours[0]]
    for hop in range(1, 4):
        pieces.append(lax.ppermute(ours[hop], "cls", [(k, (k + hop) % 4) for k in range(4)]))
    site, part = pl.pallas_call(
        upper_kernel,
        out_shape=(pltpu.VMEM((2, 128), FLOAT), pltpu.VMEM((128, 128), FLOAT)),
        in_specs=[smem] + [vmem] * 5,
        out_specs=(vmem, vmem),
        scratch_shapes=[pltpu.VMEM((32, STATES, 8, 128), FLOAT)],
        compiler_params=pltpu.CompilerParams(vmem_limit_bytes=16 * 1024 * 1024),
        name="upper_tree",
    )(places, *pieces, top)
    every = lax.all_to_all(part, ("cls", "site"), split_axis=0, concat_axis=0, tiled=True)
    own, mean, site = pl.pallas_call(
        last_kernel,
        out_shape=tuple(jax.ShapeDtypeStruct(shape, FLOAT) for shape in ((1, 1), (1, 1), (2, 128))),
        in_specs=[vmem, vmem],
        out_specs=(hbm, hbm, hbm),
        scratch_shapes=[
            pltpu.VMEM((1, 1), FLOAT),
            pltpu.VMEM((1, 1), FLOAT),
            pltpu.SemaphoreType.DMA((3,)),
        ],
        compiler_params=pltpu.CompilerParams(vmem_limit_bytes=16 * 1024 * 1024),
        name="last_sums",
    )(every, site)
    return site.reshape(1, 256), own.reshape(1), mean.reshape(())


def solution(mesh):
    return jax.shard_map(
        per_device,
        mesh=mesh,
        in_specs=(P("cls", "site"), P("site"), P(), P(), P(), P()),
        out_specs=(P("cls", "site"), P("cls"), P()),
        check_vma=False,
    )
```

```python
import jax
import jax.numpy as jnp
from jax import lax
from jax.experimental import pallas as pl
from jax.experimental.pallas import tpu as pltpu
from jax.sharding import PartitionSpec as P

CLS = 4
STATES = 4
FLOAT = jnp.float32
SMEM = pltpu.MemorySpace.SMEM
VMEM = pltpu.MemorySpace.VMEM
TILE = (8, 128)
BUILD = 8
TOP_RATES, TOP_PI, TOP_CONST, TOP_WEIGHT, TOP_ROWS = 0, 30, 34, 35, 36


def mean_state(pi, values):
    return (pi[0] * values[0] + pi[1] * values[1]) + (pi[2] * values[2] + pi[3] * values[3])


def mean_by_last(ratios, values):
    return (ratios[0] * values[0] + ratios[1] * values[1]) + (ratios[2] * values[2] + values[3])


def moved(values, rate, average):
    step = rate * average
    return [value + step for value in values]


def product(left, right):
    return [a * b for a, b in zip(left, right)]


def choose(selector, options):
    value = jnp.where(selector == 1, options[1], options[0])
    value = jnp.where(selector == 2, options[2], value)
    return jnp.where(selector == 3, options[3], value)


def pick(masks, options):
    value = jnp.where(masks[1], options[1], options[0])
    value = jnp.where(masks[2], options[2], value)
    return jnp.where(masks[3], options[3], value)


def lanes_of(rows, places):
    return lax.gather(
        rows,
        places[..., None],
        lax.GatherDimensionNumbers(
            offset_dims=(),
            collapsed_slice_dims=(1,),
            start_index_map=(1,),
            operand_batching_dims=(0,),
            start_indices_batching_dims=(0,),
        ),
        slice_sizes=(1, 1),
        mode=lax.GatherScatterMode.PROMISE_IN_BOUNDS,
    )


def lower_kernel(
    child_hbm, freq_hbm, weight_hbm, lengths_hbm, codes_hbm, counts_hbm,
    out_ref, top_ref, place_ref,
    child_vec, freq_ref, weight_ref, lengths_ref, codes_ref, counts_ref, rate_vec,
    spot_vec, spot_ref, step_vec, step_ref,
    pi_ref, ratio_ref, pattern_ref, factor_ref, table_ref, rate4_vec, rate4_ref, mid_ref, log_ref, sems,
):
    group = lax.axis_index("cls")
    small = [
        pltpu.make_async_copy(source, target, sems.at[4 + k])
        for k, (source, target) in enumerate(
            (
                (child_hbm, child_vec),
                (lengths_hbm, lengths_ref),
                (freq_hbm, freq_ref),
                (weight_hbm, weight_ref),
                (counts_hbm, counts_ref),
            )
        )
    ]
    for load in small:
        load.start()
    loads = [
        pltpu.make_async_copy(
            codes_hbm.at[pl.ds(512 * j, 512)], codes_ref.at[pl.ds(512 * j, 512)], sems.at[j]
        )
        for j in range(4)
    ]
    for load in loads:
        load.start()
    small[0].wait()
    half = lax.shift_right_logical(group, 1)

    def block(ref, start):
        return ref[:, pl.ds(pl.multiple_of(start, 128), 128)]

    local = block(child_vec, 128 * group) - 256 * group
    spot_vec[0:2] = lax.shift_left(lax.shift_right_logical(local, 3), 6) + lax.bitwise_and(local, 7)
    spot_vec[2:4] = block(child_vec, 512 + 128 * half) - (1024 + 128 * group)
    spot_vec[4:6] = child_vec[:, 768:896] - (1536 + 128 * half)
    spot_vec[6:8] = jnp.concatenate([child_vec[:, 896:1023], jnp.zeros((2, 1), jnp.int32)], axis=1)
    spot_copy = pltpu.make_async_copy(spot_vec, spot_ref, sems.at[9])
    spot_copy.start()
    for load in small[1:]:
        load.wait()

    lane = lax.broadcasted_iota(jnp.int32, TILE, 1)
    sub = lax.broadcasted_iota(jnp.int32, TILE, 0)
    by_pair = lax.shift_right_logical(sub, 1)
    by_class = lax.bitwise_and(sub, 3)
    uniform, betas = [], []
    for c in range(CLS):
        raw = [jnp.full(TILE, freq_ref[c, i], FLOAT) for i in range(STATES)]
        inverse = 1.0 / ((raw[0] + raw[1]) + (raw[2] + raw[3]))
        uniform.append([value * inverse for value in raw])
        betas.append(1.0 / (1.0 - mean_state(uniform[c], uniform[c])))
        for i in range(STATES):
            pi_ref[c, i] = uniform[c][i]
        for i in range(3):
            ratio_ref[c, i] = uniform[c][i] / uniform[c][3]
    beta_rows = choose(by_class, betas)[:4]
    total = jnp.zeros((4, 128), FLOAT)
    for k in range(16):
        width = min(128, 2046 - 128 * k)
        part = lengths_ref[:, 128 * k : 128 * k + width]
        if width < 128:
            part = jnp.concatenate([part, jnp.zeros((4, 128 - width), FLOAT)], axis=1)
        total = total + part
        rate_vec[:, 128 * k : 128 * k + 128] = jnp.exp(beta_rows * part) - 1.0

    last_pi = choose(by_class, [uniform[c][3] for c in range(CLS)])[:4]
    step_vec[0:4] = block(rate_vec, 1536 + 128 * half) * last_pi
    step_vec[4:8] = rate_vec[:, 1792:1920] * last_pi
    step_vec[8:12] = rate_vec[:, 1920:2048] * last_pi
    step_vec[12:16] = jnp.zeros((4, 128), FLOAT)
    step_copy = pltpu.make_async_copy(step_vec, step_ref, sems.at[10])
    step_copy.start()

    def twice(rows):
        return jnp.concatenate([rows, rows], axis=0)

    low = twice(block(rate_vec, 256 * group))
    high = twice(block(rate_vec, 256 * group + 128))
    own = twice(block(rate_vec, 1024 + 128 * group))

    def rates_at(places):
        places = jnp.broadcast_to(places, TILE)
        inside = lax.bitwise_and(places, 127)
        return jnp.where(places < 128, lanes_of(low, inside), lanes_of(high, inside))

    left = rates_at(local[0:1])
    right = rates_at(local[1:2])
    both = left * right
    factor_ref[0] = right
    factor_ref[1] = left
    factor_ref[2] = both + own * (left + right + both)
    factor_ref[3] = own
    for k in range(4):
        rate4_vec[4 * k : 4 * k + 4] = factor_ref[k, 0:4]
    rate4_copy = pltpu.make_async_copy(rate4_vec, rate4_ref, sems.at[11])
    rate4_copy.start()

    own_state = lax.bitwise_and(lax.shift_right_logical(lane, 4), 3)
    left_code = lax.bitwise_and(lax.shift_right_logical(lane, 2), 3)
    right_code = lax.bitwise_and(lane, 3)
    left_own = own_state == left_code
    right_own = own_state == right_code
    first = lane < 64
    both_own = jnp.where(left_own, jnp.where(right_own, 1.0, 0.0), 0.0)
    by_rows = [choose(by_class, [uniform[c][i] for c in range(CLS)]) for i in range(STATES)]
    left_pi = choose(left_code, by_rows)
    right_pi = choose(right_code, by_rows)
    pattern_ref[0] = jnp.where(left_own, right_pi, 0.0)
    pattern_ref[1] = jnp.where(right_own, left_pi, 0.0)
    pattern_ref[2] = left_pi * right_pi
    pattern_ref[3] = jnp.where(left_code == right_code, left_pi, 0.0)

    for i in range(STATES):
        top_ref[TOP_PI + i] = choose(by_pair, [uniform[c][i] for c in range(CLS)])
    beta_pairs = choose(by_pair, betas)
    sums = choose(by_pair, [jnp.broadcast_to(total[c : c + 1], TILE) for c in range(CLS)])
    sums = jnp.broadcast_to(jnp.sum(sums, axis=1, keepdims=True), TILE)
    weights = [jnp.full(TILE, weight_ref[c], FLOAT) for c in range(CLS)]
    weight_sum = (weights[0] + weights[1]) + (weights[2] + weights[3])
    top_ref[TOP_CONST] = jnp.log(choose(by_pair, weights) / weight_sum) - beta_pairs * sums
    last = rate_vec[:, 1920:2048]
    last = choose(by_pair, [jnp.broadcast_to(last[c : c + 1], TILE) for c in range(CLS)])
    for k in range(30):
        top_ref[TOP_RATES + k] = jnp.broadcast_to(last[:, 96 + k : 97 + k], TILE)
    quarter = counts_ref[pl.ds(2 * group, 2), :].astype(FLOAT)
    top_ref[TOP_WEIGHT] = jnp.concatenate([quarter, quarter, quarter, quarter], axis=0)
    spot_copy.wait()

    for k in range(15):
        for side in range(2):
            place_ref[2 * k + side] = spot_ref[6 + side, 112 + k] - 2016

    def pairs_of(n):
        tops = [spot_ref[4 + side, 32 * group + n] for side in range(2)]
        return tops, [spot_ref[2 + side, top] for top in tops for side in range(2)]

    upper_half = sub < 4

    def build_table(m):
        pairs = [pairs_of(2 * m + u)[1] for u in range(2)]
        places = jnp.where(
            upper_half,
            jnp.where(first, pairs[0][0], pairs[0][2]),
            jnp.where(first, pairs[1][0], pairs[1][2]),
        )
        table = both_own
        for k in range(4):
            table = table + lanes_of(factor_ref[k], places) * pattern_ref[k]
        table_ref[m] = table

    def build_tables(m, _):
        for u in range(BUILD):
            build_table(BUILD * m + u)
        return 0

    lax.fori_loop(0, 16 // BUILD, build_tables, 0)

    def codes_of(pair):
        return [codes_ref[pl.ds(spot_ref[side, pair], 8, stride=8), :] for side in range(2)]

    def chosen_pair(pair):
        left, right = codes_of(pair)
        same = left == right
        left_is = [left == i for i in range(STATES)]
        right_is = [right == i for i in range(STATES)]
        found = []
        for c in range(CLS):
            pi = [pi_ref[c, i] for i in range(STATES)]
            left_pi = pick(left_is, pi)
            right_pi = pick(right_is, pi)
            left_step = rate4_ref[4 + c, pair] * left_pi
            right_step = rate4_ref[c, pair] * right_pi
            base = rate4_ref[8 + c, pair] * (left_pi * right_pi)
            base = base + jnp.where(same, rate4_ref[12 + c, pair] * left_pi, 0.0)
            at_right = base + left_step
            at_left = base + right_step
            at_left = jnp.where(same, at_left + (left_step + 1.0), at_left)
            found.append(
                [
                    jnp.where(left_is[i], at_left, jnp.where(right_is[i], at_right, base))
                    for i in range(STATES)
                ]
            )
        return found

    def small_tree(m, u):
        n = 2 * m + u
        tops, pairs = pairs_of(n)
        tables = [
            jnp.broadcast_to(table_ref[m, 4 * u + c : 4 * u + c + 1, :], TILE) for c in range(CLS)
        ]
        halves = []
        for h in range(2):
            sides = codes_of(pairs[2 * h])
            code = lax.shift_left(sides[0], 2) + sides[1] + 64 * h
            looked = []
            for i in range(STATES):
                place = code + 16 * i if i else code
                looked.append([lanes_of(tables[c], place) for c in range(CLS)])
            chosen = chosen_pair(pairs[2 * h + 1])
            parts = []
            for c in range(CLS):
                ratios = [ratio_ref[c, i] for i in range(3)]
                values = [looked[i][c] * chosen[c][i] for i in range(STATES)]
                parts.append(moved(values, step_ref[c, tops[h]], mean_by_last(ratios, values)))
            halves.append(parts)
        for c in range(CLS):
            ratios = [ratio_ref[c, i] for i in range(3)]
            values = product(halves[0][c], halves[1][c])
            average = mean_by_last(ratios, values)
            inverse = 1.0 / average
            own_rate = step_ref[4 + c, 32 * group + n]
            for i in range(STATES):
                mid_ref[n, c, i] = values[i] * inverse + own_rate
            log_ref[n, c] = jnp.log(average)

    def small_trees(m, _):
        for u in range(8):
            small_tree(4 * m + u // 2, u % 2)
        return 0

    def tail_pair(at):
        return [spot_ref[6 + side, at] for side in range(2)]

    def send(at, c, value):
        for q in range(4):
            out_ref[lax.bitwise_and(q - group, 3), at, 2 * c : 2 * c + 2, :] = value[2 * q : 2 * q + 2, :]

    def clade(j, totals):
        tops = [top - 1920 for top in tail_pair(96 + 4 * group + j)]
        pairs = [pair - 1920 for top in tops for pair in tail_pair(top)]
        leaves = [leaf - 1792 - group * 32 for pair in pairs for leaf in tail_pair(pair)]
        for c in range(CLS):
            ratios = [ratio_ref[c, i] for i in range(3)]
            scale = log_ref[leaves[0], c]
            for leaf in leaves[1:]:
                scale = scale + log_ref[leaf, c]
            halves = []
            for h in range(2):
                quads = []
                for at in (2 * h, 2 * h + 1):
                    joined = [
                        mid_ref[leaves[2 * at], c, i] * mid_ref[leaves[2 * at + 1], c, i]
                        for i in range(STATES)
                    ]
                    quads.append(moved(joined, step_ref[8 + c, pairs[at]], mean_by_last(ratios, joined)))
                joined = product(quads[0], quads[1])
                halves.append(moved(joined, step_ref[8 + c, tops[h]], mean_by_last(ratios, joined)))
            joined = product(halves[0], halves[1])
            inverse = 1.0 / joined[3]
            for v in range(3):
                send(3 * j + v, c, joined[v] * inverse)
            scale = scale + jnp.log(joined[3])
            totals[c] = scale if j == 0 else totals[c] + scale

    step_copy.wait()
    rate4_copy.wait()
    for load in loads:
        load.wait()
    lax.fori_loop(0, 4, small_trees, 0)
    totals = [None] * CLS
    for j in range(4):
        clade(j, totals)
    for c in range(CLS):
        send(12, c, totals[c])


def upper_kernel(
    place_ref, own_ref, one_ref, two_ref, three_ref, top_ref, site_ref, part_ref, node_ref
):
    group = lax.axis_index("cls")
    pi = [top_ref[TOP_PI + i] for i in range(STATES)]
    scale = top_ref[TOP_CONST]
    for hop, piece_ref in enumerate((own_ref, one_ref, two_ref, three_ref)):
        scale = scale + piece_ref[12]
        source = 4 * lax.bitwise_and(group - hop, 3)
        for j in range(4):
            values = [piece_ref[3 * j + i] for i in range(3)]
            average = (pi[0] * values[0] + pi[1] * values[1]) + (pi[2] * values[2] + pi[3])
            step = top_ref[TOP_RATES + source + j] * average
            for i in range(3):
                node_ref[source + j, i] = values[i] + step
            node_ref[source + j, 3] = step + 1.0
    at = 16
    for level, count in ((6, 8), (7, 4), (8, 2), (9, 1)):
        for k in range(count):
            left = place_ref[2 * (at - 16)]
            right = place_ref[2 * (at - 16) + 1]
            joined = [node_ref[left, i] * node_ref[right, i] for i in range(STATES)]
            average = mean_state(pi, joined)
            if level == 6:
                scale = scale + jnp.log(average)
                inverse = 1.0 / average
                for i in range(STATES):
                    node_ref[at, i] = joined[i] * inverse + top_ref[TOP_RATES + at]
            elif level < 9:
                step = top_ref[TOP_RATES + at] * average
                for i in range(STATES):
                    node_ref[at, i] = joined[i] + step
            else:
                scale = scale + jnp.log(average)
            at += 1
    top = jnp.maximum(scale, pltpu.roll(scale, 2, 0))
    top = jnp.maximum(top, pltpu.roll(top, 4, 0))
    share = jnp.exp(scale - top)
    mass = share + pltpu.roll(share, 2, 0)
    mass = mass + pltpu.roll(mass, 4, 0)
    total = top + jnp.log(mass)
    site_ref[...] = total[0:2] * (1.0 / 1024.0)
    weight = top_ref[TOP_WEIGHT]
    classes = weight * (share / mass)
    row = lax.broadcasted_iota(jnp.int32, TILE, 0)
    column = lax.broadcasted_iota(jnp.int32, TILE, 1)
    by_row = [
        jnp.sum(values, axis=1, keepdims=True) for values in (classes, weight * total, weight)
    ]
    by_pair = lax.shift_right_logical(row, 1)
    line = jnp.where(by_pair == column, by_row[0], 0.0)
    line = jnp.where((column == 4) & (row < 2), by_row[1], line)
    line = jnp.where((column == 5) & (row < 2), by_row[2], line)
    line = jnp.sum(line, axis=0, keepdims=True)
    for k in range(16):
        part_ref[8 * k : 8 * k + 8, :] = jnp.broadcast_to(line, TILE)


def last_kernel(every_ref, site_ref, own_hbm, mean_hbm, site_hbm, own_ref, mean_ref, sems):
    site_copy = pltpu.make_async_copy(site_ref, site_hbm, sems.at[2])
    site_copy.start()
    group = lax.axis_index("cls")
    sums = every_ref[0:8, :]
    for k in range(1, 16):
        sums = sums + every_ref[8 * k : 8 * k + 8, :]
    sums = jnp.sum(sums, axis=0, keepdims=True)
    column = lax.broadcasted_iota(jnp.int32, (1, 128), 1)

    def entry(at):
        return jnp.sum(jnp.where(column == at, sums, 0.0), axis=1, keepdims=True)

    count = entry(5)
    own_ref[...] = entry(group) / count
    mean_ref[...] = entry(4) / (count * 1024.0)
    own_copy = pltpu.make_async_copy(own_ref, own_hbm, sems.at[0])
    mean_copy = pltpu.make_async_copy(mean_ref, mean_hbm, sems.at[1])
    own_copy.start()
    mean_copy.start()
    own_copy.wait()
    mean_copy.wait()
    site_copy.wait()


def per_device(tip_codes, counts, children, lengths, frequencies, weights):
    codes = tip_codes.reshape(32, 8, 8, 128).transpose(0, 2, 1, 3).reshape(2048, 128)
    child_rows = children.T
    smem = pl.BlockSpec(memory_space=SMEM)
    vmem = pl.BlockSpec(memory_space=VMEM)
    hbm = pl.BlockSpec(memory_space=pltpu.MemorySpace.HBM)
    ours, top, places = pl.pallas_call(
        lower_kernel,
        out_shape=(pltpu.VMEM((4, 13, 8, 128), FLOAT), pltpu.VMEM((TOP_ROWS, 8, 128), FLOAT), pltpu.SMEM((32,), jnp.int32)),
        in_specs=[hbm] * 6,
        out_specs=(vmem, vmem, smem),
        scratch_shapes=[
            pltpu.VMEM((2, 1023), jnp.int32),
            pltpu.SMEM((4, 4), FLOAT),
            pltpu.SMEM((4,), FLOAT),
            pltpu.VMEM((4, 2046), FLOAT),
            pltpu.VMEM((2048, 128), jnp.int32),
            pltpu.VMEM(TILE, jnp.int32),
            pltpu.VMEM((4, 2048), FLOAT),
            pltpu.VMEM(TILE, jnp.int32),
            pltpu.SMEM(TILE, jnp.int32),
            pltpu.VMEM((16, 128), FLOAT),
            pltpu.SMEM((16, 128), FLOAT),
            pltpu.VMEM((CLS, STATES, 8, 128), FLOAT),
            pltpu.VMEM((CLS, 3, 8, 128), FLOAT),
            pltpu.VMEM((4, 8, 128), FLOAT),
            pltpu.VMEM((4, 8, 128), FLOAT),
            pltpu.VMEM((16, 8, 128), FLOAT),
            pltpu.VMEM((16, 128), FLOAT),
            pltpu.SMEM((16, 128), FLOAT),
            pltpu.VMEM((32, CLS, STATES, 8, 128), FLOAT),
            pltpu.VMEM((32, CLS, 8, 128), FLOAT),
            pltpu.SemaphoreType.DMA((12,)),
        ],
        compiler_params=pltpu.CompilerParams(vmem_limit_bytes=16 * 1024 * 1024),
        name="lower_tree",
    )(
        *(
            pltpu.with_memory_space_constraint(array, pltpu.MemorySpace.HBM)
            for array in (child_rows, frequencies, weights, lengths, codes, counts.reshape(8, 128))
        )
    )
    pieces = [ours[0]]
    for hop in range(1, 4):
        pieces.append(lax.ppermute(ours[hop], "cls", [(k, (k + hop) % 4) for k in range(4)]))
    site, part = pl.pallas_call(
        upper_kernel,
        out_shape=(pltpu.VMEM((2, 128), FLOAT), pltpu.VMEM((128, 128), FLOAT)),
        in_specs=[smem] + [vmem] * 5,
        out_specs=(vmem, vmem),
        scratch_shapes=[pltpu.VMEM((32, STATES, 8, 128), FLOAT)],
        compiler_params=pltpu.CompilerParams(vmem_limit_bytes=16 * 1024 * 1024),
        name="upper_tree",
    )(places, *pieces, top)
    every = lax.all_to_all(part, ("cls", "site"), split_axis=0, concat_axis=0, tiled=True)
    own, mean, site = pl.pallas_call(
        last_kernel,
        out_shape=tuple(jax.ShapeDtypeStruct(shape, FLOAT) for shape in ((1, 1), (1, 1), (2, 128))),
        in_specs=[vmem, vmem],
        out_specs=(hbm, hbm, hbm),
        scratch_shapes=[
            pltpu.VMEM((1, 1), FLOAT),
            pltpu.VMEM((1, 1), FLOAT),
            pltpu.SemaphoreType.DMA((3,)),
        ],
        compiler_params=pltpu.CompilerParams(vmem_limit_bytes=16 * 1024 * 1024),
        name="last_sums",
    )(every, site)
    return site.reshape(1, 256), own.reshape(1), mean.reshape(())


def solution(mesh):
    return jax.shard_map(
        per_device,
        mesh=mesh,
        in_specs=(P("cls", "site"), P("site"), P(), P(), P(), P()),
        out_specs=(P("cls", "site"), P("cls"), P()),
        check_vma=False,
    )
```

```python
import jax
import jax.numpy as jnp
from jax import lax
from jax.experimental import pallas as pl
from jax.experimental.pallas import tpu as pltpu
from jax.sharding import PartitionSpec as P

CLS = 4
STATES = 4
FLOAT = jnp.float32
SMEM = pltpu.MemorySpace.SMEM
VMEM = pltpu.MemorySpace.VMEM
TILE = (8, 128)
BUILD = 8
TOP_RATES, TOP_PI, TOP_CONST, TOP_WEIGHT, TOP_ROWS = 0, 30, 34, 35, 36


def mean_state(pi, values):
    return (pi[0] * values[0] + pi[1] * values[1]) + (pi[2] * values[2] + pi[3] * values[3])


def mean_by_last(ratios, values):
    return (ratios[0] * values[0] + ratios[1] * values[1]) + (ratios[2] * values[2] + values[3])


def moved(values, rate, average):
    step = rate * average
    return [value + step for value in values]


def product(left, right):
    return [a * b for a, b in zip(left, right)]


def choose(selector, options):
    value = jnp.where(selector == 1, options[1], options[0])
    value = jnp.where(selector == 2, options[2], value)
    return jnp.where(selector == 3, options[3], value)


def pick(masks, options):
    value = jnp.where(masks[1], options[1], options[0])
    value = jnp.where(masks[2], options[2], value)
    return jnp.where(masks[3], options[3], value)


def lanes_of(rows, places):
    return lax.gather(
        rows,
        places[..., None],
        lax.GatherDimensionNumbers(
            offset_dims=(),
            collapsed_slice_dims=(1,),
            start_index_map=(1,),
            operand_batching_dims=(0,),
            start_indices_batching_dims=(0,),
        ),
        slice_sizes=(1, 1),
        mode=lax.GatherScatterMode.PROMISE_IN_BOUNDS,
    )


def lower_kernel(
    child_hbm, freq_hbm, weight_hbm, lengths_hbm, codes_hbm, counts_hbm,
    out_ref, top_ref, place_ref,
    child_vec, freq_ref, weight_ref, lengths_ref, codes_ref, counts_ref, rate_vec,
    spot_vec, spot_ref, step_vec, step_ref,
    pi_ref, ratio_ref, pattern_ref, factor_ref, table_ref, rate4_vec, rate4_ref, mid_ref, log_ref, sems,
):
    group = lax.axis_index("cls")
    small = [
        pltpu.make_async_copy(source, target, sems.at[4 + k])
        for k, (source, target) in enumerate(
            (
                (child_hbm, child_vec),
                (lengths_hbm, lengths_ref),
                (freq_hbm, freq_ref),
                (weight_hbm, weight_ref),
                (counts_hbm, counts_ref),
            )
        )
    ]
    for load in small:
        load.start()
    loads = [
        pltpu.make_async_copy(
            codes_hbm.at[pl.ds(512 * j, 512)], codes_ref.at[pl.ds(512 * j, 512)], sems.at[j]
        )
        for j in range(4)
    ]
    for load in loads:
        load.start()
    small[0].wait()
    half = lax.shift_right_logical(group, 1)

    def block(ref, start):
        return ref[:, pl.ds(pl.multiple_of(start, 128), 128)]

    local = block(child_vec, 128 * group) - 256 * group
    spot_vec[0:2] = lax.shift_left(lax.shift_right_logical(local, 3), 6) + lax.bitwise_and(local, 7)
    spot_vec[2:4] = block(child_vec, 512 + 128 * half) - (1024 + 128 * group)
    spot_vec[4:6] = child_vec[:, 768:896] - (1536 + 128 * half)
    spot_vec[6:8] = jnp.concatenate([child_vec[:, 896:1023], jnp.zeros((2, 1), jnp.int32)], axis=1)
    spot_copy = pltpu.make_async_copy(spot_vec, spot_ref, sems.at[9])
    spot_copy.start()
    for load in small[1:]:
        load.wait()

    lane = lax.broadcasted_iota(jnp.int32, TILE, 1)
    sub = lax.broadcasted_iota(jnp.int32, TILE, 0)
    by_pair = lax.shift_right_logical(sub, 1)
    by_class = lax.bitwise_and(sub, 3)
    uniform, betas = [], []
    for c in range(CLS):
        raw = [jnp.full(TILE, freq_ref[c, i], FLOAT) for i in range(STATES)]
        inverse = 1.0 / ((raw[0] + raw[1]) + (raw[2] + raw[3]))
        uniform.append([value * inverse for value in raw])
        betas.append(1.0 / (1.0 - mean_state(uniform[c], uniform[c])))
        for i in range(STATES):
            pi_ref[c, i] = uniform[c][i]
        for i in range(3):
            ratio_ref[c, i] = uniform[c][i] / uniform[c][3]
    beta_rows = choose(by_class, betas)[:4]
    total = jnp.zeros((4, 128), FLOAT)
    for k in range(16):
        width = min(128, 2046 - 128 * k)
        part = lengths_ref[:, 128 * k : 128 * k + width]
        if width < 128:
            part = jnp.concatenate([part, jnp.zeros((4, 128 - width), FLOAT)], axis=1)
        total = total + part
        decay = jnp.exp(-(beta_rows * part))
        rate_vec[:, 128 * k : 128 * k + 128] = (1.0 - decay) / decay

    last_pi = choose(by_class, [uniform[c][3] for c in range(CLS)])[:4]
    step_vec[0:4] = block(rate_vec, 1536 + 128 * half) * last_pi
    step_vec[4:8] = rate_vec[:, 1792:1920] * last_pi
    step_vec[8:12] = rate_vec[:, 1920:2048] * last_pi
    step_vec[12:16] = jnp.zeros((4, 128), FLOAT)
    step_copy = pltpu.make_async_copy(step_vec, step_ref, sems.at[10])
    step_copy.start()

    def twice(rows):
        return jnp.concatenate([rows, rows], axis=0)

    low = twice(block(rate_vec, 256 * group))
    high = twice(block(rate_vec, 256 * group + 128))
    own = twice(block(rate_vec, 1024 + 128 * group))

    def rates_at(places):
        places = jnp.broadcast_to(places, TILE)
        inside = lax.bitwise_and(places, 127)
        return jnp.where(places < 128, lanes_of(low, inside), lanes_of(high, inside))

    left = rates_at(local[0:1])
    right = rates_at(local[1:2])
    both = left * right
    factor_ref[0] = right
    factor_ref[1] = left
    factor_ref[2] = both + own * (left + right + both)
    factor_ref[3] = own
    for k in range(4):
        rate4_vec[4 * k : 4 * k + 4] = factor_ref[k, 0:4]
    rate4_copy = pltpu.make_async_copy(rate4_vec, rate4_ref, sems.at[11])
    rate4_copy.start()

    own_state = lax.bitwise_and(lax.shift_right_logical(lane, 4), 3)
    left_code = lax.bitwise_and(lax.shift_right_logical(lane, 2), 3)
    right_code = lax.bitwise_and(lane, 3)
    left_own = own_state == left_code
    right_own = own_state == right_code
    first = lane < 64
    both_own = jnp.where(left_own, jnp.where(right_own, 1.0, 0.0), 0.0)
    by_rows = [choose(by_class, [uniform[c][i] for c in range(CLS)]) for i in range(STATES)]
    left_pi = choose(left_code, by_rows)
    right_pi = choose(right_code, by_rows)
    pattern_ref[0] = jnp.where(left_own, right_pi, 0.0)
    pattern_ref[1] = jnp.where(right_own, left_pi, 0.0)
    pattern_ref[2] = left_pi * right_pi
    pattern_ref[3] = jnp.where(left_code == right_code, left_pi, 0.0)

    for i in range(STATES):
        top_ref[TOP_PI + i] = choose(by_pair, [uniform[c][i] for c in range(CLS)])
    beta_pairs = choose(by_pair, betas)
    sums = choose(by_pair, [jnp.broadcast_to(total[c : c + 1], TILE) for c in range(CLS)])
    sums = jnp.broadcast_to(jnp.sum(sums, axis=1, keepdims=True), TILE)
    weights = [jnp.full(TILE, weight_ref[c], FLOAT) for c in range(CLS)]
    weight_sum = (weights[0] + weights[1]) + (weights[2] + weights[3])
    top_ref[TOP_CONST] = jnp.log(choose(by_pair, weights) / weight_sum) - beta_pairs * sums
    last = rate_vec[:, 1920:2048]
    last = choose(by_pair, [jnp.broadcast_to(last[c : c + 1], TILE) for c in range(CLS)])
    for k in range(30):
        top_ref[TOP_RATES + k] = jnp.broadcast_to(last[:, 96 + k : 97 + k], TILE)
    quarter = counts_ref[pl.ds(2 * group, 2), :].astype(FLOAT)
    top_ref[TOP_WEIGHT] = jnp.concatenate([quarter, quarter, quarter, quarter], axis=0)
    spot_copy.wait()

    for k in range(15):
        for side in range(2):
            place_ref[2 * k + side] = spot_ref[6 + side, 112 + k] - 2016

    def pairs_of(n):
        tops = [spot_ref[4 + side, 32 * group + n] for side in range(2)]
        return tops, [spot_ref[2 + side, top] for top in tops for side in range(2)]

    upper_half = sub < 4

    def build_table(m):
        pairs = [pairs_of(2 * m + u)[1] for u in range(2)]
        places = jnp.where(
            upper_half,
            jnp.where(first, pairs[0][0], pairs[0][2]),
            jnp.where(first, pairs[1][0], pairs[1][2]),
        )
        table = both_own
        for k in range(4):
            table = table + lanes_of(factor_ref[k], places) * pattern_ref[k]
        table_ref[m] = table

    def build_tables(m, _):
        for u in range(BUILD):
            build_table(BUILD * m + u)
        return 0

    lax.fori_loop(0, 16 // BUILD, build_tables, 0)

    def codes_of(pair):
        return [codes_ref[pl.ds(spot_ref[side, pair], 8, stride=8), :] for side in range(2)]

    def chosen_pair(pair):
        left, right = codes_of(pair)
        same = left == right
        left_is = [left == i for i in range(STATES)]
        right_is = [right == i for i in range(STATES)]
        found = []
        for c in range(CLS):
            pi = [pi_ref[c, i] for i in range(STATES)]
            left_pi = pick(left_is, pi)
            right_pi = pick(right_is, pi)
            left_step = rate4_ref[4 + c, pair] * left_pi
            right_step = rate4_ref[c, pair] * right_pi
            base = rate4_ref[8 + c, pair] * (left_pi * right_pi)
            base = base + jnp.where(same, rate4_ref[12 + c, pair] * left_pi, 0.0)
            at_right = base + left_step
            at_left = base + right_step
            at_left = jnp.where(same, at_left + (left_step + 1.0), at_left)
            found.append(
                [
                    jnp.where(left_is[i], at_left, jnp.where(right_is[i], at_right, base))
                    for i in range(STATES)
                ]
            )
        return found

    def small_tree(m, u):
        n = 2 * m + u
        tops, pairs = pairs_of(n)
        tables = [
            jnp.broadcast_to(table_ref[m, 4 * u + c : 4 * u + c + 1, :], TILE) for c in range(CLS)
        ]
        halves = []
        for h in range(2):
            sides = codes_of(pairs[2 * h])
            code = lax.shift_left(sides[0], 2) + sides[1] + 64 * h
            looked = []
            for i in range(STATES):
                place = code + 16 * i if i else code
                looked.append([lanes_of(tables[c], place) for c in range(CLS)])
            chosen = chosen_pair(pairs[2 * h + 1])
            parts = []
            for c in range(CLS):
                ratios = [ratio_ref[c, i] for i in range(3)]
                values = [looked[i][c] * chosen[c][i] for i in range(STATES)]
                parts.append(moved(values, step_ref[c, tops[h]], mean_by_last(ratios, values)))
            halves.append(parts)
        for c in range(CLS):
            ratios = [ratio_ref[c, i] for i in range(3)]
            values = product(halves[0][c], halves[1][c])
            average = mean_by_last(ratios, values)
            inverse = 1.0 / average
            own_rate = step_ref[4 + c, 32 * group + n]
            for i in range(STATES):
                mid_ref[n, c, i] = values[i] * inverse + own_rate
            log_ref[n, c] = jnp.log(average)

    def small_trees(m, _):
        for u in range(16):
            small_tree(8 * m + u // 2, u % 2)
        return 0

    def tail_pair(at):
        return [spot_ref[6 + side, at] for side in range(2)]

    def send(at, c, value):
        for q in range(4):
            out_ref[lax.bitwise_and(q - group, 3), at, 2 * c : 2 * c + 2, :] = value[2 * q : 2 * q + 2, :]

    def clade(j, totals):
        tops = [top - 1920 for top in tail_pair(96 + 4 * group + j)]
        pairs = [pair - 1920 for top in tops for pair in tail_pair(top)]
        leaves = [leaf - 1792 - group * 32 for pair in pairs for leaf in tail_pair(pair)]
        for c in range(CLS):
            ratios = [ratio_ref[c, i] for i in range(3)]
            scale = log_ref[leaves[0], c]
            for leaf in leaves[1:]:
                scale = scale + log_ref[leaf, c]
            halves = []
            for h in range(2):
                quads = []
                for at in (2 * h, 2 * h + 1):
                    joined = [
                        mid_ref[leaves[2 * at], c, i] * mid_ref[leaves[2 * at + 1], c, i]
                        for i in range(STATES)
                    ]
                    quads.append(moved(joined, step_ref[8 + c, pairs[at]], mean_by_last(ratios, joined)))
                joined = product(quads[0], quads[1])
                halves.append(moved(joined, step_ref[8 + c, tops[h]], mean_by_last(ratios, joined)))
            joined = product(halves[0], halves[1])
            inverse = 1.0 / joined[3]
            for v in range(3):
                send(3 * j + v, c, joined[v] * inverse)
            scale = scale + jnp.log(joined[3])
            totals[c] = scale if j == 0 else totals[c] + scale

    step_copy.wait()
    rate4_copy.wait()
    for load in loads:
        load.wait()
    lax.fori_loop(0, 2, small_trees, 0)
    totals = [None] * CLS
    for j in range(4):
        clade(j, totals)
    for c in range(CLS):
        send(12, c, totals[c])


def upper_kernel(
    place_ref, own_ref, one_ref, two_ref, three_ref, top_ref, site_ref, part_ref, node_ref
):
    group = lax.axis_index("cls")
    pi = [top_ref[TOP_PI + i] for i in range(STATES)]
    scale = top_ref[TOP_CONST]
    for hop, piece_ref in enumerate((own_ref, one_ref, two_ref, three_ref)):
        scale = scale + piece_ref[12]
        source = 4 * lax.bitwise_and(group - hop, 3)
        for j in range(4):
            values = [piece_ref[3 * j + i] for i in range(3)]
            average = (pi[0] * values[0] + pi[1] * values[1]) + (pi[2] * values[2] + pi[3])
            step = top_ref[TOP_RATES + source + j] * average
            for i in range(3):
                node_ref[source + j, i] = values[i] + step
            node_ref[source + j, 3] = step + 1.0
    at = 16
    for level, count in ((6, 8), (7, 4), (8, 2), (9, 1)):
        for k in range(count):
            left = place_ref[2 * (at - 16)]
            right = place_ref[2 * (at - 16) + 1]
            joined = [node_ref[left, i] * node_ref[right, i] for i in range(STATES)]
            average = mean_state(pi, joined)
            if level == 6:
                scale = scale + jnp.log(average)
                inverse = 1.0 / average
                for i in range(STATES):
                    node_ref[at, i] = joined[i] * inverse + top_ref[TOP_RATES + at]
            elif level < 9:
                step = top_ref[TOP_RATES + at] * average
                for i in range(STATES):
                    node_ref[at, i] = joined[i] + step
            else:
                scale = scale + jnp.log(average)
            at += 1
    top = jnp.maximum(scale, pltpu.roll(scale, 2, 0))
    top = jnp.maximum(top, pltpu.roll(top, 4, 0))
    share = jnp.exp(scale - top)
    mass = share + pltpu.roll(share, 2, 0)
    mass = mass + pltpu.roll(mass, 4, 0)
    total = top + jnp.log(mass)
    site_ref[...] = total[0:2] * (1.0 / 1024.0)
    weight = top_ref[TOP_WEIGHT]
    classes = weight * (share / mass)
    row = lax.broadcasted_iota(jnp.int32, TILE, 0)
    column = lax.broadcasted_iota(jnp.int32, TILE, 1)
    by_row = [
        jnp.sum(values, axis=1, keepdims=True) for values in (classes, weight * total, weight)
    ]
    by_pair = lax.shift_right_logical(row, 1)
    line = jnp.where(by_pair == column, by_row[0], 0.0)
    line = jnp.where((column == 4) & (row < 2), by_row[1], line)
    line = jnp.where((column == 5) & (row < 2), by_row[2], line)
    line = jnp.sum(line, axis=0, keepdims=True)
    for k in range(16):
        part_ref[8 * k : 8 * k + 8, :] = jnp.broadcast_to(line, TILE)


def last_kernel(every_ref, site_ref, own_hbm, mean_hbm, site_hbm, own_ref, mean_ref, sems):
    site_copy = pltpu.make_async_copy(site_ref, site_hbm, sems.at[2])
    site_copy.start()
    group = lax.axis_index("cls")
    sums = every_ref[0:8, :]
    for k in range(1, 16):
        sums = sums + every_ref[8 * k : 8 * k + 8, :]
    sums = jnp.sum(sums, axis=0, keepdims=True)
    column = lax.broadcasted_iota(jnp.int32, (1, 128), 1)

    def entry(at):
        return jnp.sum(jnp.where(column == at, sums, 0.0), axis=1, keepdims=True)

    count = entry(5)
    own_ref[...] = entry(group) / count
    mean_ref[...] = entry(4) / (count * 1024.0)
    own_copy = pltpu.make_async_copy(own_ref, own_hbm, sems.at[0])
    mean_copy = pltpu.make_async_copy(mean_ref, mean_hbm, sems.at[1])
    own_copy.start()
    mean_copy.start()
    own_copy.wait()
    mean_copy.wait()
    site_copy.wait()


def per_device(tip_codes, counts, children, lengths, frequencies, weights):
    codes = tip_codes.reshape(32, 8, 8, 128).transpose(0, 2, 1, 3).reshape(2048, 128)
    child_rows = children.T
    smem = pl.BlockSpec(memory_space=SMEM)
    vmem = pl.BlockSpec(memory_space=VMEM)
    hbm = pl.BlockSpec(memory_space=pltpu.MemorySpace.HBM)
    ours, top, places = pl.pallas_call(
        lower_kernel,
        out_shape=(pltpu.VMEM((4, 13, 8, 128), FLOAT), pltpu.VMEM((TOP_ROWS, 8, 128), FLOAT), pltpu.SMEM((32,), jnp.int32)),
        in_specs=[hbm] * 6,
        out_specs=(vmem, vmem, smem),
        scratch_shapes=[
            pltpu.VMEM((2, 1023), jnp.int32),
            pltpu.SMEM((4, 4), FLOAT),
            pltpu.SMEM((4,), FLOAT),
            pltpu.VMEM((4, 2046), FLOAT),
            pltpu.VMEM((2048, 128), jnp.int32),
            pltpu.VMEM(TILE, jnp.int32),
            pltpu.VMEM((4, 2048), FLOAT),
            pltpu.VMEM(TILE, jnp.int32),
            pltpu.SMEM(TILE, jnp.int32),
            pltpu.VMEM((16, 128), FLOAT),
            pltpu.SMEM((16, 128), FLOAT),
            pltpu.VMEM((CLS, STATES, 8, 128), FLOAT),
            pltpu.VMEM((CLS, 3, 8, 128), FLOAT),
            pltpu.VMEM((4, 8, 128), FLOAT),
            pltpu.VMEM((4, 8, 128), FLOAT),
            pltpu.VMEM((16, 8, 128), FLOAT),
            pltpu.VMEM((16, 128), FLOAT),
            pltpu.SMEM((16, 128), FLOAT),
            pltpu.VMEM((32, CLS, STATES, 8, 128), FLOAT),
            pltpu.VMEM((32, CLS, 8, 128), FLOAT),
            pltpu.SemaphoreType.DMA((12,)),
        ],
        compiler_params=pltpu.CompilerParams(vmem_limit_bytes=16 * 1024 * 1024),
        name="lower_tree",
    )(
        *(
            pltpu.with_memory_space_constraint(array, pltpu.MemorySpace.HBM)
            for array in (child_rows, frequencies, weights, lengths, codes, counts.reshape(8, 128))
        )
    )
    pieces = [ours[0]]
    for hop in range(1, 4):
        pieces.append(lax.ppermute(ours[hop], "cls", [(k, (k + hop) % 4) for k in range(4)]))
    site, part = pl.pallas_call(
        upper_kernel,
        out_shape=(pltpu.VMEM((2, 128), FLOAT), pltpu.VMEM((128, 128), FLOAT)),
        in_specs=[smem] + [vmem] * 5,
        out_specs=(vmem, vmem),
        scratch_shapes=[pltpu.VMEM((32, STATES, 8, 128), FLOAT)],
        compiler_params=pltpu.CompilerParams(vmem_limit_bytes=16 * 1024 * 1024),
        name="upper_tree",
    )(places, *pieces, top)
    every = lax.all_to_all(part, ("cls", "site"), split_axis=0, concat_axis=0, tiled=True)
    own, mean, site = pl.pallas_call(
        last_kernel,
        out_shape=tuple(jax.ShapeDtypeStruct(shape, FLOAT) for shape in ((1, 1), (1, 1), (2, 128))),
        in_specs=[vmem, vmem],
        out_specs=(hbm, hbm, hbm),
        scratch_shapes=[
            pltpu.VMEM((1, 1), FLOAT),
            pltpu.VMEM((1, 1), FLOAT),
            pltpu.SemaphoreType.DMA((3,)),
        ],
        compiler_params=pltpu.CompilerParams(vmem_limit_bytes=16 * 1024 * 1024),
        name="last_sums",
    )(every, site)
    return site.reshape(1, 256), own.reshape(1), mean.reshape(())


def solution(mesh):
    return jax.shard_map(
        per_device,
        mesh=mesh,
        in_specs=(P("cls", "site"), P("site"), P(), P(), P(), P()),
        out_specs=(P("cls", "site"), P("cls"), P()),
        check_vma=False,
    )
```

```python
import jax
import jax.numpy as jnp
from jax import lax
from jax.experimental import pallas as pl
from jax.experimental.pallas import tpu as pltpu
from jax.sharding import PartitionSpec as P

CLS = 4
STATES = 4
FLOAT = jnp.float32
SMEM = pltpu.MemorySpace.SMEM
VMEM = pltpu.MemorySpace.VMEM
TILE = (8, 128)
BUILD = 16
TOP_RATES, TOP_PI, TOP_CONST, TOP_WEIGHT, TOP_ROWS = 0, 30, 34, 35, 36


def mean_state(pi, values):
    return (pi[0] * values[0] + pi[1] * values[1]) + (pi[2] * values[2] + pi[3] * values[3])


def mean_by_last(ratios, values):
    return (ratios[0] * values[0] + ratios[1] * values[1]) + (ratios[2] * values[2] + values[3])


def moved(values, rate, average):
    step = rate * average
    return [value + step for value in values]


def product(left, right):
    return [a * b for a, b in zip(left, right)]


def choose(selector, options):
    value = jnp.where(selector == 1, options[1], options[0])
    value = jnp.where(selector == 2, options[2], value)
    return jnp.where(selector == 3, options[3], value)


def pick(masks, options):
    value = jnp.where(masks[1], options[1], options[0])
    value = jnp.where(masks[2], options[2], value)
    return jnp.where(masks[3], options[3], value)


def lanes_of(rows, places):
    return lax.gather(
        rows,
        places[..., None],
        lax.GatherDimensionNumbers(
            offset_dims=(),
            collapsed_slice_dims=(1,),
            start_index_map=(1,),
            operand_batching_dims=(0,),
            start_indices_batching_dims=(0,),
        ),
        slice_sizes=(1, 1),
        mode=lax.GatherScatterMode.PROMISE_IN_BOUNDS,
    )


def lower_kernel(
    child_hbm, freq_hbm, weight_hbm, lengths_hbm, codes_hbm, counts_hbm,
    out_ref, top_ref, place_ref,
    child_vec, freq_ref, weight_ref, lengths_ref, codes_ref, counts_ref, rate_vec,
    spot_vec, spot_ref, step_vec, step_ref,
    pi_ref, ratio_ref, pattern_ref, factor_ref, table_ref, rate4_vec, rate4_ref, mid_ref, log_ref, sems,
):
    group = lax.axis_index("cls")
    small = [
        pltpu.make_async_copy(source, target, sems.at[4 + k])
        for k, (source, target) in enumerate(
            (
                (child_hbm, child_vec),
                (lengths_hbm, lengths_ref),
                (freq_hbm, freq_ref),
                (weight_hbm, weight_ref),
                (counts_hbm, counts_ref),
            )
        )
    ]
    for load in small:
        load.start()
    loads = [
        pltpu.make_async_copy(
            codes_hbm.at[pl.ds(512 * j, 512)], codes_ref.at[pl.ds(512 * j, 512)], sems.at[j]
        )
        for j in range(4)
    ]
    for load in loads:
        load.start()
    small[0].wait()
    half = lax.shift_right_logical(group, 1)

    def block(ref, start):
        return ref[:, pl.ds(pl.multiple_of(start, 128), 128)]

    local = block(child_vec, 128 * group) - 256 * group
    spot_vec[0:2] = lax.shift_left(lax.shift_right_logical(local, 3), 6) + lax.bitwise_and(local, 7)
    spot_vec[2:4] = block(child_vec, 512 + 128 * half) - (1024 + 128 * group)
    spot_vec[4:6] = child_vec[:, 768:896] - (1536 + 128 * half)
    spot_vec[6:8] = jnp.concatenate([child_vec[:, 896:1023], jnp.zeros((2, 1), jnp.int32)], axis=1)
    spot_copy = pltpu.make_async_copy(spot_vec, spot_ref, sems.at[9])
    spot_copy.start()
    for load in small[1:]:
        load.wait()

    lane = lax.broadcasted_iota(jnp.int32, TILE, 1)
    sub = lax.broadcasted_iota(jnp.int32, TILE, 0)
    by_pair = lax.shift_right_logical(sub, 1)
    by_class = lax.bitwise_and(sub, 3)
    uniform, betas = [], []
    for c in range(CLS):
        raw = [jnp.full(TILE, freq_ref[c, i], FLOAT) for i in range(STATES)]
        inverse = 1.0 / ((raw[0] + raw[1]) + (raw[2] + raw[3]))
        uniform.append([value * inverse for value in raw])
        betas.append(1.0 / (1.0 - mean_state(uniform[c], uniform[c])))
        for i in range(STATES):
            pi_ref[c, i] = uniform[c][i]
        for i in range(3):
            ratio_ref[c, i] = uniform[c][i] / uniform[c][3]
    beta_rows = choose(by_class, betas)[:4]
    total = jnp.zeros((4, 128), FLOAT)
    for k in range(16):
        width = min(128, 2046 - 128 * k)
        part = lengths_ref[:, 128 * k : 128 * k + width]
        if width < 128:
            part = jnp.concatenate([part, jnp.zeros((4, 128 - width), FLOAT)], axis=1)
        total = total + part
        decay = jnp.exp(-(beta_rows * part))
        rate_vec[:, 128 * k : 128 * k + 128] = (1.0 - decay) / decay

    last_pi = choose(by_class, [uniform[c][3] for c in range(CLS)])[:4]
    step_vec[0:4] = block(rate_vec, 1536 + 128 * half) * last_pi
    step_vec[4:8] = rate_vec[:, 1792:1920] * last_pi
    step_vec[8:12] = rate_vec[:, 1920:2048] * last_pi
    step_vec[12:16] = jnp.zeros((4, 128), FLOAT)
    step_copy = pltpu.make_async_copy(step_vec, step_ref, sems.at[10])
    step_copy.start()

    def twice(rows):
        return jnp.concatenate([rows, rows], axis=0)

    low = twice(block(rate_vec, 256 * group))
    high = twice(block(rate_vec, 256 * group + 128))
    own = twice(block(rate_vec, 1024 + 128 * group))

    def rates_at(places):
        places = jnp.broadcast_to(places, TILE)
        inside = lax.bitwise_and(places, 127)
        return jnp.where(places < 128, lanes_of(low, inside), lanes_of(high, inside))

    left = rates_at(local[0:1])
    right = rates_at(local[1:2])
    both = left * right
    factor_ref[0] = right
    factor_ref[1] = left
    factor_ref[2] = both + own * (left + right + both)
    factor_ref[3] = own
    for k in range(4):
        rate4_vec[4 * k : 4 * k + 4] = factor_ref[k, 0:4]
    rate4_copy = pltpu.make_async_copy(rate4_vec, rate4_ref, sems.at[11])
    rate4_copy.start()

    own_state = lax.bitwise_and(lax.shift_right_logical(lane, 4), 3)
    left_code = lax.bitwise_and(lax.shift_right_logical(lane, 2), 3)
    right_code = lax.bitwise_and(lane, 3)
    left_own = own_state == left_code
    right_own = own_state == right_code
    first = lane < 64
    both_own = jnp.where(left_own, jnp.where(right_own, 1.0, 0.0), 0.0)
    by_rows = [choose(by_class, [uniform[c][i] for c in range(CLS)]) for i in range(STATES)]
    left_pi = choose(left_code, by_rows)
    right_pi = choose(right_code, by_rows)
    pattern_ref[0] = jnp.where(left_own, right_pi, 0.0)
    pattern_ref[1] = jnp.where(right_own, left_pi, 0.0)
    pattern_ref[2] = left_pi * right_pi
    pattern_ref[3] = jnp.where(left_code == right_code, left_pi, 0.0)

    for i in range(STATES):
        top_ref[TOP_PI + i] = choose(by_pair, [uniform[c][i] for c in range(CLS)])
    beta_pairs = choose(by_pair, betas)
    sums = choose(by_pair, [jnp.broadcast_to(total[c : c + 1], TILE) for c in range(CLS)])
    sums = jnp.broadcast_to(jnp.sum(sums, axis=1, keepdims=True), TILE)
    weights = [jnp.full(TILE, weight_ref[c], FLOAT) for c in range(CLS)]
    weight_sum = (weights[0] + weights[1]) + (weights[2] + weights[3])
    top_ref[TOP_CONST] = jnp.log(choose(by_pair, weights) / weight_sum) - beta_pairs * sums
    last = rate_vec[:, 1920:2048]
    last = choose(by_pair, [jnp.broadcast_to(last[c : c + 1], TILE) for c in range(CLS)])
    for k in range(30):
        top_ref[TOP_RATES + k] = jnp.broadcast_to(last[:, 96 + k : 97 + k], TILE)
    quarter = counts_ref[pl.ds(2 * group, 2), :].astype(FLOAT)
    top_ref[TOP_WEIGHT] = jnp.concatenate([quarter, quarter, quarter, quarter], axis=0)
    spot_copy.wait()

    for k in range(15):
        for side in range(2):
            place_ref[2 * k + side] = spot_ref[6 + side, 112 + k] - 2016

    def pairs_of(n):
        tops = [spot_ref[4 + side, 32 * group + n] for side in range(2)]
        return tops, [spot_ref[2 + side, top] for top in tops for side in range(2)]

    upper_half = sub < 4

    def build_table(m):
        pairs = [pairs_of(2 * m + u)[1] for u in range(2)]
        places = jnp.where(
            upper_half,
            jnp.where(first, pairs[0][0], pairs[0][2]),
            jnp.where(first, pairs[1][0], pairs[1][2]),
        )
        table = both_own
        for k in range(4):
            table = table + lanes_of(factor_ref[k], places) * pattern_ref[k]
        table_ref[m] = table

    def build_tables(m, _):
        for u in range(BUILD):
            build_table(BUILD * m + u)
        return 0

    lax.fori_loop(0, 16 // BUILD, build_tables, 0)

    def codes_of(pair):
        return [codes_ref[pl.ds(spot_ref[side, pair], 8, stride=8), :] for side in range(2)]

    def chosen_pair(pair):
        left, right = codes_of(pair)
        same = left == right
        left_is = [left == i for i in range(STATES)]
        right_is = [right == i for i in range(STATES)]
        found = []
        for c in range(CLS):
            pi = [pi_ref[c, i] for i in range(STATES)]
            left_pi = pick(left_is, pi)
            right_pi = pick(right_is, pi)
            left_step = rate4_ref[4 + c, pair] * left_pi
            right_step = rate4_ref[c, pair] * right_pi
            base = rate4_ref[8 + c, pair] * (left_pi * right_pi)
            base = base + jnp.where(same, rate4_ref[12 + c, pair] * left_pi, 0.0)
            at_right = base + left_step
            at_left = base + right_step
            at_left = jnp.where(same, at_left + (left_step + 1.0), at_left)
            found.append(
                [
                    jnp.where(left_is[i], at_left, jnp.where(right_is[i], at_right, base))
                    for i in range(STATES)
                ]
            )
        return found

    def small_tree(m, u):
        n = 2 * m + u
        tops, pairs = pairs_of(n)
        tables = [
            jnp.broadcast_to(table_ref[m, 4 * u + c : 4 * u + c + 1, :], TILE) for c in range(CLS)
        ]
        halves = []
        for h in range(2):
            sides = codes_of(pairs[2 * h])
            code = lax.shift_left(sides[0], 2) + sides[1] + 64 * h
            looked = []
            for i in range(STATES):
                place = code + 16 * i if i else code
                looked.append([lanes_of(tables[c], place) for c in range(CLS)])
            chosen = chosen_pair(pairs[2 * h + 1])
            parts = []
            for c in range(CLS):
                ratios = [ratio_ref[c, i] for i in range(3)]
                values = [looked[i][c] * chosen[c][i] for i in range(STATES)]
                parts.append(moved(values, step_ref[c, tops[h]], mean_by_last(ratios, values)))
            halves.append(parts)
        for c in range(CLS):
            ratios = [ratio_ref[c, i] for i in range(3)]
            values = product(halves[0][c], halves[1][c])
            average = mean_by_last(ratios, values)
            inverse = 1.0 / average
            own_rate = step_ref[4 + c, 32 * group + n]
            for i in range(STATES):
                mid_ref[n, c, i] = values[i] * inverse + own_rate
            log_ref[n, c] = jnp.log(average)

    def small_trees(m, _):
        for u in range(16):
            small_tree(8 * m + u // 2, u % 2)
        return 0

    def tail_pair(at):
        return [spot_ref[6 + side, at] for side in range(2)]

    def send(at, c, value):
        for q in range(4):
            out_ref[lax.bitwise_and(q - group, 3), at, 2 * c : 2 * c + 2, :] = value[2 * q : 2 * q + 2, :]

    def clade(j, totals):
        tops = [top - 1920 for top in tail_pair(96 + 4 * group + j)]
        pairs = [pair - 1920 for top in tops for pair in tail_pair(top)]
        leaves = [leaf - 1792 - group * 32 for pair in pairs for leaf in tail_pair(pair)]
        for c in range(CLS):
            ratios = [ratio_ref[c, i] for i in range(3)]
            scale = log_ref[leaves[0], c]
            for leaf in leaves[1:]:
                scale = scale + log_ref[leaf, c]
            halves = []
            for h in range(2):
                quads = []
                for at in (2 * h, 2 * h + 1):
                    joined = [
                        mid_ref[leaves[2 * at], c, i] * mid_ref[leaves[2 * at + 1], c, i]
                        for i in range(STATES)
                    ]
                    quads.append(moved(joined, step_ref[8 + c, pairs[at]], mean_by_last(ratios, joined)))
                joined = product(quads[0], quads[1])
                halves.append(moved(joined, step_ref[8 + c, tops[h]], mean_by_last(ratios, joined)))
            joined = product(halves[0], halves[1])
            inverse = 1.0 / joined[3]
            for v in range(3):
                send(3 * j + v, c, joined[v] * inverse)
            scale = scale + jnp.log(joined[3])
            totals[c] = scale if j == 0 else totals[c] + scale

    step_copy.wait()
    rate4_copy.wait()
    for load in loads:
        load.wait()
    lax.fori_loop(0, 2, small_trees, 0)
    totals = [None] * CLS
    for j in range(4):
        clade(j, totals)
    for c in range(CLS):
        send(12, c, totals[c])


def upper_kernel(
    place_ref, own_ref, one_ref, two_ref, three_ref, top_ref, site_ref, part_ref, node_ref
):
    group = lax.axis_index("cls")
    pi = [top_ref[TOP_PI + i] for i in range(STATES)]
    scale = top_ref[TOP_CONST]
    for hop, piece_ref in enumerate((own_ref, one_ref, two_ref, three_ref)):
        scale = scale + piece_ref[12]
        source = 4 * lax.bitwise_and(group - hop, 3)
        for j in range(4):
            values = [piece_ref[3 * j + i] for i in range(3)]
            average = (pi[0] * values[0] + pi[1] * values[1]) + (pi[2] * values[2] + pi[3])
            step = top_ref[TOP_RATES + source + j] * average
            for i in range(3):
                node_ref[source + j, i] = values[i] + step
            node_ref[source + j, 3] = step + 1.0
    at = 16
    for level, count in ((6, 8), (7, 4), (8, 2), (9, 1)):
        for k in range(count):
            left = place_ref[2 * (at - 16)]
            right = place_ref[2 * (at - 16) + 1]
            joined = [node_ref[left, i] * node_ref[right, i] for i in range(STATES)]
            average = mean_state(pi, joined)
            if level == 6:
                scale = scale + jnp.log(average)
                inverse = 1.0 / average
                for i in range(STATES):
                    node_ref[at, i] = joined[i] * inverse + top_ref[TOP_RATES + at]
            elif level < 9:
                step = top_ref[TOP_RATES + at] * average
                for i in range(STATES):
                    node_ref[at, i] = joined[i] + step
            else:
                scale = scale + jnp.log(average)
            at += 1
    top = jnp.maximum(scale, pltpu.roll(scale, 2, 0))
    top = jnp.maximum(top, pltpu.roll(top, 4, 0))
    share = jnp.exp(scale - top)
    mass = share + pltpu.roll(share, 2, 0)
    mass = mass + pltpu.roll(mass, 4, 0)
    total = top + jnp.log(mass)
    site_ref[...] = total[0:2] * (1.0 / 1024.0)
    weight = top_ref[TOP_WEIGHT]
    classes = weight * (share / mass)
    row = lax.broadcasted_iota(jnp.int32, TILE, 0)
    column = lax.broadcasted_iota(jnp.int32, TILE, 1)
    by_row = [
        jnp.sum(values, axis=1, keepdims=True) for values in (classes, weight * total, weight)
    ]
    by_pair = lax.shift_right_logical(row, 1)
    line = jnp.where(by_pair == column, by_row[0], 0.0)
    line = jnp.where((column == 4) & (row < 2), by_row[1], line)
    line = jnp.where((column == 5) & (row < 2), by_row[2], line)
    line = jnp.sum(line, axis=0, keepdims=True)
    for k in range(16):
        part_ref[8 * k : 8 * k + 8, :] = jnp.broadcast_to(line, TILE)


def last_kernel(every_ref, site_ref, own_hbm, mean_hbm, site_hbm, own_ref, mean_ref, sems):
    site_copy = pltpu.make_async_copy(site_ref, site_hbm, sems.at[2])
    site_copy.start()
    group = lax.axis_index("cls")
    sums = every_ref[0:8, :]
    for k in range(1, 16):
        sums = sums + every_ref[8 * k : 8 * k + 8, :]
    sums = jnp.sum(sums, axis=0, keepdims=True)
    column = lax.broadcasted_iota(jnp.int32, (1, 128), 1)

    def entry(at):
        return jnp.sum(jnp.where(column == at, sums, 0.0), axis=1, keepdims=True)

    count = entry(5)
    own_ref[...] = entry(group) / count
    mean_ref[...] = entry(4) / (count * 1024.0)
    own_copy = pltpu.make_async_copy(own_ref, own_hbm, sems.at[0])
    mean_copy = pltpu.make_async_copy(mean_ref, mean_hbm, sems.at[1])
    own_copy.start()
    mean_copy.start()
    own_copy.wait()
    mean_copy.wait()
    site_copy.wait()


def per_device(tip_codes, counts, children, lengths, frequencies, weights):
    codes = tip_codes.reshape(32, 8, 8, 128).transpose(0, 2, 1, 3).reshape(2048, 128)
    child_rows = children.T
    smem = pl.BlockSpec(memory_space=SMEM)
    vmem = pl.BlockSpec(memory_space=VMEM)
    hbm = pl.BlockSpec(memory_space=pltpu.MemorySpace.HBM)
    ours, top, places = pl.pallas_call(
        lower_kernel,
        out_shape=(pltpu.VMEM((4, 13, 8, 128), FLOAT), pltpu.VMEM((TOP_ROWS, 8, 128), FLOAT), pltpu.SMEM((32,), jnp.int32)),
        in_specs=[hbm] * 6,
        out_specs=(vmem, vmem, smem),
        scratch_shapes=[
            pltpu.VMEM((2, 1023), jnp.int32),
            pltpu.SMEM((4, 4), FLOAT),
            pltpu.SMEM((4,), FLOAT),
            pltpu.VMEM((4, 2046), FLOAT),
            pltpu.VMEM((2048, 128), jnp.int32),
            pltpu.VMEM(TILE, jnp.int32),
            pltpu.VMEM((4, 2048), FLOAT),
            pltpu.VMEM(TILE, jnp.int32),
            pltpu.SMEM(TILE, jnp.int32),
            pltpu.VMEM((16, 128), FLOAT),
            pltpu.SMEM((16, 128), FLOAT),
            pltpu.VMEM((CLS, STATES, 8, 128), FLOAT),
            pltpu.VMEM((CLS, 3, 8, 128), FLOAT),
            pltpu.VMEM((4, 8, 128), FLOAT),
            pltpu.VMEM((4, 8, 128), FLOAT),
            pltpu.VMEM((16, 8, 128), FLOAT),
            pltpu.VMEM((16, 128), FLOAT),
            pltpu.SMEM((16, 128), FLOAT),
            pltpu.VMEM((32, CLS, STATES, 8, 128), FLOAT),
            pltpu.VMEM((32, CLS, 8, 128), FLOAT),
            pltpu.SemaphoreType.DMA((12,)),
        ],
        compiler_params=pltpu.CompilerParams(vmem_limit_bytes=16 * 1024 * 1024),
        name="lower_tree",
    )(
        *(
            pltpu.with_memory_space_constraint(array, pltpu.MemorySpace.HBM)
            for array in (child_rows, frequencies, weights, lengths, codes, counts.reshape(8, 128))
        )
    )
    pieces = [ours[0]]
    for hop in range(1, 4):
        pieces.append(lax.ppermute(ours[hop], "cls", [(k, (k + hop) % 4) for k in range(4)]))
    site, part = pl.pallas_call(
        upper_kernel,
        out_shape=(pltpu.VMEM((2, 128), FLOAT), pltpu.VMEM((128, 128), FLOAT)),
        in_specs=[smem] + [vmem] * 5,
        out_specs=(vmem, vmem),
        scratch_shapes=[pltpu.VMEM((32, STATES, 8, 128), FLOAT)],
        compiler_params=pltpu.CompilerParams(vmem_limit_bytes=16 * 1024 * 1024),
        name="upper_tree",
    )(places, *pieces, top)
    every = lax.all_to_all(part, ("cls", "site"), split_axis=0, concat_axis=0, tiled=True)
    own, mean, site = pl.pallas_call(
        last_kernel,
        out_shape=tuple(jax.ShapeDtypeStruct(shape, FLOAT) for shape in ((1, 1), (1, 1), (2, 128))),
        in_specs=[vmem, vmem],
        out_specs=(hbm, hbm, hbm),
        scratch_shapes=[
            pltpu.VMEM((1, 1), FLOAT),
            pltpu.VMEM((1, 1), FLOAT),
            pltpu.SemaphoreType.DMA((3,)),
        ],
        compiler_params=pltpu.CompilerParams(vmem_limit_bytes=16 * 1024 * 1024),
        name="last_sums",
    )(every, site)
    return site.reshape(1, 256), own.reshape(1), mean.reshape(())


def solution(mesh):
    return jax.shard_map(
        per_device,
        mesh=mesh,
        in_specs=(P("cls", "site"), P("site"), P(), P(), P(), P()),
        out_specs=(P("cls", "site"), P("cls"), P()),
        check_vma=False,
    )
```

```python
import jax
import jax.numpy as jnp
from jax import lax
from jax.experimental import pallas as pl
from jax.experimental.pallas import tpu as pltpu
from jax.sharding import PartitionSpec as P

CLS = 4
STATES = 4
FLOAT = jnp.float32
SMEM = pltpu.MemorySpace.SMEM
VMEM = pltpu.MemorySpace.VMEM
TILE = (8, 128)
BUILD = 16
TOP_RATES, TOP_PI, TOP_CONST, TOP_WEIGHT, TOP_ROWS = 0, 30, 34, 35, 36


def mean_state(pi, values):
    return (pi[0] * values[0] + pi[1] * values[1]) + (pi[2] * values[2] + pi[3] * values[3])


def mean_by_last(ratios, values):
    return (ratios[0] * values[0] + ratios[1] * values[1]) + (ratios[2] * values[2] + values[3])


def moved(values, rate, average):
    step = rate * average
    return [value + step for value in values]


def product(left, right):
    return [a * b for a, b in zip(left, right)]


def choose(selector, options):
    value = jnp.where(selector == 1, options[1], options[0])
    value = jnp.where(selector == 2, options[2], value)
    return jnp.where(selector == 3, options[3], value)


def pick(masks, options):
    value = jnp.where(masks[1], options[1], options[0])
    value = jnp.where(masks[2], options[2], value)
    return jnp.where(masks[3], options[3], value)


def lanes_of(rows, places):
    return lax.gather(
        rows,
        places[..., None],
        lax.GatherDimensionNumbers(
            offset_dims=(),
            collapsed_slice_dims=(1,),
            start_index_map=(1,),
            operand_batching_dims=(0,),
            start_indices_batching_dims=(0,),
        ),
        slice_sizes=(1, 1),
        mode=lax.GatherScatterMode.PROMISE_IN_BOUNDS,
    )


def lower_kernel(
    child_hbm, freq_hbm, weight_hbm, lengths_hbm, codes_hbm, counts_hbm,
    out_ref, top_ref, place_ref,
    child_vec, freq_ref, weight_ref, lengths_ref, codes_ref, counts_ref, rate_vec,
    spot_vec, spot_ref, step_vec, step_ref,
    pi_ref, ratio_ref, pattern_ref, factor_ref, table_ref, rate4_vec, rate4_ref, mid_ref, log_ref, sems,
):
    group = lax.axis_index("cls")
    small = [
        pltpu.make_async_copy(source, target, sems.at[4 + k])
        for k, (source, target) in enumerate(
            (
                (child_hbm, child_vec),
                (lengths_hbm, lengths_ref),
                (freq_hbm, freq_ref),
                (weight_hbm, weight_ref),
                (counts_hbm, counts_ref),
            )
        )
    ]
    for load in small:
        load.start()
    loads = [
        pltpu.make_async_copy(
            codes_hbm.at[pl.ds(512 * j, 512)], codes_ref.at[pl.ds(512 * j, 512)], sems.at[j]
        )
        for j in range(4)
    ]
    for load in loads:
        load.start()
    small[0].wait()
    half = lax.shift_right_logical(group, 1)

    def block(ref, start):
        return ref[:, pl.ds(pl.multiple_of(start, 128), 128)]

    local = block(child_vec, 128 * group) - 256 * group
    spot_vec[0:2] = lax.shift_left(lax.shift_right_logical(local, 3), 6) + lax.bitwise_and(local, 7)
    spot_vec[2:4] = block(child_vec, 512 + 128 * half) - (1024 + 128 * group)
    spot_vec[4:6] = child_vec[:, 768:896] - (1536 + 128 * half)
    spot_vec[6:8] = jnp.concatenate([child_vec[:, 896:1023], jnp.zeros((2, 1), jnp.int32)], axis=1)
    spot_copy = pltpu.make_async_copy(spot_vec, spot_ref, sems.at[9])
    spot_copy.start()
    for load in small[1:4]:
        load.wait()

    lane = lax.broadcasted_iota(jnp.int32, TILE, 1)
    sub = lax.broadcasted_iota(jnp.int32, TILE, 0)
    by_pair = lax.shift_right_logical(sub, 1)
    by_class = lax.bitwise_and(sub, 3)
    uniform, betas = [], []
    for c in range(CLS):
        raw = [jnp.full(TILE, freq_ref[c, i], FLOAT) for i in range(STATES)]
        inverse = 1.0 / ((raw[0] + raw[1]) + (raw[2] + raw[3]))
        uniform.append([value * inverse for value in raw])
        betas.append(1.0 / (1.0 - mean_state(uniform[c], uniform[c])))
        for i in range(STATES):
            pi_ref[c, i] = uniform[c][i]
        for i in range(3):
            ratio_ref[c, i] = uniform[c][i] / uniform[c][3]
    beta_rows = choose(by_class, betas)[:4]
    total = jnp.zeros((4, 128), FLOAT)
    for k in range(16):
        width = min(128, 2046 - 128 * k)
        part = lengths_ref[:, 128 * k : 128 * k + width]
        if width < 128:
            part = jnp.concatenate([part, jnp.zeros((4, 128 - width), FLOAT)], axis=1)
        total = total + part
        decay = jnp.exp(-(beta_rows * part))
        rate_vec[:, 128 * k : 128 * k + 128] = (1.0 - decay) / decay

    last_pi = choose(by_class, [uniform[c][3] for c in range(CLS)])[:4]
    step_vec[0:4] = block(rate_vec, 1536 + 128 * half) * last_pi
    step_vec[4:8] = rate_vec[:, 1792:1920] * last_pi
    step_vec[8:12] = rate_vec[:, 1920:2048] * last_pi
    step_vec[12:16] = jnp.zeros((4, 128), FLOAT)
    step_copy = pltpu.make_async_copy(step_vec, step_ref, sems.at[10])
    step_copy.start()

    def twice(rows):
        return jnp.concatenate([rows, rows], axis=0)

    low = twice(block(rate_vec, 256 * group))
    high = twice(block(rate_vec, 256 * group + 128))
    own = twice(block(rate_vec, 1024 + 128 * group))

    def rates_at(places):
        places = jnp.broadcast_to(places, TILE)
        inside = lax.bitwise_and(places, 127)
        return jnp.where(places < 128, lanes_of(low, inside), lanes_of(high, inside))

    left = rates_at(local[0:1])
    right = rates_at(local[1:2])
    both = left * right
    factor_ref[0] = right
    factor_ref[1] = left
    factor_ref[2] = both + own * (left + right + both)
    factor_ref[3] = own
    for k in range(4):
        rate4_vec[4 * k : 4 * k + 4] = factor_ref[k, 0:4]
    rate4_copy = pltpu.make_async_copy(rate4_vec, rate4_ref, sems.at[11])
    rate4_copy.start()

    own_state = lax.bitwise_and(lax.shift_right_logical(lane, 4), 3)
    left_code = lax.bitwise_and(lax.shift_right_logical(lane, 2), 3)
    right_code = lax.bitwise_and(lane, 3)
    left_own = own_state == left_code
    right_own = own_state == right_code
    first = lane < 64
    both_own = jnp.where(left_own, jnp.where(right_own, 1.0, 0.0), 0.0)
    by_rows = [choose(by_class, [uniform[c][i] for c in range(CLS)]) for i in range(STATES)]
    left_pi = choose(left_code, by_rows)
    right_pi = choose(right_code, by_rows)
    pattern_ref[0] = jnp.where(left_own, right_pi, 0.0)
    pattern_ref[1] = jnp.where(right_own, left_pi, 0.0)
    pattern_ref[2] = left_pi * right_pi
    pattern_ref[3] = jnp.where(left_code == right_code, left_pi, 0.0)

    for i in range(STATES):
        top_ref[TOP_PI + i] = choose(by_pair, [uniform[c][i] for c in range(CLS)])
    beta_pairs = choose(by_pair, betas)
    sums = choose(by_pair, [jnp.broadcast_to(total[c : c + 1], TILE) for c in range(CLS)])
    sums = jnp.broadcast_to(jnp.sum(sums, axis=1, keepdims=True), TILE)
    weights = [jnp.full(TILE, weight_ref[c], FLOAT) for c in range(CLS)]
    weight_sum = (weights[0] + weights[1]) + (weights[2] + weights[3])
    top_ref[TOP_CONST] = jnp.log(choose(by_pair, weights) / weight_sum) - beta_pairs * sums
    last = rate_vec[:, 1920:2048]
    last = choose(by_pair, [jnp.broadcast_to(last[c : c + 1], TILE) for c in range(CLS)])
    for k in range(30):
        top_ref[TOP_RATES + k] = jnp.broadcast_to(last[:, 96 + k : 97 + k], TILE)
    small[4].wait()
    quarter = counts_ref[pl.ds(2 * group, 2), :].astype(FLOAT)
    top_ref[TOP_WEIGHT] = jnp.concatenate([quarter, quarter, quarter, quarter], axis=0)
    spot_copy.wait()

    for k in range(15):
        for side in range(2):
            place_ref[2 * k + side] = spot_ref[6 + side, 112 + k] - 2016

    def pairs_of(n):
        tops = [spot_ref[4 + side, 32 * group + n] for side in range(2)]
        return tops, [spot_ref[2 + side, top] for top in tops for side in range(2)]

    upper_half = sub < 4

    def build_table(m):
        pairs = [pairs_of(2 * m + u)[1] for u in range(2)]
        places = jnp.where(
            upper_half,
            jnp.where(first, pairs[0][0], pairs[0][2]),
            jnp.where(first, pairs[1][0], pairs[1][2]),
        )
        table = both_own
        for k in range(4):
            table = table + lanes_of(factor_ref[k], places) * pattern_ref[k]
        table_ref[m] = table

    def build_tables(m, _):
        for u in range(BUILD):
            build_table(BUILD * m + u)
        return 0

    lax.fori_loop(0, 16 // BUILD, build_tables, 0)

    def codes_of(pair):
        return [codes_ref[pl.ds(spot_ref[side, pair], 8, stride=8), :] for side in range(2)]

    def chosen_pair(pair):
        left, right = codes_of(pair)
        same = left == right
        left_is = [left == i for i in range(STATES)]
        right_is = [right == i for i in range(STATES)]
        found = []
        for c in range(CLS):
            pi = [pi_ref[c, i] for i in range(STATES)]
            left_pi = pick(left_is, pi)
            right_pi = pick(right_is, pi)
            left_step = rate4_ref[4 + c, pair] * left_pi
            right_step = rate4_ref[c, pair] * right_pi
            base = rate4_ref[8 + c, pair] * (left_pi * right_pi)
            base = base + jnp.where(same, rate4_ref[12 + c, pair] * left_pi, 0.0)
            at_right = base + left_step
            at_left = base + right_step
            at_left = jnp.where(same, at_left + (left_step + 1.0), at_left)
            found.append(
                [
                    jnp.where(left_is[i], at_left, jnp.where(right_is[i], at_right, base))
                    for i in range(STATES)
                ]
            )
        return found

    def small_tree(m, u):
        n = 2 * m + u
        tops, pairs = pairs_of(n)
        tables = [
            jnp.broadcast_to(table_ref[m, 4 * u + c : 4 * u + c + 1, :], TILE) for c in range(CLS)
        ]
        halves = []
        for h in range(2):
            sides = codes_of(pairs[2 * h])
            code = lax.shift_left(sides[0], 2) + sides[1] + 64 * h
            looked = []
            for i in range(STATES):
                place = code + 16 * i if i else code
                looked.append([lanes_of(tables[c], place) for c in range(CLS)])
            chosen = chosen_pair(pairs[2 * h + 1])
            parts = []
            for c in range(CLS):
                ratios = [ratio_ref[c, i] for i in range(3)]
                values = [looked[i][c] * chosen[c][i] for i in range(STATES)]
                parts.append(moved(values, step_ref[c, tops[h]], mean_by_last(ratios, values)))
            halves.append(parts)
        for c in range(CLS):
            ratios = [ratio_ref[c, i] for i in range(3)]
            values = product(halves[0][c], halves[1][c])
            average = mean_by_last(ratios, values)
            inverse = 1.0 / average
            own_rate = step_ref[4 + c, 32 * group + n]
            for i in range(STATES):
                mid_ref[n, c, i] = values[i] * inverse + own_rate
            log_ref[n, c] = jnp.log(average)

    def small_trees(m, _):
        for u in range(16):
            small_tree(8 * m + u // 2, u % 2)
        return 0

    def tail_pair(at):
        return [spot_ref[6 + side, at] for side in range(2)]

    def send(at, c, value):
        for q in range(4):
            out_ref[lax.bitwise_and(q - group, 3), at, 2 * c : 2 * c + 2, :] = value[2 * q : 2 * q + 2, :]

    def clade(j, totals):
        tops = [top - 1920 for top in tail_pair(96 + 4 * group + j)]
        pairs = [pair - 1920 for top in tops for pair in tail_pair(top)]
        leaves = [leaf - 1792 - group * 32 for pair in pairs for leaf in tail_pair(pair)]
        for c in range(CLS):
            ratios = [ratio_ref[c, i] for i in range(3)]
            scale = log_ref[leaves[0], c]
            for leaf in leaves[1:]:
                scale = scale + log_ref[leaf, c]
            halves = []
            for h in range(2):
                quads = []
                for at in (2 * h, 2 * h + 1):
                    joined = [
                        mid_ref[leaves[2 * at], c, i] * mid_ref[leaves[2 * at + 1], c, i]
                        for i in range(STATES)
                    ]
                    quads.append(moved(joined, step_ref[8 + c, pairs[at]], mean_by_last(ratios, joined)))
                joined = product(quads[0], quads[1])
                halves.append(moved(joined, step_ref[8 + c, tops[h]], mean_by_last(ratios, joined)))
            joined = product(halves[0], halves[1])
            inverse = 1.0 / joined[3]
            for v in range(3):
                send(3 * j + v, c, joined[v] * inverse)
            scale = scale + jnp.log(joined[3])
            totals[c] = scale if j == 0 else totals[c] + scale

    step_copy.wait()
    rate4_copy.wait()
    for load in loads:
        load.wait()
    lax.fori_loop(0, 2, small_trees, 0)
    totals = [None] * CLS
    for j in range(4):
        clade(j, totals)
    for c in range(CLS):
        send(12, c, totals[c])


def upper_kernel(
    place_ref, own_ref, one_ref, two_ref, three_ref, top_ref, site_ref, part_ref, node_ref
):
    group = lax.axis_index("cls")
    pi = [top_ref[TOP_PI + i] for i in range(STATES)]
    scale = top_ref[TOP_CONST]
    for hop, piece_ref in enumerate((own_ref, one_ref, two_ref, three_ref)):
        scale = scale + piece_ref[12]
        source = 4 * lax.bitwise_and(group - hop, 3)
        for j in range(4):
            values = [piece_ref[3 * j + i] for i in range(3)]
            average = (pi[0] * values[0] + pi[1] * values[1]) + (pi[2] * values[2] + pi[3])
            step = top_ref[TOP_RATES + source + j] * average
            for i in range(3):
                node_ref[source + j, i] = values[i] + step
            node_ref[source + j, 3] = step + 1.0
    at = 16
    for level, count in ((6, 8), (7, 4), (8, 2), (9, 1)):
        for k in range(count):
            left = place_ref[2 * (at - 16)]
            right = place_ref[2 * (at - 16) + 1]
            joined = [node_ref[left, i] * node_ref[right, i] for i in range(STATES)]
            average = mean_state(pi, joined)
            if level == 6:
                scale = scale + jnp.log(average)
                inverse = 1.0 / average
                for i in range(STATES):
                    node_ref[at, i] = joined[i] * inverse + top_ref[TOP_RATES + at]
            elif level < 9:
                step = top_ref[TOP_RATES + at] * average
                for i in range(STATES):
                    node_ref[at, i] = joined[i] + step
            else:
                scale = scale + jnp.log(average)
            at += 1
    top = jnp.maximum(scale, pltpu.roll(scale, 2, 0))
    top = jnp.maximum(top, pltpu.roll(top, 4, 0))
    share = jnp.exp(scale - top)
    mass = share + pltpu.roll(share, 2, 0)
    mass = mass + pltpu.roll(mass, 4, 0)
    total = top + jnp.log(mass)
    site_ref[...] = total[0:2] * (1.0 / 1024.0)
    weight = top_ref[TOP_WEIGHT]
    classes = weight * (share / mass)
    row = lax.broadcasted_iota(jnp.int32, TILE, 0)
    column = lax.broadcasted_iota(jnp.int32, TILE, 1)
    by_row = [
        jnp.sum(values, axis=1, keepdims=True) for values in (classes, weight * total, weight)
    ]
    by_pair = lax.shift_right_logical(row, 1)
    line = jnp.where(by_pair == column, by_row[0], 0.0)
    line = jnp.where((column == 4) & (row < 2), by_row[1], line)
    line = jnp.where((column == 5) & (row < 2), by_row[2], line)
    line = jnp.sum(line, axis=0, keepdims=True)
    for k in range(16):
        part_ref[8 * k : 8 * k + 8, :] = jnp.broadcast_to(line, TILE)


def last_kernel(every_ref, site_ref, own_hbm, mean_hbm, site_hbm, own_ref, mean_ref, sems):
    site_copy = pltpu.make_async_copy(site_ref, site_hbm, sems.at[2])
    site_copy.start()
    group = lax.axis_index("cls")
    sums = every_ref[0:8, :]
    for k in range(1, 16):
        sums = sums + every_ref[8 * k : 8 * k + 8, :]
    sums = jnp.sum(sums, axis=0, keepdims=True)
    column = lax.broadcasted_iota(jnp.int32, (1, 128), 1)

    def entry(at):
        return jnp.sum(jnp.where(column == at, sums, 0.0), axis=1, keepdims=True)

    count = entry(5)
    own_ref[...] = entry(group) / count
    mean_ref[...] = entry(4) / (count * 1024.0)
    own_copy = pltpu.make_async_copy(own_ref, own_hbm, sems.at[0])
    mean_copy = pltpu.make_async_copy(mean_ref, mean_hbm, sems.at[1])
    own_copy.start()
    mean_copy.start()
    own_copy.wait()
    mean_copy.wait()
    site_copy.wait()


def per_device(tip_codes, counts, children, lengths, frequencies, weights):
    codes = tip_codes.reshape(32, 8, 8, 128).transpose(0, 2, 1, 3).reshape(2048, 128)
    child_rows = children.T
    smem = pl.BlockSpec(memory_space=SMEM)
    vmem = pl.BlockSpec(memory_space=VMEM)
    hbm = pl.BlockSpec(memory_space=pltpu.MemorySpace.HBM)
    ours, top, places = pl.pallas_call(
        lower_kernel,
        out_shape=(pltpu.VMEM((4, 13, 8, 128), FLOAT), pltpu.VMEM((TOP_ROWS, 8, 128), FLOAT), pltpu.SMEM((32,), jnp.int32)),
        in_specs=[hbm] * 6,
        out_specs=(vmem, vmem, smem),
        scratch_shapes=[
            pltpu.VMEM((2, 1023), jnp.int32),
            pltpu.SMEM((4, 4), FLOAT),
            pltpu.SMEM((4,), FLOAT),
            pltpu.VMEM((4, 2046), FLOAT),
            pltpu.VMEM((2048, 128), jnp.int32),
            pltpu.VMEM(TILE, jnp.int32),
            pltpu.VMEM((4, 2048), FLOAT),
            pltpu.VMEM(TILE, jnp.int32),
            pltpu.SMEM(TILE, jnp.int32),
            pltpu.VMEM((16, 128), FLOAT),
            pltpu.SMEM((16, 128), FLOAT),
            pltpu.VMEM((CLS, STATES, 8, 128), FLOAT),
            pltpu.VMEM((CLS, 3, 8, 128), FLOAT),
            pltpu.VMEM((4, 8, 128), FLOAT),
            pltpu.VMEM((4, 8, 128), FLOAT),
            pltpu.VMEM((16, 8, 128), FLOAT),
            pltpu.VMEM((16, 128), FLOAT),
            pltpu.SMEM((16, 128), FLOAT),
            pltpu.VMEM((32, CLS, STATES, 8, 128), FLOAT),
            pltpu.VMEM((32, CLS, 8, 128), FLOAT),
            pltpu.SemaphoreType.DMA((12,)),
        ],
        compiler_params=pltpu.CompilerParams(vmem_limit_bytes=16 * 1024 * 1024),
        name="lower_tree",
    )(
        *(
            pltpu.with_memory_space_constraint(array, pltpu.MemorySpace.HBM)
            for array in (child_rows, frequencies, weights, lengths, codes, counts.reshape(8, 128))
        )
    )
    pieces = [ours[0]]
    for hop in range(1, 4):
        pieces.append(lax.ppermute(ours[hop], "cls", [(k, (k + hop) % 4) for k in range(4)]))
    site, part = pl.pallas_call(
        upper_kernel,
        out_shape=(pltpu.VMEM((2, 128), FLOAT), pltpu.VMEM((128, 128), FLOAT)),
        in_specs=[smem] + [vmem] * 5,
        out_specs=(vmem, vmem),
        scratch_shapes=[pltpu.VMEM((32, STATES, 8, 128), FLOAT)],
        compiler_params=pltpu.CompilerParams(vmem_limit_bytes=16 * 1024 * 1024),
        name="upper_tree",
    )(places, *pieces, top)
    every = lax.all_to_all(part, ("cls", "site"), split_axis=0, concat_axis=0, tiled=True)
    own, mean, site = pl.pallas_call(
        last_kernel,
        out_shape=tuple(jax.ShapeDtypeStruct(shape, FLOAT) for shape in ((1, 1), (1, 1), (2, 128))),
        in_specs=[vmem, vmem],
        out_specs=(hbm, hbm, hbm),
        scratch_shapes=[
            pltpu.VMEM((1, 1), FLOAT),
            pltpu.VMEM((1, 1), FLOAT),
            pltpu.SemaphoreType.DMA((3,)),
        ],
        compiler_params=pltpu.CompilerParams(vmem_limit_bytes=16 * 1024 * 1024),
        name="last_sums",
    )(every, site)
    return site.reshape(1, 256), own.reshape(1), mean.reshape(())


def solution(mesh):
    return jax.shard_map(
        per_device,
        mesh=mesh,
        in_specs=(P("cls", "site"), P("site"), P(), P(), P(), P()),
        out_specs=(P("cls", "site"), P("cls"), P()),
        check_vma=False,
    )
```
